32 devices in a mesh: section: 2 (over x), grp: 4 (over y, core), dp: 4 (over z).
Axes of the slice: x: 2, y: 2, z: 4, core: 2. Of those that a mesh axis runs over, the one named last changes fastest.
Arguments:
- embeddings: bfloat16 [32, 256, 768], P(('grp', 'dp')), may hold values from -6 to 6
- mask_flags: int32 [32, 256], P(('grp', 'dp')), may hold values 0 or 1
- timesteps: int32 [32], P(('grp', 'dp')), may hold values from 0 to 999, as said below
- time_table: bfloat16 [1000, 768], replicated, may hold values from -6 to 6
- mask_vector: bfloat16 [768], replicated, may hold values from -6 to 6
- attn_qkv: bfloat16 [2, 768, 2304], P('section', 'grp'), may hold values from -0.21875 to 0.21875
- attn_out: bfloat16 [2, 768, 768], P('section', 'grp'), may hold values from -0.875 to 0.875
- mlp_in: bfloat16 [2, 768, 3072], P('section', 'grp'), may hold values from -0.21875 to 0.21875
- mlp_out: bfloat16 [2, 3072, 768], P('section', 'grp'), may hold values from -0.109375 to 0.109375
- norm_gains: float32 [2, 2, 768], P('section'), may hold values from 0.5 to 1.5
- cotangent: bfloat16 [32, 256, 768], P(('grp', 'dp')), may hold values from -6 to 6
Outputs:
- activations: bfloat16 [2, 32, 256, 768], P('section', ('grp', 'dp'))
- input_grads: float32 [2, 32, 256, 768], P('section', ('grp', 'dp'))
- grad_qkv: float32 [2, 768, 2304], P('section', 'grp')
- grad_attn_out: float32 [2, 768, 768], P('section', 'grp')
- grad_mlp_in: float32 [2, 768, 3072], P('section', 'grp')
- grad_mlp_out: float32 [2, 3072, 768], P('section', 'grp')
- grad_gains: float32 [2, 2, 768], P('section', None, 'grp')
- grad_table: float32 [1000, 768], P(('section', 'grp'))
- grad_mask_vector: float32 [768], P(('section', 'grp'))
The draws below stay inside these ranges and needn't reach their ends.
Inputs may be any that keep to these rules, and one draw needn't show every extreme that they name: per-sequence timesteps, concentrated toward the high end; both ends are taken.
All inputs are finite; a program needn't handle non-finite values. No bound on the sum of `mask_flags` on one device may be relied on, other than what follows from the above.
Results may differ from the reference program's by a relative error of at most 0.018.
Values may be sent and summed in bfloat16 or wider, within the bound.
A program may use at most 192 MiB of HBM per device.

```python
import math
import jax
import jax.numpy as jnp
from jax import lax

D = 768
HEADS = 12
HEAD = 64
FF = 3072
TSTEPS = 1000
SEQ = 256
SEQS = 32


def draw_timesteps(key, part):
    key_one, key_two, key_three, key_four = jax.random.split(key, 4)
    draw_one = jax.random.randint(key_one, (SEQS,), 0, TSTEPS)
    draw_two = jax.random.randint(key_two, (SEQS,), 0, TSTEPS)
    level_draw = TSTEPS - 1 - jnp.minimum(draw_one, draw_two)
    top_place = jax.random.randint(key_three, (), 0, SEQS)
    low_place = (top_place + 1 + jax.random.randint(key_four, (), 0, SEQS - 1)) % SEQS
    level_draw = level_draw.at[top_place].set(TSTEPS - 1).at[low_place].set(0)
    return level_draw.astype(jnp.int32)


def set_ends(array, key, smallest, top_value):
    place = [jax.random.randint(jax.random.fold_in(key, axis), (), 0, length) for axis, length in enumerate(array.shape)]
    longest = array.shape.index(max(array.shape))
    beside = place[:longest] + [(place[longest] + 1) % array.shape[longest]] + place[longest + 1:]
    return array.at[tuple(place)].set(smallest).at[tuple(beside)].set(top_value)


def steps_of(rng, dims, pieces, low, top_value):
    loudness, own = 1.0, jax.random.fold_in(rng, 6)
    for axis_at, shards_of in pieces:
        steps = jnp.exp(jax.random.uniform(jax.random.fold_in(own, axis_at), (shards_of,), jnp.float32, low / len(pieces), top_value / len(pieces)))
        loudness = loudness * jnp.repeat(steps, dims[axis_at] // shards_of).reshape([-1 if axis == axis_at else 1 for axis in range(len(dims))])
    return loudness


def centred(stream_key, extent, width, limit, cuts=(), kind=jnp.bfloat16):
    result = width * jax.random.normal(stream_key, extent, jnp.float32)
    if cuts:
        result = result * steps_of(stream_key, extent, cuts, -0.22, 0.18)
    return jnp.clip(result, -limit, limit).astype(kind)


def setup_inputs(seed: int = 0) -> dict:
    streams_of = jax.random.split(jax.random.key(seed), 12)
    return {
        "embeddings": centred(streams_of[0], (SEQS, SEQ, D), 1.0, 6.0, ((0, 16),)),
        "mask_flags": set_ends((jax.random.randint(streams_of[1], (SEQS, SEQ), 0, 2) < 1).astype(jnp.int32), jax.random.fold_in(streams_of[1], 1), 0, 1),
        "timesteps": draw_timesteps(jax.random.fold_in(streams_of[11], 71), 0),
        "time_table": centred(streams_of[3], (TSTEPS, D), 1.0, 6.0),
        "mask_vector": centred(streams_of[4], (D,), 1.0, 6.0),
        "attn_qkv": centred(streams_of[5], (2, D, 3 * D), D ** -0.5, 0.21875, ((0, 2), (1, 4))),
        "attn_out": centred(streams_of[6], (2, D, D), (D // 16) ** -0.5, 0.875, ((0, 2), (1, 4))),
        "mlp_in": centred(streams_of[7], (2, D, FF), D ** -0.5, 0.21875, ((0, 2), (1, 4))),
        "mlp_out": centred(streams_of[8], (2, FF, D), FF ** -0.5, 0.109375, ((0, 2), (1, 4))),
        "norm_gains": jnp.clip(1.0 + 0.1 * jax.random.normal(streams_of[9], (2, 2, D), jnp.float32), 0.5, 1.5),
        "cotangent": centred(streams_of[10], (SEQS, SEQ, D), 1.0, 6.0, ((0, 16),)),
    }


exact_mode = lax.Precision.HIGHEST

@jax.custom_vjp
def low(v):
    return lax.optimization_barrier(v.astype(jnp.bfloat16)).astype(jnp.float32)

@jax.custom_vjp
def low_back(v):
    return v

def low_keep(v):
    return (low(v), None)

def low_pass(kept, grad):
    return (grad,)

def back_keep(v):
    return (v, None)

def back_low(kept, grad):
    return (low(grad),)
low.defvjp(low_keep, low_pass)
low_back.defvjp(back_keep, back_low)

def both_ways(value):
    return low(low_back(value))

def layer_norm(hidden, gain_row):
    center = hidden - lax.optimization_barrier(jnp.mean(hidden, axis=-1, keepdims=True))
    spread = lax.optimization_barrier(jnp.mean(center * center, axis=-1, keepdims=True))
    return center * lax.rsqrt(spread + 1e-05) * gain_row

def residual_block(hidden, w_qkv, w_proj, w_up, w_down, gains):
    batch_size, length, model_width = hidden.shape
    normed = low(layer_norm(hidden, gains[0]))
    packed = both_ways(jnp.einsum('bsd,df->bsf', normed, w_qkv, precision=exact_mode))
    queries = packed[..., :model_width].reshape(batch_size, length, HEADS, HEAD)
    attn_keys = packed[..., model_width:2 * model_width].reshape(batch_size, length, HEADS, HEAD)
    values = packed[..., 2 * model_width:].reshape(batch_size, length, HEADS, HEAD)
    scaling = 1.0 / math.sqrt(HEAD)
    scores = low_back(scaling * jnp.einsum('bqhe,bkhe->bhqk', queries, attn_keys, precision=exact_mode))
    attn_probs = low(jax.nn.softmax(scores, axis=-1))
    attn_mixed = both_ways(jnp.einsum('bhqk,bkhe->bqhe', attn_probs, values, precision=exact_mode).reshape(batch_size, length, model_width))
    middle = hidden + low_back(jnp.einsum('bsd,df->bsf', attn_mixed, w_proj, precision=exact_mode))
    normed_two = low(layer_norm(middle, gains[1]))
    upward = low_back(jnp.einsum('bsd,df->bsf', normed_two, w_up, precision=exact_mode))
    activated = low(jax.nn.gelu(upward, approximate=True))
    return middle + low_back(jnp.einsum('bsf,fd->bsd', activated, w_down, precision=exact_mode))

def forward(embeds, time_table, mask_vec, w_qkv, w_proj, w_up, w_down, gains, offset, steps_index, flag_rows):
    onehot = (steps_index[:, None] == jnp.arange(TSTEPS, dtype=jnp.int32)[None, :]).astype(jnp.float32)
    table_rows = jnp.dot(onehot, time_table, precision=exact_mode)
    start_rows = jnp.where(flag_rows[..., None] == 1, mask_vec[None, None, :], embeds) + table_rows[:, None, :]
    first_out = low_back(low(residual_block(start_rows, w_qkv[0], w_proj[0], w_up[0], w_down[0], gains[0])))
    second_out = residual_block(first_out + offset, w_qkv[1], w_proj[1], w_up[1], w_down[1], gains[1])
    return (second_out, first_out)

def reference(embeddings, mask_flags, timesteps, time_table, mask_vector, attn_qkv, attn_out, mlp_in, mlp_out, norm_gains, cotangent):
    group_size = 1
    for candidate in range(1, SEQS + 1):
        if SEQS % candidate == 0 and candidate * SEQ <= max(4096, SEQ):
            group_size = candidate
    groups = SEQS // group_size
    table32 = time_table.astype(jnp.float32)
    vector32 = mask_vector.astype(jnp.float32)
    weights32 = (attn_qkv.astype(jnp.float32), attn_out.astype(jnp.float32), mlp_in.astype(jnp.float32), mlp_out.astype(jnp.float32))
    gains32 = norm_gains.astype(jnp.float32)

    def group_step(totals, inputs):
        embeds, flag_rows, steps_index, cot_rows = inputs

        def wrapped(embeds_in, table_in, vector_in, wq_in, wp_in, wu_in, wd_in, gains_in, offset_in):
            return forward(embeds_in, table_in, vector_in, wq_in, wp_in, wu_in, wd_in, gains_in, offset_in, steps_index, flag_rows)
        offset = jnp.zeros_like(embeds)
        second_out, back_fn, first_out = jax.vjp(wrapped, embeds, table32, vector32, weights32[0], weights32[1], weights32[2], weights32[3], gains32, offset, has_aux=True)
        grad_all = back_fn(cot_rows)
        new_totals = tuple((total + part_grad for total, part_grad in zip(totals, grad_all[1:8])))
        return (new_totals, (second_out, first_out, grad_all[0], grad_all[8]))
    totals_init = (jnp.zeros_like(table32), jnp.zeros_like(vector32), jnp.zeros_like(weights32[0]), jnp.zeros_like(weights32[1]), jnp.zeros_like(weights32[2]), jnp.zeros_like(weights32[3]), jnp.zeros_like(gains32))
    inputs = (embeddings.astype(jnp.float32).reshape(groups, group_size, SEQ, D), mask_flags.reshape(groups, group_size, SEQ), timesteps.reshape(groups, group_size), cotangent.astype(jnp.float32).reshape(groups, group_size, SEQ, D))
    totals, stacked = lax.scan(group_step, totals_init, inputs)
    second_all = stacked[0].reshape(SEQS, SEQ, D)
    first_all = stacked[1].reshape(SEQS, SEQ, D)
    embed_grad = stacked[2].reshape(SEQS, SEQ, D)
    offset_grad = stacked[3].reshape(SEQS, SEQ, D)
    activations = jnp.stack([first_all, second_all]).astype(jnp.bfloat16)
    input_grads = jnp.stack([embed_grad, offset_grad])
    return (activations, input_grads, totals[2], totals[3], totals[4], totals[5], totals[6], totals[0], totals[1])
```

```python
import functools
import math

import jax
import jax.numpy as jnp
from jax import lax
from jax.experimental import pallas as pl
from jax.experimental.pallas import tpu as pltpu
from jax.sharding import PartitionSpec as P

HEADS = 12
HEAD = 64
BF = jnp.bfloat16
F32 = jnp.float32
MESH = pl.DeviceIdType.MESH
EPS = 1e-05
GELU_C = math.sqrt(2.0 / math.pi)

OUT0, IN0, PROJ, QKV0, CHUNKS = 0, 4, 8, 9, 12
GATHER_ORDER = (9, 10, 11, 8, 4, 5, 6, 7, 0, 1, 2, 3)


def dot_nn(a, b):
    return lax.dot_general(a, b, (((1,), (0,)), ((), ())), preferred_element_type=F32)


def dot_nt(a, b):
    return lax.dot_general(a, b, (((1,), (1,)), ((), ())), preferred_element_type=F32)


def dot_tn(a, b):
    return lax.dot_general(a, b, (((0,), (0,)), ((), ())), preferred_element_type=F32)


def loop(n, body):
    lax.fori_loop(0, n, lambda i, c: (body(i), c)[1], 0)


def mega(
    cfg,
    times_ref,
    mask_ref,
    vector_ref,
    gains_ref,
    emb_hbm,
    cot_hbm,
    table_hbm,
    wq_hbm,
    wp_hbm,
    wi_hbm,
    wo_hbm,
    act_out,
    dx_out,
    grad_out,
    small_out,
    table_out,
    w,
    h,
    mid,
    acc,
    tmp,
    normed,
    mixed,
    n2,
    actv,
    gp,
    packed,
    probs,
    glow,
    dmlow,
    dpk,
    do_ref,
    outb,
    relay,
    maskc,
    trow,
    pay,
    gains_acc,
    cbuf,
    ybuf,
    z1,
    z2,
    in_sem,
    own_sem,
    gsend,
    grecv,
    rsend,
    rrecv,
    csend,
    crecv,
    usend,
    urecv,
    psend,
    precv,
    osem,
    *extra,
):
    count, seq, width, nz, unit = cfg
    quarter = width // 4
    units = CHUNKS * quarter // unit
    per_block = quarter // unit
    table_rows = table_hbm.shape[0]
    s = lax.axis_index("section")
    g = lax.axis_index("grp")
    d = lax.axis_index("dp")
    x0 = s == 0
    x1 = jnp.logical_not(x0)
    c = lax.rem(g, 2)
    y = g // 2
    twin = g + 1 - 2 * c
    across = lax.rem(g + 2, 4)
    zpair = d + 1 - 2 * lax.rem(d, 2)
    zfar = lax.rem(d + 2, 4)
    half = lax.rem(d, 2)

    peers = [{"section": 1 - s}, {"grp": twin}, {"grp": across}, {"dp": zpair}]
    if nz == 4:
        peers += [{"dp": 3 - d}, {"dp": zfar}]
    barrier = pltpu.get_barrier_semaphore()
    for peer in peers:
        pl.semaphore_signal(barrier, inc=1, device_id=peer, device_id_type=MESH)
    pl.semaphore_wait(barrier, len(peers))

    def remote(src, dst, send, recv, peer):
        return pltpu.make_async_remote_copy(
            src_ref=src, dst_ref=dst, send_sem=send, recv_sem=recv, device_id=peer, device_id_type=MESH
        )

    def rows(start, size, by):
        return pl.ds(pl.multiple_of(start, by), size)

    def place(i, q):
        return jnp.where(i < IN0, q * width + quarter * i, i * width + quarter * q)

    def source(i):
        if i < IN0:
            return wo_hbm.at[pl.ds(i * quarter, quarter)]
        if i < PROJ:
            return wi_hbm.at[:, pl.ds((i - IN0) * width, width)]
        if i == PROJ:
            return wp_hbm
        return wq_hbm.at[:, pl.ds((i - QKV0) * width, width)]

    hq = quarter // 2
    far = across
    far_twin = lax.rem(twin + 2, 4)

    def own_copy(i):
        return pltpu.make_async_copy(source(i), w.at[rows(place(i, g), quarter, hq)], own_sem.at[i])

    def own_to_twin(i):
        return remote(source(i), w.at[rows(place(i, g), quarter, hq)], gsend.at[0, i], grecv.at[0, i], {"grp": twin})

    def own_across(i):
        return remote(
            source(i).at[rows(half * hq, hq, hq)],
            w.at[rows(place(i, g) + half * hq, hq, hq)],
            gsend.at[1, i],
            grecv.at[1, i],
            {"grp": across},
        )

    def y_half(i, q):
        return w.at[rows(place(i, q) + half * hq, hq, hq)]

    def z_half(i, q):
        return w.at[rows(place(i, q) + (1 - half) * hq, hq, hq)]

    def y_to_z(i):
        return remote(y_half(i, far), y_half(i, far), gsend.at[2, i], grecv.at[2, i], {"dp": zpair})

    def y_to_twin(i):
        return remote(y_half(i, far), y_half(i, far), gsend.at[3, i], grecv.at[3, i], {"grp": twin})

    def z_to_twin(i):
        return remote(z_half(i, far), z_half(i, far), gsend.at[4, i], grecv.at[4, i], {"grp": twin})

    def recv_y(i):
        remote(y_half(i, far), y_half(i, far), gsend.at[1, i], grecv.at[1, i], {"grp": across}).wait_recv()

    def recv_z(i):
        remote(z_half(i, far), z_half(i, far), gsend.at[2, i], grecv.at[2, i], {"dp": zpair}).wait_recv()

    def near_ready(i):
        dst = w.at[rows(place(i, twin), quarter, hq)]
        remote(dst, dst, gsend.at[0, i], grecv.at[0, i], {"grp": twin}).wait_recv()
        own_copy(i).wait()

    def far_ready(i):
        dst = y_half(i, far_twin)
        remote(dst, dst, gsend.at[3, i], grecv.at[3, i], {"grp": twin}).wait_recv()
        dst = z_half(i, far_twin)
        remote(dst, dst, gsend.at[4, i], grecv.at[4, i], {"grp": twin}).wait_recv()

    def gather_order(k):
        return jnp.where(k < 3, QKV0 + k, jnp.where(k == 3, PROJ, jnp.where(k < 8, k, k - 8)))

    zlag = 2
    gather_steps = CHUNKS + zlag

    def gather_step(k):
        @pl.when(k < CHUNKS)
        def _():
            i = gather_order(k)
            recv_y(i)
            y_to_z(i).start()
            y_to_twin(i).start()

        @pl.when(k >= zlag)
        def _():
            i = gather_order(k - zlag)
            recv_z(i)
            z_to_twin(i).start()

    def load(src, dst, k):
        return pltpu.make_async_copy(src, dst, in_sem.at[k])

    table_copy = load(table_hbm, dpk.at[pl.ds(0, table_rows)], 0)
    emb_copy = load(emb_hbm, outb, 1)

    def cot_copy(mb):
        return load(cot_hbm.at[mb], glow.at[rows(mb * seq, seq, seq)], 2 + mb)

    for i in GATHER_ORDER:
        own_across(i).start()
    for i in GATHER_ORDER:
        own_to_twin(i).start()
        own_copy(i).start()

    @pl.when(x0)
    def _():
        table_copy.start()
        emb_copy.start()

    @pl.when(x1)
    def _():
        for mb in range(2):
            cot_copy(mb).start()

    def chunk(k):
        return w[rows(k * width, width, width), :]

    step_rows = 64
    parts_of = seq // step_rows
    lane = lax.broadcasted_iota(jnp.int32, (1, 128), 1)
    low_half = (lane < HEAD).astype(F32)
    masks = (low_half.astype(BF), (1.0 - low_half).astype(BF))
    scaled = ((low_half * 0.125).astype(BF), ((1.0 - low_half) * 0.125).astype(BF))

    def seq_rows(mb):
        return rows(mb * seq, seq, seq)

    def sub_rows(mb, r):
        return rows(mb * seq + r * step_rows, step_rows, step_rows)

    def r_rows(r):
        return rows(r * step_rows, step_rows, step_rows)

    def norm_parts(v):
        center = v - jnp.mean(v, axis=-1, keepdims=True)
        spread = jnp.mean(center * center, axis=-1, keepdims=True)
        inv = lax.rsqrt(spread + EPS)
        return center * inv, inv

    pay[...] = jnp.zeros_like(pay)
    gains_acc[...] = jnp.zeros_like(gains_acc)
    for mb in range(2):
        maskc[mb] = jnp.transpose(jnp.broadcast_to(mask_ref[mb : mb + 1, :].astype(F32), (128, seq)))

    @pl.when(x0)
    def _():
        table_copy.wait()
        emb_copy.wait()
        ids = lax.broadcasted_iota(jnp.int32, (8, table_rows), 1)
        pick = lax.broadcasted_iota(jnp.int32, (8, table_rows), 0)
        want = jnp.where(pick == 0, times_ref[0], times_ref[1])
        hot = jnp.where(jnp.logical_and(pick < 2, ids == want), 1.0, 0.0).astype(BF)
        trow[...] = dot_nn(hot, dpk[pl.ds(0, table_rows), :])
        for mb in range(2):

            def make(r):
                m = maskc[mb, r_rows(r), 0:1]
                base = jnp.where(m > 0.5, vector_ref[...], outb[mb, r_rows(r), :].astype(F32))
                h[mb, r_rows(r), :] = base + trow[mb : mb + 1, :]

            loop(parts_of, make)

    def first_half(mb, t):
        @pl.when(x1)
        def _():
            h[mb] = relay[mb].astype(F32)

        def ln(r):
            xhat, _ = norm_parts(h[mb, r_rows(r), :])
            normed[sub_rows(mb, r), :] = (xhat * gains_ref[0:1, :]).astype(BF)

        loop(parts_of, ln)

        @pl.when(jnp.logical_and(x0, t == 0))
        def _():
            loop(6, gather_step)
            for i in (9, 10, 11, 8):
                near_ready(i)
                far_ready(i)

        def qkv(k):
            packed[k, seq_rows(mb), :] = dot_nn(normed[seq_rows(mb), :], chunk(QKV0 + k)).astype(BF)

        loop(3, qkv)

        @pl.when(x0)
        def _():
            gather_step(6 + 2 * t)

        def attend(j):
            cols = pl.ds(pl.multiple_of(j * 128, 128), 128)
            q2 = packed[0, seq_rows(mb), cols]
            k2 = packed[1, seq_rows(mb), cols]
            v2 = packed[2, seq_rows(mb), cols]
            total = jnp.zeros((seq, 128), F32)
            for e in range(2):
                sc = dot_nt(q2 * scaled[e], k2)
                ex = jnp.exp(sc - jnp.max(sc, axis=-1, keepdims=True))
                pr = (ex / jnp.sum(ex, axis=-1, keepdims=True)).astype(BF)
                probs[mb, 2 * j + e] = pr
                total = total + dot_nn(pr, v2 * masks[e])
            mixed[seq_rows(mb), cols] = total.astype(BF)

        loop(HEADS // 2, attend)

        @pl.when(x0)
        def _():
            gather_step(7 + 2 * t)

        mid[mb] = h[mb] + dot_nn(mixed[seq_rows(mb), :], chunk(PROJ))

        def ln_two(r):
            xhat, _ = norm_parts(mid[mb, r_rows(r), :])
            n2[sub_rows(mb, r), :] = (xhat * gains_ref[1:2, :]).astype(BF)

        loop(parts_of, ln_two)

    def mlp_up(q, mb):
        up = dot_nn(n2[seq_rows(mb), :], chunk(IN0 + q))
        sq = up * up
        t = jnp.tanh(GELU_C * up * (1.0 + 0.044715 * sq))
        hp = 0.5 * (1.0 + t)
        actv[q, seq_rows(mb), :] = (up * hp).astype(BF)
        gp[q, seq_rows(mb), :] = (hp + (0.5 * GELU_C) * up * (1.0 - t * t) * (1.0 + 0.134145 * sq)).astype(BF)

    def mlp_down(q, mb):
        acc[mb] += dot_nn(actv[q, seq_rows(mb), :], chunk(OUT0 + q))

    def second_half(base, number):
        @pl.when(x0)
        def _():
            for i in range(IN0, PROJ):
                near_ready(i)
                far_ready(i)

        def up(i):
            mlp_up(i // number, base + lax.rem(i, number))

        loop(4 * number, up)

        def init(i):
            acc[base + i] = mid[base + i]

        loop(number, init)

        def down(i):
            mlp_down(lax.rem(2 * y + i // number, 4), base + lax.rem(i, number))

        @pl.when(x0)
        def _():
            gather_step(10)
            gather_step(11)
            for i in range(IN0):
                near_ready(i)

        loop(2 * number, down)

        @pl.when(x0)
        def _():
            gather_step(12)
            gather_step(13)
            for i in range(IN0):
                far_ready(i)

        loop(2 * number, lambda i: down(2 * number + i))

        def finish(i):
            outb[base + i] = acc[base + i].astype(BF)

        loop(number, finish)

    def relay_copy(mb, part):
        r = pl.ds(part * (seq // 2), seq // 2)
        return remote(
            outb.at[mb, r], relay.at[mb, r], rsend.at[mb, part], rrecv.at[mb, part], {"section": 1 - s}
        )

    def act_copy(mb):
        return pltpu.make_async_copy(outb.at[mb], act_out.at[mb], osem.at[0, mb])

    def dx_copy(mb):
        return pltpu.make_async_copy(h.at[mb], dx_out.at[mb], osem.at[1, mb])

    def norm_back(v, gain, dy):
        xhat, inv = norm_parts(v)
        dxh = dy * gain
        m1 = jnp.mean(dxh, axis=-1, keepdims=True)
        m2 = jnp.mean(dxh * xhat, axis=-1, keepdims=True)
        return inv * (dxh - m1 - xhat * m2), jnp.sum(dy * xhat, axis=0, keepdims=True)

    def backward_mlp(mb):
        @pl.when(x0)
        def _():
            glow[seq_rows(mb), :] = relay[mb]

        @pl.when(x1)
        def _():
            cot_copy(mb).wait()

        tmp[...] = jnp.zeros_like(tmp)

        def mlp(q):
            da = dot_nt(glow[seq_rows(mb), :], chunk(OUT0 + q))
            du = (gp[q, seq_rows(mb), :].astype(F32) * da).astype(BF)
            gp[q, seq_rows(mb), :] = du
            tmp[...] += dot_nt(du, chunk(IN0 + q))

        loop(4, mlp)

        def ln_two(r):
            dx, dg = norm_back(mid[mb, r_rows(r), :], gains_ref[1:2, :], tmp[r_rows(r), :])
            dm = glow[sub_rows(mb, r), :].astype(F32) + dx
            acc[mb, r_rows(r), :] = dm
            dmlow[sub_rows(mb, r), :] = dm.astype(BF)
            gains_acc[1:2, :] += dg

        loop(parts_of, ln_two)

    def backward_attention(mb):
        do_ref[...] = dot_nt(dmlow[seq_rows(mb), :], chunk(PROJ)).astype(BF)

        def attend(j):
            cols = pl.ds(pl.multiple_of(j * 128, 128), 128)
            q2 = packed[0, seq_rows(mb), cols]
            k2 = packed[1, seq_rows(mb), cols]
            v2 = packed[2, seq_rows(mb), cols]
            do2 = do_ref[:, cols]
            dq = jnp.zeros((seq, 128), F32)
            dk = jnp.zeros((seq, 128), F32)
            dv = jnp.zeros((seq, 128), F32)
            for e in range(2):
                pr = probs[mb, 2 * j + e]
                dom = do2 * masks[e]
                dp = dot_nt(dom, v2)
                pf = pr.astype(F32)
                inner = jnp.sum(dp * pf, axis=-1, keepdims=True)
                ds = (pf * (dp - inner)).astype(BF)
                dv = dv + dot_tn(pr, dom)
                dq = dq + dot_nn(ds, k2 * scaled[e])
                dk = dk + dot_tn(ds, q2 * scaled[e])
            for k, v in enumerate((dq, dk, dv)):
                dpk[rows(k * 2 * seq + mb * seq, seq, seq), cols] = v.astype(BF)

        loop(HEADS // 2, attend)
        tmp[...] = jnp.zeros_like(tmp)

        def qkv(k):
            tmp[...] += dot_nt(dpk[rows(k * 2 * seq + mb * seq, seq, seq), :], chunk(QKV0 + k))

        loop(3, qkv)

        for part in range(2):

            def ln_one(rr):
                r = rr + part * (parts_of // 2)
                dx, dg = norm_back(h[mb, r_rows(r), :], gains_ref[0:1, :], tmp[r_rows(r), :])
                dm = acc[mb, r_rows(r), :] + dx
                outb[mb, r_rows(r), :] = dm.astype(BF)
                gains_acc[0:1, :] += dg
                m = maskc[mb, r_rows(r), 0:1]
                kept = jnp.where(jnp.logical_and(x0, m > 0.5), 0.0, dm)
                h[mb, r_rows(r), :] = kept
                pay[pl.ds(2 + mb, 1), 0:width] += jnp.sum(dm, axis=0, keepdims=True)
                pay[4:5, 0:width] += jnp.sum(dm - kept, axis=0, keepdims=True)

            loop(parts_of // 2, ln_one)

            @pl.when(x1)
            def _():
                relay_copy(mb, part).start()

        dx_copy(mb).start()

    def grad_chunk(a, b, k):
        w[rows(k * width, width, width), :] = dot_tn(a, b).astype(BF)

    def cslot(i, yy):
        return cbuf.at[yy, rows(i * quarter, quarter, quarter)]

    def to_twin(i, yy):
        q = 2 * yy + (1 - c)
        return remote(
            w.at[rows(place(i, q), quarter, quarter)], cslot(i, yy), csend.at[yy, i], crecv.at[yy, i], {"grp": twin}
        )

    def urows(u):
        return rows(u * unit, unit, unit)

    def y_send(u):
        return remote(
            cbuf.at[1 - y, urows(u)], ybuf.at[urows(u)], usend.at[0, u], urecv.at[0, u], {"grp": across}
        )

    def publish(first, number):
        def send(j):
            for yy in range(2):
                to_twin(first + j, yy).start()

        loop(number, send)

        def merge(j):
            i = first + j
            for yy in range(2):
                to_twin(i, yy).wait_recv()
            for yy in range(2):
                old = cbuf[yy, rows(i * quarter, quarter, quarter), :].astype(F32)
                mine = w[rows(place(i, 2 * yy + c), quarter, quarter), :].astype(F32)
                cbuf[yy, rows(i * quarter, quarter, quarter), :] = (old + mine).astype(BF)
            loop(per_block, lambda m: y_send(i * per_block + m).start())

        loop(number, merge)

    def mlp_grads():
        loop(4, lambda q: grad_chunk(actv[q], glow[...], OUT0 + q))
        publish(OUT0, 4)
        loop(4, lambda q: grad_chunk(n2[...], gp[q], IN0 + q))
        publish(IN0, 4)

    def attention_grads():
        grad_chunk(mixed[...], dmlow[...], PROJ)
        loop(3, lambda k: grad_chunk(normed[...], dpk[rows(k * 2 * seq, 2 * seq, 2 * seq), :], QKV0 + k))
        publish(PROJ, 4)

    def step(t):
        mb = jnp.where(x0, lax.rem(t, 2), t // 2)
        is_f = jnp.where(x0, t < 2, lax.rem(t, 2) == 0)

        @pl.when(is_f)
        def _():
            @pl.when(x1)
            def _():
                relay_copy(mb, 0).wait_recv()
                relay_copy(mb, 1).wait_recv()

            first_half(mb, t)

            @pl.when(jnp.logical_or(x1, t == 1))
            def _():
                second_half(jnp.where(x0, 0, mb), jnp.where(x0, 2, 1))

                @pl.when(x0)
                def _():
                    for b in range(2):
                        relay_copy(b, 0).start()
                        relay_copy(b, 1).start()
                        act_copy(b).start()

                @pl.when(x1)
                def _():
                    act_copy(mb).start()

        @pl.when(jnp.logical_not(is_f))
        def _():
            act_copy(mb).wait()

            @pl.when(x0)
            def _():
                for part in range(2):
                    relay_copy(mb, part).wait_send()
                    relay_copy(mb, part).wait_recv()

            backward_mlp(mb)

            @pl.when(jnp.logical_and(x0, t == 3))
            def _():
                gather_sent()
                mlp_grads()

            backward_attention(mb)

    def gather_sent():
        for i in range(CHUNKS):
            own_across(i).wait_send()
            own_to_twin(i).wait_send()
            y_to_z(i).wait_send()
            y_to_twin(i).wait_send()
            z_to_twin(i).wait_send()

    @pl.when(x1)
    def _():
        loop(gather_steps, gather_step)
        for i in range(CHUNKS):
            near_ready(i)
            far_ready(i)

    loop(4, step)

    @pl.when(x1)
    def _():
        gather_sent()
        mlp_grads()

    attention_grads()

    pay[0:2, 0:width] = gains_acc[0:2, :]
    for mb in range(2):
        pay[2 + mb : 3 + mb, pl.ds(width, 128)] = jnp.full((1, 128), times_ref[mb].astype(F32))
    for r in (0, 1, 4, 5, 6, 7):
        pay[r : r + 1, pl.ds(width, 128)] = jnp.full((1, 128), -1.0, F32)

    def add_rows(dst, dst_rows, a, b):
        dst[dst_rows, :] = (a.astype(F32) + b.astype(F32)).astype(BF)

    if nz == 4:
        end = jnp.logical_or(d == 0, d == 3)
        inner = jnp.logical_not(end)
        slots, pay_in = extra

        def slot_copy(k):
            first, size, peer = (
                (d * 4 + g, 1, {"grp": twin}),
                (d * 4 + 2 * y, 2, {"grp": across}),
                (d * 4, 4, {"dp": zpair}),
                ((d // 2) * 8, 8, {"dp": zfar}),
            )[k]
            ref = slots.at[rows(first * 8, size * 8, 8)]
            return remote(ref, ref, psend.at[1 + k], precv.at[1 + k], peer)

        def slot_wait(k):
            first, size, peer = (
                (d * 4 + twin, 1, {"grp": twin}),
                (d * 4 + 2 * (1 - y), 2, {"grp": across}),
                (zpair * 4, 4, {"dp": zpair}),
                ((1 - d // 2) * 8, 8, {"dp": zfar}),
            )[k]
            ref = slots.at[rows(first * 8, size * 8, 8)]
            remote(ref, ref, psend.at[1 + k], precv.at[1 + k], peer).wait_recv()

        pay_copy = remote(pay, pay_in, psend.at[0], precv.at[0], {"section": 1 - s})

        @pl.when(x0)
        def _():
            pay_copy.start()

        def small_start():
            @pl.when(x1)
            def _():
                pay_copy.wait_recv()
                pay[2:8, :] = pay_in[2:8, :]

            slots[rows((d * 4 + g) * 8, 8, 8), :] = pay[...]
            slot_copy(0).start()

        def small_next(k):
            slot_wait(k)
            slot_copy(k + 1).start()

        def small_end():
            slot_wait(3)
            total = slots[0:8, :]
            for k in range(1, 16):
                total = total + slots[k * 8 : k * 8 + 8, :]
            shard = s * 4 + g
            small_out[0:8, :] = pltpu.roll(total[:, 0:width], lax.rem(width - quarter * g, width), 1)
            small_out[8:16, :] = pltpu.roll(
                total[:, 0:width], lax.rem(width - (width // 8) * shard, width), 1
            )
            base = shard * (table_rows // 8)
            ids = (base + lax.broadcasted_iota(jnp.int32, (128, 128), 1)).astype(F32)
            pick = jnp.where(slots[:, pl.ds(width, 128)] == ids, 1.0, 0.0)
            table_out[...] = lax.dot_general(
                pick,
                slots[:, 0:width],
                (((0,), (0,)), ((), ())),
                precision=lax.Precision.HIGHEST,
                preferred_element_type=F32,
            )

        def end_to_inner(u):
            return remote(
                ybuf.at[urows(u)], z1.at[urows(u)], usend.at[1, u], urecv.at[1, u], {"dp": zpair}
            )

        def inner_swap(u):
            return remote(
                z1.at[urows(u)], z2.at[urows(u)], usend.at[2, u], urecv.at[2, u], {"dp": 3 - d}
            )

        def inner_to_end(u):
            return remote(
                z2.at[urows(u)], z1.at[urows(u)], usend.at[1, u], urecv.at[1, u], {"dp": zpair}
            )

        def out_end(u):
            return pltpu.make_async_copy(z1.at[urows(u)], grad_out.at[urows(u)], usend.at[2, u])

        def out_inner(u):
            return pltpu.make_async_copy(z2.at[urows(u)], grad_out.at[urows(u)], urecv.at[3, u])

        lag3, lag4, lag5 = 2, 4, 6
        first_small = 12

        def tick(t):
            u2, u3, u4, u5 = t, t - lag3, t - lag4, t - lag5

            @pl.when(u2 < units)
            def _():
                y_send(u2).wait_recv()
                add_rows(ybuf, urows(u2), cbuf[y, urows(u2), :], ybuf[urows(u2), :])

                @pl.when(end)
                def _():
                    end_to_inner(u2).start()

            @pl.when(jnp.logical_and(inner, jnp.logical_and(u3 >= 0, u3 < units)))
            def _():
                end_to_inner(u3).wait_recv()
                add_rows(z1, urows(u3), ybuf[urows(u3), :], z1[urows(u3), :])
                inner_swap(u3).start()

            @pl.when(jnp.logical_and(inner, jnp.logical_and(u4 >= 0, u4 < units)))
            def _():
                inner_swap(u4).wait_recv()
                add_rows(z2, urows(u4), z1[urows(u4), :], z2[urows(u4), :])
                inner_to_end(u4).start()
                out_inner(u4).start()

            @pl.when(jnp.logical_and(end, jnp.logical_and(u5 >= 0, u5 < units)))
            def _():
                inner_to_end(u5).wait_recv()
                out_end(u5).start()

            pl.when(t == first_small)(small_start)
            for k in range(3):
                pl.when(t == first_small + 2 + 2 * k)(functools.partial(small_next, k))
            pl.when(t == first_small + 8)(small_end)

        loop(units + lag5, tick)

        def drain(u):
            y_send(u).wait_send()

            @pl.when(end)
            def _():
                end_to_inner(u).wait_send()
                out_end(u).wait()

            @pl.when(inner)
            def _():
                inner_swap(u).wait_send()
                inner_to_end(u).wait_send()
                out_inner(u).wait()

        loop(units, drain)

        @pl.when(x0)
        def _():
            pay_copy.wait_send()

        for k in range(4):
            slot_copy(k).wait_send()
    else:
        small_out[...] = pay[...]
        table_out[...] = jnp.zeros_like(table_out)

        def out_sum(u):
            return pltpu.make_async_copy(ybuf.at[urows(u)], grad_out.at[urows(u)], usend.at[1, u])

        def tick(u):
            y_send(u).wait_recv()
            add_rows(ybuf, urows(u), cbuf[y, urows(u), :], ybuf[urows(u), :])
            out_sum(u).start()

        loop(units, tick)

        def drain(u):
            y_send(u).wait_send()
            out_sum(u).wait()

        loop(units, drain)

    def sent(i):
        for yy in range(2):
            to_twin(i, yy).wait_send()

    loop(CHUNKS, sent)
    for mb in range(2):
        dx_copy(mb).wait()

        @pl.when(x1)
        def _():
            for part in range(2):
                relay_copy(mb, part).wait_send()


def run_mega(timesteps, mask_flags, vector, gains, emb, cot, table, wq, wp, wi, wo, nz):
    count, seq, width = emb.shape
    quarter = wp.shape[0]
    unit = quarter // 2
    units = CHUNKS * quarter // unit
    tokens = count * seq
    assert count == 2 and quarter * 4 == width and wi.shape[1] == 4 * width and wo.shape[0] == width
    vmem = pl.BlockSpec(memory_space=pltpu.VMEM)
    smem = pl.BlockSpec(memory_space=pltpu.SMEM)
    hbm = pl.BlockSpec(memory_space=pl.ANY)
    dma = pltpu.SemaphoreType.DMA
    small = (16, width) if nz == 4 else (8, width + 128)
    extra = [pltpu.VMEM((nz * 4 * 8, width + 128), F32), pltpu.VMEM((8, width + 128), F32)]
    return pl.pallas_call(
        functools.partial(mega, (count, seq, width, nz, unit)),
        out_shape=(
            jax.ShapeDtypeStruct((count, seq, width), BF),
            jax.ShapeDtypeStruct((count, seq, width), F32),
            jax.ShapeDtypeStruct((CHUNKS * quarter, width), BF),
            jax.ShapeDtypeStruct(small, F32),
            jax.ShapeDtypeStruct((128, width), F32),
        ),
        in_specs=[smem, vmem, vmem, vmem] + [hbm] * 7,
        out_specs=(hbm, hbm, hbm, vmem, vmem),
        scratch_shapes=[
            pltpu.VMEM((CHUNKS * width, width), BF),
            pltpu.VMEM((count, seq, width), F32),
            pltpu.VMEM((count, seq, width), F32),
            pltpu.VMEM((count, seq, width), F32),
            pltpu.VMEM((seq, width), F32),
            pltpu.VMEM((tokens, width), BF),
            pltpu.VMEM((tokens, width), BF),
            pltpu.VMEM((tokens, width), BF),
            pltpu.VMEM((4, tokens, width), BF),
            pltpu.VMEM((4, tokens, width), BF),
            pltpu.VMEM((3, tokens, width), BF),
            pltpu.VMEM((count, HEADS, seq, seq), BF),
            pltpu.VMEM((tokens, width), BF),
            pltpu.VMEM((tokens, width), BF),
            pltpu.VMEM((3 * tokens, width), BF),
            pltpu.VMEM((seq, width), BF),
            pltpu.VMEM((count, seq, width), BF),
            pltpu.VMEM((count, seq, width), BF),
            pltpu.VMEM((count, seq, 128), F32),
            pltpu.VMEM((8, width), F32),
            pltpu.VMEM((8, width + 128), F32),
            pltpu.VMEM((8, width), F32),
            pltpu.VMEM((2, CHUNKS * quarter, width), BF),
            pltpu.VMEM((CHUNKS * quarter, width), BF),
            pltpu.VMEM((CHUNKS * quarter, width), BF),
            pltpu.VMEM((CHUNKS * quarter, width), BF),
            dma((4,)),
            dma((CHUNKS,)),
            dma((5, CHUNKS)),
            dma((5, CHUNKS)),
            dma((2, 2)),
            dma((2, 2)),
            dma((2, CHUNKS)),
            dma((2, CHUNKS)),
            dma((3, units)),
            dma((4, units)),
            dma((5,)),
            dma((5,)),
            dma((2, 2)),
        ]
        + (extra if nz == 4 else []),
        compiler_params=pltpu.CompilerParams(
            collective_id=0, has_side_effects=True, vmem_limit_bytes=67043328
        ),
        name="relay_layers",
    )(timesteps, mask_flags, vector, gains, emb, cot, table, wq, wp, wi, wo)


def small_sums(sizes, small, timesteps, rows_count, quarter):
    ns, ng, nz = sizes
    width = quarter * 4
    section, member = lax.axis_index("section"), lax.axis_index("grp")
    every = lax.all_gather(small, ("section", "grp", "dp"), axis=0, tiled=False)
    per_plane = every.reshape(ns, ng * nz, 8, width + 128)
    mine = lax.dynamic_index_in_dim(per_plane, section, 0, keepdims=False)[:, :2, :width].sum(axis=0)
    grad_gains = lax.dynamic_slice(mine, (0, member * quarter), (2, quarter))
    shard = section * ng + member
    here = rows_count // (ns * ng)
    ids = (shard * here + jnp.arange(here)).astype(F32)
    stamp = per_plane[0, :, :, width].reshape(-1)
    pick = (ids[:, None] == stamp[None, :]).astype(F32)
    grad_table = jnp.dot(pick, per_plane[0, :, :, :width].reshape(-1, width), precision=lax.Precision.HIGHEST)
    mask_here = width // (ns * ng)
    grad_mask = lax.dynamic_slice(per_plane[0, :, 4, :width].sum(axis=0), (shard * mask_here,), (mask_here,))
    return grad_gains, grad_table, grad_mask


def on_device(
    sizes,
    embeddings,
    mask_flags,
    timesteps,
    time_table,
    mask_vector,
    attn_qkv,
    attn_out,
    mlp_in,
    mlp_out,
    norm_gains,
    cotangent,
):
    ns, ng, nz = sizes
    rows_count, width = time_table.shape
    activations, dx, grads, small, table = run_mega(
        timesteps,
        mask_flags,
        mask_vector.astype(F32)[None],
        norm_gains[0],
        embeddings,
        cotangent,
        time_table,
        attn_qkv[0],
        attn_out[0],
        mlp_in[0],
        mlp_out[0],
        nz,
    )
    quarter = attn_out.shape[1]
    if nz == 4:
        grad_gains = small[:2, :quarter]
        grad_table = table[: rows_count // (ns * ng)]
        grad_mask = small[12, : width // (ns * ng)]
    else:
        grads = lax.psum(grads, "dp")
        grad_gains, grad_table, grad_mask = small_sums(sizes, small, timesteps, rows_count, quarter)

    def blocks(first, n):
        return jnp.concatenate(
            [grads[(first + j) * quarter : (first + j + 1) * quarter] for j in range(n)], axis=1
        ).astype(F32)

    return (
        activations[None],
        dx[None],
        blocks(QKV0, 3)[None],
        blocks(PROJ, 1)[None],
        blocks(IN0, 4)[None],
        grads[: 4 * quarter].astype(F32)[None],
        grad_gains[None],
        grad_table,
        grad_mask,
    )


def solution(mesh):
    sizes = (mesh.shape["section"], mesh.shape["grp"], mesh.shape["dp"])
    placed = (
        P(("grp", "dp"), None, None),
        P(("grp", "dp"), None),
        P(("grp", "dp")),
        P(),
        P(),
        P("section", "grp", None),
        P("section", "grp", None),
        P("section", "grp", None),
        P("section", "grp", None),
        P("section", None, None),
        P(("grp", "dp"), None, None),
    )
    return jax.shard_map(
        functools.partial(on_device, sizes),
        mesh=mesh,
        in_specs=placed,
        out_specs=(
            P("section", ("grp", "dp"), None, None),
            P("section", ("grp", "dp"), None, None),
            P("section", "grp", None),
            P("section", "grp", None),
            P("section", "grp", None),
            P("section", "grp", None),
            P("section", None, "grp"),
            P(("section", "grp"), None),
            P(("section", "grp")),
        ),
        check_vma=False,
    )
```

```python
import functools
import math

import jax
import jax.numpy as jnp
from jax import lax
from jax.experimental import pallas as pl
from jax.experimental.pallas import tpu as pltpu
from jax.sharding import PartitionSpec as P

HEADS = 12
HEAD = 64
BF = jnp.bfloat16
F32 = jnp.float32
MESH = pl.DeviceIdType.MESH
EPS = 1e-05
GELU_C = math.sqrt(2.0 / math.pi)

OUT0, IN0, PROJ, QKV0, CHUNKS = 0, 4, 8, 9, 12
GATHER_ORDER = (9, 10, 11, 8, 4, 5, 6, 7, 0, 1, 2, 3)


def dot_nn(a, b):
    return lax.dot_general(a, b, (((1,), (0,)), ((), ())), preferred_element_type=F32)


def dot_nt(a, b):
    return lax.dot_general(a, b, (((1,), (1,)), ((), ())), preferred_element_type=F32)


def dot_tn(a, b):
    return lax.dot_general(a, b, (((0,), (0,)), ((), ())), preferred_element_type=F32)


def loop(n, body, first=0):
    lax.fori_loop(first, n, lambda i, c: (body(i), c)[1], 0)


def unrolled(n, body):
    for i in range(n):
        body(i)


def mega(
    cfg,
    times_ref,
    mask_ref,
    vector_ref,
    gains_ref,
    emb_hbm,
    cot_hbm,
    table_hbm,
    wq_hbm,
    wp_hbm,
    wi_hbm,
    wo_hbm,
    act_out,
    dx_out,
    grad_out,
    small_out,
    table_out,
    w,
    h,
    mid,
    acc,
    tmp,
    inv_sum,
    normed,
    mixed,
    n2,
    actv,
    gp,
    packed,
    probs,
    glow,
    dmlow,
    dpk,
    do_ref,
    outb,
    relay,
    maskc,
    trow,
    pay,
    gains_acc,
    cbuf,
    ybuf,
    z1,
    z2,
    in_sem,
    own_sem,
    gsend,
    grecv,
    rsend,
    rrecv,
    csend,
    crecv,
    usend,
    urecv,
    psend,
    precv,
    osem,
    *extra,
):
    count, seq, width, nz, unit = cfg
    quarter = width // 4
    units = CHUNKS * quarter // unit
    per_block = quarter // unit
    table_rows = table_hbm.shape[0]
    s = lax.axis_index("section")
    g = lax.axis_index("grp")
    d = lax.axis_index("dp")
    x0 = s == 0
    x1 = jnp.logical_not(x0)
    c = lax.rem(g, 2)
    y = g // 2
    twin = g + 1 - 2 * c
    across = lax.rem(g + 2, 4)
    zpair = d + 1 - 2 * lax.rem(d, 2)
    zfar = lax.rem(d + 2, 4)
    half = lax.rem(d, 2)

    peers = [{"section": 1 - s}, {"grp": twin}, {"grp": across}, {"dp": zpair}]
    if nz == 4:
        peers += [{"dp": 3 - d}, {"dp": zfar}]
    barrier = pltpu.get_barrier_semaphore()
    for peer in peers:
        pl.semaphore_signal(barrier, inc=1, device_id=peer, device_id_type=MESH)
    pl.semaphore_wait(barrier, len(peers))

    def remote(src, dst, send, recv, peer):
        return pltpu.make_async_remote_copy(
            src_ref=src, dst_ref=dst, send_sem=send, recv_sem=recv, device_id=peer, device_id_type=MESH
        )

    def rows(start, size, by):
        return pl.ds(pl.multiple_of(start, by), size)

    def place(i, q):
        return jnp.where(i < IN0, q * width + quarter * i, i * width + quarter * q)

    def source(i):
        if i < IN0:
            return wo_hbm.at[pl.ds(i * quarter, quarter)]
        if i < PROJ:
            return wi_hbm.at[:, pl.ds((i - IN0) * width, width)]
        if i == PROJ:
            return wp_hbm
        return wq_hbm.at[:, pl.ds((i - QKV0) * width, width)]

    hq = quarter // 2
    far = across
    far_twin = lax.rem(twin + 2, 4)

    def own_copy(i):
        return pltpu.make_async_copy(source(i), w.at[rows(place(i, g), quarter, hq)], own_sem.at[i])

    def own_to_twin(i):
        return remote(source(i), w.at[rows(place(i, g), quarter, hq)], gsend.at[0, i], grecv.at[0, i], {"grp": twin})

    def own_across(i):
        return remote(
            source(i).at[rows(half * hq, hq, hq)],
            w.at[rows(place(i, g) + half * hq, hq, hq)],
            gsend.at[1, i],
            grecv.at[1, i],
            {"grp": across},
        )

    def y_half(i, q):
        return w.at[rows(place(i, q) + half * hq, hq, hq)]

    def z_half(i, q):
        return w.at[rows(place(i, q) + (1 - half) * hq, hq, hq)]

    def y_to_z(i):
        return remote(y_half(i, far), y_half(i, far), gsend.at[2, i], grecv.at[2, i], {"dp": zpair})

    def y_to_twin(i):
        return remote(y_half(i, far), y_half(i, far), gsend.at[3, i], grecv.at[3, i], {"grp": twin})

    def z_to_twin(i):
        return remote(z_half(i, far), z_half(i, far), gsend.at[4, i], grecv.at[4, i], {"grp": twin})

    def recv_y(i):
        remote(y_half(i, far), y_half(i, far), gsend.at[1, i], grecv.at[1, i], {"grp": across}).wait_recv()

    def recv_z(i):
        remote(z_half(i, far), z_half(i, far), gsend.at[2, i], grecv.at[2, i], {"dp": zpair}).wait_recv()

    def near_ready(i):
        dst = w.at[rows(place(i, twin), quarter, hq)]
        remote(dst, dst, gsend.at[0, i], grecv.at[0, i], {"grp": twin}).wait_recv()
        own_copy(i).wait()

    def far_ready(i):
        dst = y_half(i, far_twin)
        remote(dst, dst, gsend.at[3, i], grecv.at[3, i], {"grp": twin}).wait_recv()
        dst = z_half(i, far_twin)
        remote(dst, dst, gsend.at[4, i], grecv.at[4, i], {"grp": twin}).wait_recv()

    def gather_order(k):
        return jnp.where(k < 3, QKV0 + k, jnp.where(k == 3, PROJ, jnp.where(k < 8, k, k - 8)))

    zlag = 2
    gather_steps = CHUNKS + zlag

    def gather_step(k):
        @pl.when(k < CHUNKS)
        def _():
            i = gather_order(k)
            recv_y(i)
            y_to_z(i).start()
            y_to_twin(i).start()

        @pl.when(k >= zlag)
        def _():
            i = gather_order(k - zlag)
            recv_z(i)
            z_to_twin(i).start()

    def load(src, dst, k):
        return pltpu.make_async_copy(src, dst, in_sem.at[k])

    table_copy = load(table_hbm, dpk.at[pl.ds(0, table_rows)], 0)
    emb_copy = load(emb_hbm, outb, 1)

    def cot_copy(mb):
        return load(cot_hbm.at[mb], glow.at[rows(mb * seq, seq, seq)], 2 + mb)

    for i in GATHER_ORDER:
        own_across(i).start()
    for i in GATHER_ORDER:
        own_to_twin(i).start()
        own_copy(i).start()

    @pl.when(x0)
    def _():
        table_copy.start()
        emb_copy.start()

    @pl.when(x1)
    def _():
        for mb in range(2):
            cot_copy(mb).start()

    def chunk(k):
        return w[rows(k * width, width, width), :]

    step_rows = 32
    parts_of = seq // step_rows
    lane = lax.broadcasted_iota(jnp.int32, (1, 128), 1)
    low_lane = lax.broadcasted_iota(jnp.int32, (seq, 128), 1) < HEAD
    low_half = (lane < HEAD).astype(F32)
    masks = (low_half.astype(BF), (1.0 - low_half).astype(BF))
    scaled = ((low_half * 0.125).astype(BF), ((1.0 - low_half) * 0.125).astype(BF))

    def seq_rows(mb):
        return rows(mb * seq, seq, seq)

    def sub_rows(mb, r):
        return rows(mb * seq + r * step_rows, step_rows, step_rows)

    def r_rows(r):
        return rows(r * step_rows, step_rows, step_rows)

    def norm_parts(v):
        center = v - jnp.mean(v, axis=-1, keepdims=True)
        spread = jnp.mean(center * center, axis=-1, keepdims=True)
        inv = lax.rsqrt(spread + EPS)
        return center * inv, inv

    @pl.when(x1)
    def _():
        loop(gather_steps, gather_step)
        for i in range(CHUNKS):
            near_ready(i)
            far_ready(i)

    pay[...] = jnp.zeros_like(pay)
    gains_acc[...] = jnp.zeros_like(gains_acc)
    for mb in range(2):
        maskc[mb] = jnp.transpose(jnp.broadcast_to(mask_ref[mb : mb + 1, :].astype(F32), (128, seq)))

    @pl.when(x0)
    def _():
        table_copy.wait()
        emb_copy.wait()
        ids = lax.broadcasted_iota(jnp.int32, (8, table_rows), 1)
        pick = lax.broadcasted_iota(jnp.int32, (8, table_rows), 0)
        want = jnp.where(pick == 0, times_ref[0], times_ref[1])
        hot = jnp.where(jnp.logical_and(pick < 2, ids == want), 1.0, 0.0).astype(BF)
        trow[...] = dot_nn(hot, dpk[pl.ds(0, table_rows), :])
        for mb in range(2):

            def make(r):
                m = maskc[mb, r_rows(r), 0:1]
                base = jnp.where(m > 0.5, vector_ref[...], outb[mb, r_rows(r), :].astype(F32))
                h[mb, r_rows(r), :] = base + trow[mb : mb + 1, :]

            loop(parts_of, make)

    def first_half(mb, t):
        @pl.when(x1)
        def _():
            h[mb] = relay[mb].astype(F32)

        def ln(r):
            xhat, _ = norm_parts(h[mb, r_rows(r), :])
            normed[sub_rows(mb, r), :] = (xhat * gains_ref[0:1, :]).astype(BF)

        unrolled(parts_of, ln)

        @pl.when(jnp.logical_and(x0, t == 0))
        def _():
            loop(6, gather_step)
            for i in (9, 10, 11, 8):
                near_ready(i)
                far_ready(i)

        def qkv(k):
            packed[k, seq_rows(mb), :] = dot_nn(normed[seq_rows(mb), :], chunk(QKV0 + k)).astype(BF)

        loop(3, qkv)

        @pl.when(x0)
        def _():
            gather_step(6 + 2 * t)

        def attend(j):
            cols = pl.ds(j * 128, 128)
            q2 = packed[0, seq_rows(mb), cols]
            k2 = packed[1, seq_rows(mb), cols]
            v2 = packed[2, seq_rows(mb), cols]
            got = []
            for e in range(2):
                sc = dot_nt(q2 * scaled[e], k2)
                ex = jnp.exp(sc - jnp.max(sc, axis=-1, keepdims=True)).astype(BF)
                probs[mb, 2 * j + e] = ex
                got.append(dot_nn(ex, v2 * masks[e] + masks[1 - e]))
            inv = 1.0 / pltpu.roll(jnp.where(low_lane, got[1], got[0]), HEAD, 1)
            inv_sum[mb, :, cols] = inv
            mixed[seq_rows(mb), cols] = (jnp.where(low_lane, got[0], got[1]) * inv).astype(BF)

        unrolled(HEADS // 2, attend)

        @pl.when(x0)
        def _():
            gather_step(7 + 2 * t)

        mid[mb] = h[mb] + dot_nn(mixed[seq_rows(mb), :], chunk(PROJ))

        def ln_two(r):
            xhat, _ = norm_parts(mid[mb, r_rows(r), :])
            n2[sub_rows(mb, r), :] = (xhat * gains_ref[1:2, :]).astype(BF)

        unrolled(parts_of, ln_two)

    def mlp_up(q, mb):
        up = dot_nn(n2[seq_rows(mb), :], chunk(IN0 + q))
        sq = up * up
        hp = 0.5 + 0.5 * jnp.tanh(up * (GELU_C + (GELU_C * 0.044715) * sq))
        act = up * hp
        actv[q, seq_rows(mb), :] = act.astype(BF)
        gp[q, seq_rows(mb), :] = (
            hp + act * ((1.0 - hp) * (2.0 * GELU_C + (2.0 * GELU_C * 0.134145) * sq))
        ).astype(BF)

    def mlp_down(q, mb):
        acc[mb] += dot_nn(actv[q, seq_rows(mb), :], chunk(OUT0 + q))

    def second_half(base, number):
        @pl.when(x0)
        def _():
            for i in range(IN0, PROJ):
                near_ready(i)
                far_ready(i)

        def up(i):
            mlp_up(i // number, base + lax.rem(i, number))

            @pl.when(jnp.logical_and(x0, jnp.logical_or(i == 2, i == 5)))
            def _():
                gather_step(10 + i // 4)

        loop(4 * number, up)

        def init(i):
            acc[base + i] = mid[base + i]

        loop(number, init)

        def down(i):
            mlp_down(lax.rem(2 * y + i // number, 4), base + lax.rem(i, number))

        @pl.when(x0)
        def _():
            for i in range(IN0):
                near_ready(i)

        loop(2 * number, down)

        @pl.when(x0)
        def _():
            gather_step(12)
            gather_step(13)
            for i in range(IN0):
                far_ready(i)

        loop(2 * number, lambda i: down(2 * number + i))

        def finish(i):
            outb[base + i] = acc[base + i].astype(BF)

        loop(number, finish)

    def relay_copy(mb, part):
        r = pl.ds(part * (seq // 2), seq // 2)
        return remote(
            outb.at[mb, r], relay.at[mb, r], rsend.at[mb, part], rrecv.at[mb, part], {"section": 1 - s}
        )

    def act_copy(mb):
        return pltpu.make_async_copy(outb.at[mb], act_out.at[mb], osem.at[0, mb])

    def dx_copy(mb):
        return pltpu.make_async_copy(h.at[mb], dx_out.at[mb], osem.at[1, mb])

    def norm_back(v, gain, dy):
        xhat, inv = norm_parts(v)
        dxh = dy * gain
        m1 = jnp.mean(dxh, axis=-1, keepdims=True)
        m2 = jnp.mean(dxh * xhat, axis=-1, keepdims=True)
        return inv * (dxh - m1 - xhat * m2), jnp.sum(dy * xhat, axis=0, keepdims=True)

    def backward_mlp(mb, t):
        @pl.when(x0)
        def _():
            glow[seq_rows(mb), :] = relay[mb]

        @pl.when(x1)
        def _():
            cot_copy(mb).wait()

        tmp[...] = jnp.zeros_like(tmp)

        def mlp(q):
            da = dot_nt(glow[seq_rows(mb), :], chunk(OUT0 + q))
            du = (gp[q, seq_rows(mb), :].astype(F32) * da).astype(BF)
            gp[q, seq_rows(mb), :] = du
            tmp[...] += dot_nt(du, chunk(IN0 + q))

        def mlp_and_out(k):
            q = out_order(k)
            mlp(q)
            out_terms(k)

        last = jnp.logical_and(x0, t == 3)
        pl.when(last)(lambda: loop(4, mlp_and_out))
        pl.when(jnp.logical_not(last))(lambda: loop(4, mlp))

        def ln_two(r):
            dx, dg = norm_back(mid[mb, r_rows(r), :], gains_ref[1:2, :], tmp[r_rows(r), :])
            dm = glow[sub_rows(mb, r), :].astype(F32) + dx
            mid[mb, r_rows(r), :] = dm
            dmlow[sub_rows(mb, r), :] = dm.astype(BF)
            gains_acc[1:2, :] += dg

        unrolled(parts_of, ln_two)

    def backward_attention(mb, t):
        do_ref[...] = (dot_nt(dmlow[seq_rows(mb), :], chunk(PROJ)) * inv_sum[mb]).astype(BF)

        def attend(j):
            cols = pl.ds(j * 128, 128)
            q2 = packed[0, seq_rows(mb), cols]
            k2 = packed[1, seq_rows(mb), cols]
            v2 = packed[2, seq_rows(mb), cols]
            do2 = do_ref[:, cols]
            weighed = do2.astype(F32) * mixed[seq_rows(mb), cols].astype(F32)
            dq = jnp.zeros((seq, 128), F32)
            dk = jnp.zeros((seq, 128), F32)
            dv = jnp.zeros((seq, 128), F32)
            for e in range(2):
                ex = probs[mb, 2 * j + e]
                dom = do2 * masks[e]
                inner = jnp.sum(jnp.where(low_lane if e == 0 else jnp.logical_not(low_lane), weighed, 0.0), axis=-1, keepdims=True)
                ds = (ex.astype(F32) * (dot_nt(dom, v2) - inner)).astype(BF)
                dv = dv + dot_tn(ex, dom)
                dq = dq + dot_nn(ds, k2 * scaled[e])
                dk = dk + dot_tn(ds, q2 * scaled[e])
            for k, v in enumerate((dq, dk, dv)):
                dpk[rows(k * 2 * seq + mb * seq, seq, seq), cols] = v.astype(BF)

        for j in range(HEADS // 2):
            attend(j)
            if j % 3 == 2:
                early_ticks(t, j // 3)
        tmp[...] = jnp.zeros_like(tmp)

        def qkv(k):
            tmp[...] += dot_nt(dpk[rows(k * 2 * seq + mb * seq, seq, seq), :], chunk(QKV0 + k))

        loop(3, qkv)

        for part in range(2):

            def ln_one(rr):
                r = rr + part * (parts_of // 2)
                dx, dg = norm_back(h[mb, r_rows(r), :], gains_ref[0:1, :], tmp[r_rows(r), :])
                dm = mid[mb, r_rows(r), :] + dx
                outb[mb, r_rows(r), :] = dm.astype(BF)
                gains_acc[0:1, :] += dg
                m = maskc[mb, r_rows(r), 0:1]
                kept = jnp.where(jnp.logical_and(x0, m > 0.5), 0.0, dm)
                h[mb, r_rows(r), :] = kept
                pay[pl.ds(2 + mb, 1), 0:width] += jnp.sum(dm, axis=0, keepdims=True)
                pay[4:5, 0:width] += jnp.sum(dm - kept, axis=0, keepdims=True)

            unrolled(parts_of // 2, ln_one)

            @pl.when(x1)
            def _():
                relay_copy(mb, part).start()

        dx_copy(mb).start()

    def grad_chunk(a, b, k):
        w[rows(k * width, width, width), :] = dot_tn(a, b).astype(BF)

    def cslot(i, yy):
        return cbuf.at[yy, rows(i * quarter, quarter, quarter)]

    def to_twin(i, yy):
        q = 2 * yy + (1 - c)
        return remote(
            w.at[rows(place(i, q), quarter, quarter)], cslot(i, yy), csend.at[yy, i], crecv.at[yy, i], {"grp": twin}
        )

    def urows(u):
        return rows(u * unit, unit, unit)

    def y_send(u):
        return remote(
            cbuf.at[1 - y, urows(u)], ybuf.at[urows(u)], usend.at[0, u], urecv.at[0, u], {"grp": across}
        )

    def merge_far(i):
        to_twin(i, 1 - y).wait_recv()
        part = rows(i * quarter, quarter, quarter)
        mine = w[rows(place(i, 2 * (1 - y) + c), quarter, quarter), :].astype(F32)
        cbuf[1 - y, part, :] = (cbuf[1 - y, part, :].astype(F32) + mine).astype(BF)

    ahead = 6

    def send_across(u):
        pl.when(lax.rem(u, per_block) == 0)(lambda: merge_far(u // per_block))
        y_send(u).start()

    def out_order(k):
        side = jnp.where(k < 2, 1 - y, y)
        return 2 * side + jnp.where(lax.rem(k, 2) == 0, 1 - c, c)

    def out_terms(k):
        q = out_order(k)
        grad_chunk(actv[q], glow[...], OUT0 + q)

        @pl.when(lax.rem(k, 2) == 0)
        def _():
            loop(4, lambda i: to_twin(i, jnp.where(k == 0, 1 - y, y)).start())

        @pl.when(k == 1)
        def _():
            loop(ahead, send_across)

    def other_terms(i, a, b):
        grad_chunk(a, b, i)
        to_twin(i, 1 - y).start()
        to_twin(i, y).start()

    def in_terms():
        loop(4, lambda q: other_terms(IN0 + q, n2[...], gp[q]))

    def attention_terms():
        other_terms(PROJ, mixed[...], dmlow[...])
        loop(3, lambda k: other_terms(QKV0 + k, normed[...], dpk[rows(k * 2 * seq, 2 * seq, 2 * seq), :]))

    def add_rows(dst, dst_rows, *terms):
        dst[dst_rows, :] = functools.reduce(jnp.add, [a.astype(F32) for a in terms]).astype(BF)

    def sum_across(u):
        i = u // per_block
        pl.when(lax.rem(u, per_block) == 0)(lambda: to_twin(i, y).wait_recv())
        y_send(u).wait_recv()
        mine = w[rows(place(i, g) + lax.rem(u, per_block) * unit, unit, unit), :]
        add_rows(ybuf, urows(u), cbuf[y, urows(u), :], mine, ybuf[urows(u), :])

    early = 4
    early_count = 2 * early
    if nz == 4:
        end = jnp.logical_or(d == 0, d == 3)
        inner = jnp.logical_not(end)
        slots, pay_in = extra

        def slot_copy(k):
            first, size, peer = (
                (d * 4 + g, 1, {"grp": twin}),
                (d * 4 + 2 * y, 2, {"grp": across}),
                (d * 4, 4, {"dp": zpair}),
                ((d // 2) * 8, 8, {"dp": zfar}),
            )[k]
            ref = slots.at[rows(first * 8, size * 8, 8)]
            return remote(ref, ref, psend.at[1 + k], precv.at[1 + k], peer)

        def slot_wait(k):
            first, size, peer = (
                (d * 4 + twin, 1, {"grp": twin}),
                (d * 4 + 2 * (1 - y), 2, {"grp": across}),
                (zpair * 4, 4, {"dp": zpair}),
                ((1 - d // 2) * 8, 8, {"dp": zfar}),
            )[k]
            ref = slots.at[rows(first * 8, size * 8, 8)]
            remote(ref, ref, psend.at[1 + k], precv.at[1 + k], peer).wait_recv()

        pay_copy = remote(pay, pay_in, psend.at[0], precv.at[0], {"section": 1 - s})

        def small_start():
            @pl.when(x1)
            def _():
                pay_copy.wait_recv()
                pay[2:8, :] = pay_in[2:8, :]

            slots[rows((d * 4 + g) * 8, 8, 8), :] = pay[...]
            slot_copy(0).start()

        def small_next(k):
            slot_wait(k)
            slot_copy(k + 1).start()

        def small_end():
            slot_wait(3)
            total = slots[0:8, :]
            for k in range(1, 16):
                total = total + slots[k * 8 : k * 8 + 8, :]
            shard = s * 4 + g
            small_out[0:8, :] = pltpu.roll(total[:, 0:width], lax.rem(width - quarter * g, width), 1)
            small_out[8:16, :] = pltpu.roll(
                total[:, 0:width], lax.rem(width - (width // 8) * shard, width), 1
            )
            base = shard * (table_rows // 8)
            ids = (base + lax.broadcasted_iota(jnp.int32, (128, 128), 1)).astype(F32)
            pick = jnp.where(slots[:, pl.ds(width, 128)] == ids, 1.0, 0.0).astype(BF)
            rest = slots[:, 0:width]
            found = jnp.zeros((128, width), F32)
            for _ in range(3):
                part = rest.astype(BF)
                found = found + dot_tn(pick, part)
                rest = rest - part.astype(F32)
            table_out[...] = found

        def end_to_inner(u):
            return remote(
                ybuf.at[urows(u)], z1.at[urows(u)], usend.at[1, u], urecv.at[1, u], {"dp": zpair}
            )

        def inner_swap(u):
            return remote(
                z1.at[urows(u)], z2.at[urows(u)], usend.at[2, u], urecv.at[2, u], {"dp": 3 - d}
            )

        def inner_to_end(u):
            return remote(
                z2.at[urows(u)], z1.at[urows(u)], usend.at[1, u], urecv.at[1, u], {"dp": zpair}
            )

        def out_end(u):
            return pltpu.make_async_copy(z1.at[urows(u)], grad_out.at[urows(u)], usend.at[2, u])

        def out_inner(u):
            return pltpu.make_async_copy(z2.at[urows(u)], grad_out.at[urows(u)], urecv.at[3, u])

        lag3, lag4, lag5 = 3, 6, 9
        first_small = jnp.where(x0, early_count + 2, early_count + 12)
        small_gap = 7

        def tick(t):
            u2, u3, u4, u5 = t, t - lag3, t - lag4, t - lag5
            pl.when(u2 + ahead < units)(lambda: send_across(u2 + ahead))

            @pl.when(u2 < units)
            def _():
                sum_across(u2)

                @pl.when(end)
                def _():
                    end_to_inner(u2).start()

            @pl.when(jnp.logical_and(inner, jnp.logical_and(u3 >= 0, u3 < units)))
            def _():
                end_to_inner(u3).wait_recv()
                add_rows(z1, urows(u3), ybuf[urows(u3), :], z1[urows(u3), :])
                inner_swap(u3).start()

            @pl.when(jnp.logical_and(inner, jnp.logical_and(u4 >= 0, u4 < units)))
            def _():
                inner_swap(u4).wait_recv()
                add_rows(z2, urows(u4), z1[urows(u4), :], z2[urows(u4), :])
                inner_to_end(u4).start()
                out_inner(u4).start()

            @pl.when(jnp.logical_and(end, jnp.logical_and(u5 >= 0, u5 < units)))
            def _():
                inner_to_end(u5).wait_recv()
                out_end(u5).start()

            pl.when(t == first_small)(small_start)
            for k in range(3):
                pl.when(t == first_small + small_gap * (k + 1))(functools.partial(small_next, k))
            pl.when(t == first_small + small_gap * 4)(small_end)

    else:

        def out_sum(u):
            return pltpu.make_async_copy(ybuf.at[urows(u)], grad_out.at[urows(u)], usend.at[1, u])

        def tick(u):
            pl.when(u + ahead < units)(lambda: send_across(u + ahead))
            sum_across(u)
            out_sum(u).start()

    def early_ticks(t, k):
        pl.when(jnp.logical_and(x0, t == 3))(lambda: loop((k + 1) * early, tick, k * early))

    def step(t):
        mb = jnp.where(x0, lax.rem(t, 2), t // 2)
        is_f = jnp.where(x0, t < 2, lax.rem(t, 2) == 0)

        @pl.when(is_f)
        def _():
            @pl.when(x1)
            def _():
                relay_copy(mb, 0).wait_recv()
                relay_copy(mb, 1).wait_recv()

            first_half(mb, t)

            @pl.when(jnp.logical_or(x1, t == 1))
            def _():
                second_half(jnp.where(x0, 0, mb), jnp.where(x0, 2, 1))

                @pl.when(x0)
                def _():
                    for b in range(2):
                        relay_copy(b, 0).start()
                        relay_copy(b, 1).start()
                        act_copy(b).start()

                @pl.when(x1)
                def _():
                    act_copy(mb).start()

        @pl.when(jnp.logical_not(is_f))
        def _():
            act_copy(mb).wait()

            @pl.when(x0)
            def _():
                for part in range(2):
                    relay_copy(mb, part).wait_send()
                    relay_copy(mb, part).wait_recv()

            @pl.when(jnp.logical_and(x0, t == 3))
            def _():
                gather_sent()

            backward_mlp(mb, t)

            @pl.when(jnp.logical_and(x0, t == 3))
            def _():
                in_terms()

            backward_attention(mb, t)

    def gather_sent():
        for i in range(CHUNKS):
            own_across(i).wait_send()
            own_to_twin(i).wait_send()
            y_to_z(i).wait_send()
            y_to_twin(i).wait_send()
            z_to_twin(i).wait_send()

    loop(4, step)

    @pl.when(x1)
    def _():
        gather_sent()
        loop(4, out_terms)
        in_terms()

    pay[0:2, 0:width] = gains_acc[0:2, :]
    for mb in range(2):
        pay[2 + mb : 3 + mb, pl.ds(width, 128)] = jnp.full((1, 128), times_ref[mb].astype(F32))
    for r in (0, 1, 4, 5, 6, 7):
        pay[r : r + 1, pl.ds(width, 128)] = jnp.full((1, 128), -1.0, F32)

    if nz == 4:
        pl.when(x0)(lambda: pay_copy.start())

    attention_terms()

    first_tick = jnp.where(x0, early_count, 0)
    if nz == 4:
        loop(units + lag5, tick, first_tick)

        def drain(u):
            y_send(u).wait_send()

            @pl.when(end)
            def _():
                end_to_inner(u).wait_send()
                out_end(u).wait()

            @pl.when(inner)
            def _():
                inner_swap(u).wait_send()
                inner_to_end(u).wait_send()
                out_inner(u).wait()

        loop(units, drain)

        @pl.when(x0)
        def _():
            pay_copy.wait_send()

        for k in range(4):
            slot_copy(k).wait_send()
    else:
        small_out[...] = pay[...]
        table_out[...] = jnp.zeros_like(table_out)
        loop(units, tick, first_tick)

        def drain(u):
            y_send(u).wait_send()
            out_sum(u).wait()

        loop(units, drain)

    def sent(i):
        for yy in range(2):
            to_twin(i, yy).wait_send()

    loop(CHUNKS, sent)
    for mb in range(2):
        dx_copy(mb).wait()

        @pl.when(x1)
        def _():
            for part in range(2):
                relay_copy(mb, part).wait_send()


def run_mega(timesteps, mask_flags, vector, gains, emb, cot, table, wq, wp, wi, wo, nz):
    count, seq, width = emb.shape
    quarter = wp.shape[0]
    unit = quarter // 4
    units = CHUNKS * quarter // unit
    tokens = count * seq
    assert count == 2 and quarter * 4 == width and wi.shape[1] == 4 * width and wo.shape[0] == width
    vmem = pl.BlockSpec(memory_space=pltpu.VMEM)
    smem = pl.BlockSpec(memory_space=pltpu.SMEM)
    hbm = pl.BlockSpec(memory_space=pl.ANY)
    dma = pltpu.SemaphoreType.DMA
    small = (16, width) if nz == 4 else (8, width + 128)
    extra = [pltpu.VMEM((nz * 4 * 8, width + 128), F32), pltpu.VMEM((8, width + 128), F32)]
    return pl.pallas_call(
        functools.partial(mega, (count, seq, width, nz, unit)),
        out_shape=(
            jax.ShapeDtypeStruct((count, seq, width), BF),
            jax.ShapeDtypeStruct((count, seq, width), F32),
            jax.ShapeDtypeStruct((CHUNKS * quarter, width), BF),
            jax.ShapeDtypeStruct(small, F32),
            jax.ShapeDtypeStruct((128, width), F32),
        ),
        in_specs=[smem, vmem, vmem, vmem] + [hbm] * 7,
        out_specs=(hbm, hbm, hbm, vmem, vmem),
        scratch_shapes=[
            pltpu.VMEM((CHUNKS * width, width), BF),
            pltpu.VMEM((count, seq, width), F32),
            pltpu.VMEM((count, seq, width), F32),
            pltpu.VMEM((count, seq, width), F32),
            pltpu.VMEM((seq, width), F32),
            pltpu.VMEM((count, seq, width), F32),
            pltpu.VMEM((tokens, width), BF),
            pltpu.VMEM((tokens, width), BF),
            pltpu.VMEM((tokens, width), BF),
            pltpu.VMEM((4, tokens, width), BF),
            pltpu.VMEM((4, tokens, width), BF),
            pltpu.VMEM((3, tokens, width), BF),
            pltpu.VMEM((count, HEADS, seq, seq), BF),
            pltpu.VMEM((tokens, width), BF),
            pltpu.VMEM((tokens, width), BF),
            pltpu.VMEM((3 * tokens, width), BF),
            pltpu.VMEM((seq, width), BF),
            pltpu.VMEM((count, seq, width), BF),
            pltpu.VMEM((count, seq, width), BF),
            pltpu.VMEM((count, seq, 128), F32),
            pltpu.VMEM((8, width), F32),
            pltpu.VMEM((8, width + 128), F32),
            pltpu.VMEM((8, width), F32),
            pltpu.VMEM((2, CHUNKS * quarter, width), BF),
            pltpu.VMEM((CHUNKS * quarter, width), BF),
            pltpu.VMEM((CHUNKS * quarter, width), BF),
            pltpu.VMEM((CHUNKS * quarter, width), BF),
            dma((4,)),
            dma((CHUNKS,)),
            dma((5, CHUNKS)),
            dma((5, CHUNKS)),
            dma((2, 2)),
            dma((2, 2)),
            dma((2, CHUNKS)),
            dma((2, CHUNKS)),
            dma((3, units)),
            dma((4, units)),
            dma((5,)),
            dma((5,)),
            dma((2, 2)),
        ]
        + (extra if nz == 4 else []),
        compiler_params=pltpu.CompilerParams(
            collective_id=0, has_side_effects=True, vmem_limit_bytes=67043328
        ),
        name="relay_layers",
    )(timesteps, mask_flags, vector, gains, emb, cot, table, wq, wp, wi, wo)


def small_sums(sizes, small, timesteps, rows_count, quarter):
    ns, ng, nz = sizes
    width = quarter * 4
    section, member = lax.axis_index("section"), lax.axis_index("grp")
    every = lax.all_gather(small, ("section", "grp", "dp"), axis=0, tiled=False)
    per_plane = every.reshape(ns, ng * nz, 8, width + 128)
    mine = lax.dynamic_index_in_dim(per_plane, section, 0, keepdims=False)[:, :2, :width].sum(axis=0)
    grad_gains = lax.dynamic_slice(mine, (0, member * quarter), (2, quarter))
    shard = section * ng + member
    here = rows_count // (ns * ng)
    ids = (shard * here + jnp.arange(here)).astype(F32)
    stamp = per_plane[0, :, :, width].reshape(-1)
    pick = (ids[:, None] == stamp[None, :]).astype(F32)
    grad_table = jnp.dot(pick, per_plane[0, :, :, :width].reshape(-1, width), precision=lax.Precision.HIGHEST)
    mask_here = width // (ns * ng)
    grad_mask = lax.dynamic_slice(per_plane[0, :, 4, :width].sum(axis=0), (shard * mask_here,), (mask_here,))
    return grad_gains, grad_table, grad_mask


def on_device(
    sizes,
    embeddings,
    mask_flags,
    timesteps,
    time_table,
    mask_vector,
    attn_qkv,
    attn_out,
    mlp_in,
    mlp_out,
    norm_gains,
    cotangent,
):
    ns, ng, nz = sizes
    rows_count, width = time_table.shape
    activations, dx, grads, small, table = run_mega(
        timesteps,
        mask_flags,
        mask_vector.astype(F32)[None],
        norm_gains[0],
        embeddings,
        cotangent,
        time_table,
        attn_qkv[0],
        attn_out[0],
        mlp_in[0],
        mlp_out[0],
        nz,
    )
    quarter = attn_out.shape[1]
    if nz == 4:
        grad_gains = small[:2, :quarter]
        grad_table = table[: rows_count // (ns * ng)]
        grad_mask = small[12, : width // (ns * ng)]
    else:
        grads = lax.psum(grads, "dp")
        grad_gains, grad_table, grad_mask = small_sums(sizes, small, timesteps, rows_count, quarter)

    def blocks(first, n):
        return jnp.concatenate(
            [grads[(first + j) * quarter : (first + j + 1) * quarter] for j in range(n)], axis=1
        ).astype(F32)

    return (
        activations[None],
        dx[None],
        blocks(QKV0, 3)[None],
        blocks(PROJ, 1)[None],
        blocks(IN0, 4)[None],
        grads[: 4 * quarter].astype(F32)[None],
        grad_gains[None],
        grad_table,
        grad_mask,
    )


def solution(mesh):
    sizes = (mesh.shape["section"], mesh.shape["grp"], mesh.shape["dp"])
    placed = (
        P(("grp", "dp"), None, None),
        P(("grp", "dp"), None),
        P(("grp", "dp")),
        P(),
        P(),
        P("section", "grp", None),
        P("section", "grp", None),
        P("section", "grp", None),
        P("section", "grp", None),
        P("section", None, None),
        P(("grp", "dp"), None, None),
    )
    return jax.shard_map(
        functools.partial(on_device, sizes),
        mesh=mesh,
        in_specs=placed,
        out_specs=(
            P("section", ("grp", "dp"), None, None),
            P("section", ("grp", "dp"), None, None),
            P("section", "grp", None),
            P("section", "grp", None),
            P("section", "grp", None),
            P("section", "grp", None),
            P("section", None, "grp"),
            P(("section", "grp"), None),
            P(("section", "grp")),
        ),
        check_vma=False,
    )
```

```python
import functools
import math

import jax
import jax.numpy as jnp
from jax import lax
from jax.experimental import pallas as pl
from jax.experimental.pallas import tpu as pltpu
from jax.sharding import PartitionSpec as P

HEADS = 12
HEAD = 64
BF = jnp.bfloat16
F32 = jnp.float32
MESH = pl.DeviceIdType.MESH
EPS = 1e-05
GELU_C = math.sqrt(2.0 / math.pi)

OUT0, IN0, PROJ, QKV0, CHUNKS = 0, 4, 8, 9, 12
YRING, ZRING = 16, 12
GATHER_ORDER = (9, 10, 11, 8, 4, 5, 6, 7, 0, 1, 2, 3)


def dot_nn(a, b):
    return lax.dot_general(a, b, (((1,), (0,)), ((), ())), preferred_element_type=F32)


def dot_nt(a, b):
    return lax.dot_general(a, b, (((1,), (1,)), ((), ())), preferred_element_type=F32)


def dot_tn(a, b):
    return lax.dot_general(a, b, (((0,), (0,)), ((), ())), preferred_element_type=F32)


def loop(n, body, first=0):
    lax.fori_loop(first, n, lambda i, c: (body(i), c)[1], 0)


def unrolled(n, body):
    for i in range(n):
        body(i)


def mega(
    cfg,
    times_ref,
    mask_ref,
    vector_ref,
    gains_ref,
    emb_hbm,
    cot_hbm,
    table_hbm,
    wq_hbm,
    wp_hbm,
    wi_hbm,
    wo_hbm,
    act_out,
    dx_out,
    grad_out,
    small_out,
    table_out,
    w,
    h,
    mid,
    acc,
    tmp,
    inv_sum,
    normed,
    mixed,
    n2,
    actv,
    gp,
    packed,
    probs,
    glow,
    dmlow,
    dpk,
    do_ref,
    outb,
    relay,
    maskc,
    trow,
    pay,
    sums,
    cbuf,
    ybuf,
    z1,
    z2,
    in_sem,
    own_sem,
    gsend,
    grecv,
    nrecv,
    rsend,
    rrecv,
    csend,
    crecv,
    ysend,
    yrecv,
    zsend,
    zrecv,
    zout,
    psend,
    precv,
    osem,
    *extra,
):
    count, seq, width, nz, unit = cfg
    quarter = width // 4
    units = CHUNKS * quarter // unit
    per_block = quarter // unit
    table_rows = table_hbm.shape[0]
    s = lax.axis_index("section")
    g = lax.axis_index("grp")
    d = lax.axis_index("dp")
    x0 = s == 0
    x1 = jnp.logical_not(x0)
    c = lax.rem(g, 2)
    y = g // 2
    twin = g + 1 - 2 * c
    across = lax.rem(g + 2, 4)
    zpair = d + 1 - 2 * lax.rem(d, 2)
    zfar = lax.rem(d + 2, 4)
    half = lax.rem(d, 2)

    peers = [{"section": 1 - s}, {"grp": twin}, {"grp": across}, {"dp": zpair}]
    if nz == 4:
        peers += [{"dp": 3 - d}, {"dp": zfar}]
    barrier = pltpu.get_barrier_semaphore()
    for peer in peers:
        pl.semaphore_signal(barrier, inc=1, device_id=peer, device_id_type=MESH)

    def remote(src, dst, send, recv, peer):
        return pltpu.make_async_remote_copy(
            src_ref=src, dst_ref=dst, send_sem=send, recv_sem=recv, device_id=peer, device_id_type=MESH
        )

    def rows(start, size, by):
        return pl.ds(pl.multiple_of(start, by), size)

    def place(i, q):
        return jnp.where(i < IN0, q * width + quarter * i, i * width + quarter * q)

    def source(i):
        if i < IN0:
            return wo_hbm.at[pl.ds(i * quarter, quarter)]
        if i < PROJ:
            return wi_hbm.at[:, pl.ds((i - IN0) * width, width)]
        if i == PROJ:
            return wp_hbm
        return wq_hbm.at[:, pl.ds((i - QKV0) * width, width)]

    sixth = quarter // 6
    share = {0: 2, 1: 3}
    far = across

    group_size = (4, 4, 1, 3)

    def group_of(i):
        if isinstance(i, int):
            return i // 4 if i < PROJ else 2 + (i > PROJ)
        return jnp.where(i < PROJ, i // 4, jnp.where(i == PROJ, 2, 3))

    def piece(i, q, first, n):
        return w.at[rows(place(i, q) + first * sixth, n * sixth, sixth)]

    def stage(k, i):
        return dpk.at[rows((k * CHUNKS + i) * sixth, sixth, sixth)]

    def own_copy(i):
        return pltpu.make_async_copy(source(i), w.at[rows(place(i, g), quarter, sixth)], own_sem.at[group_of(i)])

    def own_to_twin(i):
        return remote(source(i), w.at[rows(place(i, g), quarter, sixth)], gsend.at[0], nrecv.at[0, group_of(i)], {"grp": twin})

    def own_across(i, n):
        return remote(
            source(i).at[rows(half * n * sixth, n * sixth, sixth)],
            piece(i, g, half * n, n),
            gsend.at[1],
            grecv.at[0, i],
            {"grp": across},
        )

    def own_across_sixth(i, p):
        r = half * share[1] + p
        return remote(
            source(i).at[rows(r * sixth, sixth, sixth)], piece(i, g, r, 1), gsend.at[1], grecv.at[0, i], {"grp": across}
        )

    def own_over(i):
        return remote(
            source(i).at[rows((4 + half) * sixth, sixth, sixth)],
            stage(0, i),
            gsend.at[5],
            grecv.at[2, i],
            {"section": 1 - s},
        )

    def y_part(i, n):
        return piece(i, far, half * n, n)

    def z_part(i, n):
        return piece(i, far, (1 - half) * n, n)

    def y_to_z(i, n):
        return remote(y_part(i, n), y_part(i, n), gsend.at[2], grecv.at[1, i], {"dp": zpair})

    def y_to_twin(i, n):
        return remote(y_part(i, n), y_part(i, n), gsend.at[3], nrecv.at[1, group_of(i)], {"grp": twin})

    def z_to_twin(i, n):
        return remote(z_part(i, n), z_part(i, n), gsend.at[4], nrecv.at[2, group_of(i)], {"grp": twin})

    def over_to_twin(i):
        both = piece(i, far, 4, 2)
        return remote(both, both, gsend.at[6], nrecv.at[3, group_of(i)], {"grp": twin})

    def wait_for(ref, sem):
        remote(ref, ref, gsend.at[0], sem, {"grp": twin}).wait_recv()

    def stage_across(i):
        return remote(stage(0, i), stage(1, i), gsend.at[5], grecv.at[3, i], {"grp": across})

    def stage_to_z(i):
        return remote(stage(1, i), stage(2, i), gsend.at[7], grecv.at[4, i], {"dp": zpair})

    def stage_back(k, i):
        which = half if k == 1 else 1 - half
        return remote(stage(k, i), piece(i, far, 4 + which, 1), gsend.at[6], grecv.at[2, i], {"section": 1 - s})

    def bulk(n, send, recv, peer):
        return remote(w.at[pl.ds(0, n)], w.at[pl.ds(0, n)], send, recv, peer)

    def near_ready(k):
        n = group_size[k] * quarter
        bulk(n, gsend.at[0], nrecv.at[0, k], {"grp": twin}).wait_recv()
        pltpu.make_async_copy(w.at[pl.ds(0, n)], w.at[pl.ds(0, n)], own_sem.at[k]).wait()

    def far_ready(k, section):
        n = group_size[k] * share[section] * sixth
        bulk(n, gsend.at[3], nrecv.at[1, k], {"grp": twin}).wait_recv()
        bulk(n, gsend.at[4], nrecv.at[2, k], {"grp": twin}).wait_recv()
        if section == 0:
            bulk(group_size[k] * 2 * sixth, gsend.at[6], nrecv.at[3, k], {"grp": twin}).wait_recv()

    def all_ready(k, section):
        near_ready(k)
        far_ready(k, section)

    def gather_order(k):
        return jnp.where(k < 3, QKV0 + k, jnp.where(k == 3, PROJ, jnp.where(k < 8, k, k - 8)))

    def when_block(k, body):
        pl.when(jnp.logical_and(k >= 0, k < CHUNKS))(lambda: body(gather_order(k)))

    zlag, overlag = 2, 5
    ylag, backlag = 2, 4

    def pass_on(k, section):
        n = share[section]

        def from_y(i):
            wait_for(y_part(i, n), grecv.at[0, i])
            y_to_z(i, n).start()
            y_to_twin(i, n).start()

        def from_z(i):
            wait_for(z_part(i, n), grecv.at[1, i])
            z_to_twin(i, n).start()

        when_block(k, from_y)
        when_block(k - zlag, from_z)

    def gather_step(k):
        def from_over(i):
            wait_for(piece(i, far, 4, 2), grecv.at[2, i])
            over_to_twin(i).start()

        pass_on(k, 0)
        when_block(k - overlag, from_over)

    def second_step(k):
        pass_on(k, 1)

    early_blocks = 1 + CHUNKS // share[1]

    def start_sixth(k):
        for m, i in enumerate(GATHER_ORDER[:early_blocks]):
            pl.when(k // share[1] == m)(lambda: own_across_sixth(i, lax.rem(k, share[1])).start())

    def help_step(k):
        def from_x(i):
            wait_for(stage(0, i), grecv.at[2, i])
            stage_across(i).start()

        def from_y(i):
            wait_for(stage(1, i), grecv.at[3, i])
            stage_back(1, i).start()
            stage_to_z(i).start()

        def from_z(i):
            wait_for(stage(2, i), grecv.at[4, i])
            stage_back(2, i).start()

        when_block(k, from_x)
        when_block(k - ylag, from_y)
        when_block(k - backlag, from_z)

    def load(src, dst, k):
        return pltpu.make_async_copy(src, dst, in_sem.at[k])

    table_copy = load(table_hbm, dpk.at[pl.ds(0, table_rows)], 0)
    emb_copy = load(emb_hbm, outb, 1)

    def cot_copy(mb):
        return load(cot_hbm.at[mb], glow.at[rows(mb * seq, seq, seq)], 2 + mb)

    @pl.when(x0)
    def _():
        table_copy.start()
        emb_copy.start()

    @pl.when(x1)
    def _():
        for mb in range(2):
            cot_copy(mb).start()

    for i in GATHER_ORDER:
        own_copy(i).start()
    sums[...] = jnp.zeros_like(sums)
    for mb in range(2):
        maskc[mb] = jnp.transpose(jnp.broadcast_to(mask_ref[mb : mb + 1, :].astype(F32), (128, seq)))

    def enter():
        pl.semaphore_wait(barrier, len(peers))

    enter()

    def issue():
        @pl.when(x0)
        def _():
            for i in GATHER_ORDER:
                own_across(i, share[0]).start()
                own_over(i).start()

        @pl.when(x1)
        def _():
            own_across(GATHER_ORDER[0], share[1]).start()

        for i in GATHER_ORDER:
            own_to_twin(i).start()

    issue()

    def chunk(k):
        return w[rows(k * width, width, width), :]

    step_rows = 32
    parts_of = seq // step_rows
    lane = lax.broadcasted_iota(jnp.int32, (1, 128), 1)
    low_lane = lax.broadcasted_iota(jnp.int32, (seq, 128), 1) < HEAD
    low_half = (lane < HEAD).astype(F32)
    masks = (low_half.astype(BF), (1.0 - low_half).astype(BF))
    scaled = ((low_half * 0.125).astype(BF), ((1.0 - low_half) * 0.125).astype(BF))

    def seq_rows(mb):
        return rows(mb * seq, seq, seq)

    def sub_rows(mb, r):
        return rows(mb * seq + r * step_rows, step_rows, step_rows)

    def r_rows(r):
        return rows(r * step_rows, step_rows, step_rows)

    def norm_parts(v):
        center = v - jnp.mean(v, axis=-1, keepdims=True)
        spread = jnp.mean(center * center, axis=-1, keepdims=True)
        inv = lax.rsqrt(spread + EPS)
        return center * inv, inv

    @pl.when(x1)
    def _():
        def help_and_gather(k):
            help_step(k)
            pl.when(k < CHUNKS)(lambda: start_sixth(k + share[1]))
            pl.when(lax.rem(k, 3) == 1)(lambda: second_step(k // 3))

        loop(CHUNKS, help_and_gather)
        for i in GATHER_ORDER[early_blocks:]:
            own_across(i, share[1]).start()
        loop(CHUNKS + backlag, help_and_gather, CHUNKS)
        loop(11, second_step, early_blocks)
        all_ready(3, 1)
        all_ready(2, 1)

    @pl.when(x0)
    def _():
        table_copy.wait()
        emb_copy.wait()
        ids = lax.broadcasted_iota(jnp.int32, (8, table_rows), 1)
        pick = lax.broadcasted_iota(jnp.int32, (8, table_rows), 0)
        want = jnp.where(pick == 0, times_ref[0], times_ref[1])
        hot = jnp.where(jnp.logical_and(pick < 2, ids == want), 1.0, 0.0).astype(BF)
        trow[...] = dot_nn(hot, dpk[pl.ds(0, table_rows), :])
        vector = vector_ref[...].astype(F32).reshape(1, width)
        for mb in range(2):

            def make(r):
                m = maskc[mb, r_rows(r), 0:1]
                base = jnp.where(m > 0.5, vector, outb[mb, r_rows(r), :].astype(F32))
                h[mb, r_rows(r), :] = base + trow[mb : mb + 1, :]

            loop(parts_of, make)

    def more(mb, t, k):
        @pl.when(x0)
        def _():
            if k < 2:
                gather_step(8 + 2 * t + k)
            else:
                pl.when(t == 1)(lambda: gather_step(12))

        if k < 2:
            pl.when(jnp.logical_and(x1, t == 0))(lambda: second_step(11 + k))

    def first_half(mb, t):
        @pl.when(x1)
        def _():
            h[mb] = relay[mb].astype(F32)

        def ln(r):
            xhat, _ = norm_parts(h[mb, r_rows(r), :])
            normed[sub_rows(mb, r), :] = (xhat * gains_ref[0:1, :]).astype(BF)

        unrolled(parts_of, ln)

        @pl.when(jnp.logical_and(x0, t == 0))
        def _():
            loop(8, gather_step)
            all_ready(3, 0)

        def qkv(k):
            packed[k, seq_rows(mb), :] = dot_nn(normed[seq_rows(mb), :], chunk(QKV0 + k)).astype(BF)

        loop(3, qkv)

        more(mb, t, 0)

        def attend(j):
            cols = pl.ds(j * 128, 128)
            q2 = packed[0, seq_rows(mb), cols]
            k2 = packed[1, seq_rows(mb), cols]
            v2 = packed[2, seq_rows(mb), cols]
            got = []
            for e in range(2):
                sc = dot_nt(q2 * scaled[e], k2)
                ex = jnp.exp(sc - jnp.max(sc, axis=-1, keepdims=True)).astype(BF)
                probs[mb, 2 * j + e] = ex
                got.append(dot_nn(ex, v2 * masks[e] + masks[1 - e]))
            inv = 1.0 / pltpu.roll(jnp.where(low_lane, got[1], got[0]), HEAD, 1)
            inv_sum[mb, :, cols] = inv
            mixed[seq_rows(mb), cols] = (jnp.where(low_lane, got[0], got[1]) * inv).astype(BF)

        unrolled(HEADS // 2, attend)

        more(mb, t, 1)

        pl.when(jnp.logical_and(x0, t == 0))(lambda: all_ready(2, 0))
        mid[mb] = h[mb] + dot_nn(mixed[seq_rows(mb), :], chunk(PROJ))

        def ln_two(r):
            xhat, _ = norm_parts(mid[mb, r_rows(r), :])
            n2[sub_rows(mb, r), :] = (xhat * gains_ref[1:2, :]).astype(BF)

        unrolled(parts_of, ln_two)
        more(mb, t, 2)

    def mlp_up(q, mb):
        lhs = n2[seq_rows(mb), :]
        piece = 256
        chunk_rows = rows((IN0 + q) * width, width, width)

        def product(j):
            return dot_nn(lhs, w[chunk_rows, pl.ds(j * piece, piece)])

        up = product(0)
        for j in range(width // piece):
            after = product(j + 1) if (j + 1) * piece < width else None
            cols = pl.ds(j * piece, piece)
            sq = up * up
            hp = 0.5 + 0.5 * jnp.tanh(up * (GELU_C + (GELU_C * 0.044715) * sq))
            act = up * hp
            actv[q, seq_rows(mb), cols] = act.astype(BF)
            gp[q, seq_rows(mb), cols] = (
                hp + act * ((1.0 - hp) * (2.0 * GELU_C + (2.0 * GELU_C * 0.134145) * sq))
            ).astype(BF)
            up = after

    def mlp_down(q, mb):
        acc[mb] += dot_nn(actv[q, seq_rows(mb), :], chunk(OUT0 + q))

    def second_half_one(mb, t):
        def at_first(body):
            pl.when(t == 0)(body)

        at_first(lambda: all_ready(1, 1))
        for q in range(4):
            mlp_up(q, mb)
        acc[mb] = mid[mb]
        at_first(lambda: near_ready(0))
        for r in range(2):
            mlp_down(2 * y + r, mb)

        @at_first
        def _():
            second_step(13)
            far_ready(0, 1)
            for k, n in ((5, 1), (6, 2), (7, 1)):
                bulk(CHUNKS * n * sixth, gsend.at[k], grecv.at[0, 0], {"grp": twin}).wait_send()

        for r in range(2):
            mlp_down(2 * (1 - y) + r, mb)
        outb[mb] = acc[mb].astype(BF)

    def second_half_both():
        all_ready(1, 0)

        def up(i):
            q, mb = i // 2, lax.rem(i, 2)
            mlp_up(q, mb)

            pl.when(lax.rem(i, 2) == 1)(lambda: gather_step(13 + i // 2))

        loop(8, up)
        acc[...] = mid[...]
        near_ready(0)
        loop(4, lambda i: mlp_down(2 * y + i // 2, lax.rem(i, 2)))
        far_ready(0, 0)

        def down(mb):
            for r in range(2):
                mlp_down(2 * (1 - y) + r, mb)
            outb[mb] = acc[mb].astype(BF)
            relay_copy(mb, 0).start()
            relay_copy(mb, 1).start()
            act_copy(mb).start()

        loop(2, down)

    def relay_copy(mb, part):
        r = pl.ds(part * (seq // 2), seq // 2)
        return remote(
            outb.at[mb, r], relay.at[mb, r], rsend.at[mb, part], rrecv.at[mb, part], {"section": 1 - s}
        )

    def act_copy(mb):
        return pltpu.make_async_copy(outb.at[mb], act_out.at[mb], osem.at[0, mb])

    def dx_copy(mb):
        return pltpu.make_async_copy(h.at[mb], dx_out.at[mb], osem.at[1, mb])

    def norm_back(v, gain, dy):
        xhat, inv = norm_parts(v)
        dxh = dy * gain
        m1 = jnp.mean(dxh, axis=-1, keepdims=True)
        m2 = jnp.mean(dxh * xhat, axis=-1, keepdims=True)
        return inv * (dxh - m1 - xhat * m2), jnp.sum(dy * xhat, axis=0, keepdims=True)

    def backward_mlp(mb, t):
        @pl.when(x0)
        def _():
            glow[seq_rows(mb), :] = relay[mb]

        @pl.when(x1)
        def _():
            cot_copy(mb).wait()

        tmp[...] = jnp.zeros_like(tmp)

        def slope(q):
            da = dot_nt(glow[seq_rows(mb), :], chunk(OUT0 + q))
            du = (gp[q, seq_rows(mb), :].astype(F32) * da).astype(BF)
            gp[q, seq_rows(mb), :] = du
            return du

        def back_up(q):
            tmp[...] += dot_nt(gp[q, seq_rows(mb), :], chunk(IN0 + q))

        def mlp(q):
            tmp[...] += dot_nt(slope(q), chunk(IN0 + q))

        def slope_and_out(k):
            slope(out_order(k))
            out_terms(k)

        last = jnp.logical_and(x0, t == 3)

        @pl.when(last)
        def _():
            loop(4, slope_and_out)
            loop(4, back_up)

        pl.when(jnp.logical_not(last))(lambda: loop(4, mlp))

        def ln_two(r):
            dx, dg = norm_back(mid[mb, r_rows(r), :], gains_ref[1:2, :], tmp[r_rows(r), :])
            dm = glow[sub_rows(mb, r), :].astype(F32) + dx
            mid[mb, r_rows(r), :] = dm
            dmlow[sub_rows(mb, r), :] = dm.astype(BF)
            sums[1:2, :] += dg

        unrolled(parts_of, ln_two)

    def backward_attention(mb, t):
        do_ref[...] = (dot_nt(dmlow[seq_rows(mb), :], chunk(PROJ)) * inv_sum[mb]).astype(BF)

        def attend(j):
            cols = pl.ds(j * 128, 128)
            q2 = packed[0, seq_rows(mb), cols]
            k2 = packed[1, seq_rows(mb), cols]
            v2 = packed[2, seq_rows(mb), cols]
            do2 = do_ref[:, cols]
            weighed = do2.astype(F32) * mixed[seq_rows(mb), cols].astype(F32)
            dq = jnp.zeros((seq, 128), F32)
            dk = jnp.zeros((seq, 128), F32)
            dv = jnp.zeros((seq, 128), F32)
            for e in range(2):
                ex = probs[mb, 2 * j + e]
                dom = do2 * masks[e]
                inner = jnp.sum(jnp.where(low_lane if e == 0 else jnp.logical_not(low_lane), weighed, 0.0), axis=-1, keepdims=True)
                ds = (ex.astype(F32) * (dot_nt(dom, v2) - inner)).astype(BF)
                dv = dv + dot_tn(ex, dom)
                dq = dq + dot_nn(ds, k2 * scaled[e])
                dk = dk + dot_tn(ds, q2 * scaled[e])
            for k, v in enumerate((dq, dk, dv)):
                dpk[rows(k * 2 * seq + mb * seq, seq, seq), cols] = v.astype(BF)

        for j in range(HEADS // 2):
            attend(j)

        early_tick(t, 5)
        early_tick(t, 6)
        tmp[...] = jnp.zeros_like(tmp)

        def qkv(k):
            tmp[...] += dot_nt(dpk[rows(k * 2 * seq + mb * seq, seq, seq), :], chunk(QKV0 + k))

        loop(3, qkv)
        early_tick(t, 7)
        act_copy(mb).wait()

        @pl.when(x0)
        def _():
            for part in range(2):
                relay_copy(mb, part).wait_send()

        for part in range(2):

            def ln_one(rr):
                r = rr + part * (parts_of // 2)
                dx, dg = norm_back(h[mb, r_rows(r), :], gains_ref[0:1, :], tmp[r_rows(r), :])
                dm = mid[mb, r_rows(r), :] + dx
                outb[mb, r_rows(r), :] = dm.astype(BF)
                sums[0:1, :] += dg
                m = maskc[mb, r_rows(r), 0:1]
                kept = jnp.where(jnp.logical_and(x0, m > 0.5), 0.0, dm)
                h[mb, r_rows(r), :] = kept
                sums[pl.ds(2 + mb, 1), :] += jnp.sum(dm, axis=0, keepdims=True)
                sums[4:5, :] += jnp.sum(dm - kept, axis=0, keepdims=True)

            unrolled(parts_of // 2, ln_one)

            @pl.when(x1)
            def _():
                relay_copy(mb, part).start()

        dx_copy(mb).start()
        early_tick(t, 8)

    def grad_chunk(a, b, k):
        w[rows(k * width, width, width), :] = dot_tn(a, b).astype(BF)

    def cslot(i, yy):
        return cbuf.at[yy, rows(i * quarter, quarter, quarter)]

    def to_twin(i, yy):
        q = 2 * yy + (1 - c)
        return remote(
            w.at[rows(place(i, q), quarter, quarter)], cslot(i, yy), csend.at[yy], crecv.at[yy, i // 4], {"grp": twin}
        )

    def from_twin(k, yy):
        ref = cbuf.at[yy, rows(4 * k * quarter, 4 * quarter, quarter)]
        remote(ref, ref, csend.at[yy], crecv.at[yy, k], {"grp": twin}).wait_recv()

    def urows(u):
        return rows(u * unit, unit, unit)

    def y_send(u):
        k = lax.rem(u, YRING)
        return remote(
            cbuf.at[1 - y, urows(u)], ybuf.at[urows(u)], ysend.at[k], yrecv.at[k], {"grp": across}
        )

    def merge_far(i):
        pl.when(lax.rem(i, 4) == 0)(lambda: from_twin(i // 4, 1 - y))
        part = rows(i * quarter, quarter, quarter)
        mine = w[rows(place(i, 2 * (1 - y) + c), quarter, quarter), :].astype(F32)
        cbuf[1 - y, part, :] = (cbuf[1 - y, part, :].astype(F32) + mine).astype(BF)

    ahead = 6

    def send_across(u):
        pl.when(lax.rem(u, per_block) == 0)(lambda: merge_far(u // per_block))
        pl.when(u >= YRING)(lambda: y_send(u - YRING).wait_send())
        y_send(u).start()

    def out_order(k):
        side = jnp.where(k < 2, 1 - y, y)
        return 2 * side + jnp.where(lax.rem(k, 2) == 0, 1 - c, c)

    def out_terms(k):
        q = out_order(k)
        grad_chunk(actv[q], glow[...], OUT0 + q)

        @pl.when(lax.rem(k, 2) == 0)
        def _():
            loop(4, lambda i: to_twin(i, jnp.where(k == 0, 1 - y, y)).start())

        @pl.when(k == 1)
        def _():
            loop(ahead, send_across)

    def other_terms(i, a, b):
        grad_chunk(a, b, i)
        to_twin(i, 1 - y).start()
        to_twin(i, y).start()

    def in_terms():
        early_tick_now(0)

        def one(q):
            other_terms(IN0 + q, n2[...], gp[q])
            early_tick_now(1 + q)

        loop(4, one)

    def attention_terms():
        first = jnp.where(x0, 9, 5)
        other_terms(PROJ, mixed[...], dmlow[...])
        early_tick_now(first)

        def one(k):
            other_terms(QKV0 + k, normed[...], dpk[rows(k * 2 * seq, 2 * seq, 2 * seq), :])
            early_tick_now(first + 1 + k)

        loop(3, one)

    def add_rows(dst, dst_rows, *terms):
        dst[dst_rows, :] = functools.reduce(jnp.add, [a.astype(F32) for a in terms]).astype(BF)

    def sum_across(u):
        i = u // per_block
        pl.when(lax.rem(u, 4 * per_block) == 0)(lambda: from_twin(i // 4, y))
        y_send(u).wait_recv()
        mine = w[rows(place(i, g) + lax.rem(u, per_block) * unit, unit, unit), :]
        add_rows(ybuf, urows(u), cbuf[y, urows(u), :], mine, ybuf[urows(u), :])

    first_tick = jnp.where(x0, 13, 9)
    if nz == 4:
        end = jnp.logical_or(d == 0, d == 3)
        inner = jnp.logical_not(end)
        slots, landed = extra
        pay_copy = remote(pay, landed.at[0], psend.at[0], precv.at[0], {"section": 1 - s})
        last_part = pl.ds(8, 8)

        sums_rows = pl.ds(nz * 8, 8)

        def small_copy(k):
            peer = ({"grp": twin}, {"grp": across}, {"dp": zpair}, {"dp": zfar})[k]
            part = pl.ds(0, 16) if k < 3 else last_part
            return remote(pay.at[part], landed.at[1 + k, part], psend.at[1 + k], precv.at[1 + k], peer)

        pair_rows = rows((d // 2) * 16, 16, 16)
        far_rows = rows((1 - d // 2) * 16, 16, 16)
        pair_copy = remote(slots.at[pair_rows], slots.at[pair_rows], psend.at[5], precv.at[5], {"dp": zfar})
        pair_wait = remote(slots.at[far_rows], slots.at[far_rows], psend.at[5], precv.at[5], {"dp": zfar})
        give_back = remote(slots, slots, psend.at[6], precv.at[6], {"section": 1 - s})

        def small_start():
            pay_copy.wait_recv()
            pay[0:8, :] = landed[0, 0:8, :]
            row = lax.broadcasted_iota(jnp.int32, (8, width + 128), 0)
            other = landed[0, last_part, :]
            pay[last_part, :] = jnp.where(
                row < 2, pay[last_part, :], jnp.where(row == 2, other, pltpu.roll(other, 3, 0))
            )
            small_copy(0).start()

        def small_next(k):
            small_copy(k).wait_recv()
            small_copy(k).wait_send()
            if k < 2:
                pay[...] = pay[...] + landed[1 + k]
                if k == 1:
                    slots[rows(d * 8, 8, 8), :] = pay[0:8, :]
                small_copy(k + 1).start()
            else:
                slots[rows(zpair * 8, 8, 8), :] = landed[3, 0:8, :]
                pay[last_part, :] = pay[last_part, :] + landed[3, last_part, :]
                small_copy(3).start()
                pair_copy.start()

        def small_end():
            small_copy(3).wait_recv()
            small_copy(3).wait_send()
            pair_wait.wait_recv()
            slots[sums_rows, :] = pay[last_part, :] + landed[4, last_part, :]
            give_back.start()

        def small_results():
            pl.when(x0)(lambda: give_back.wait_recv())
            total = slots[sums_rows, 0:width]
            shard = s * 4 + g
            mine = jnp.where(x0, pltpu.roll(total, 5, 0), total)
            small_out[0:8, :] = pltpu.roll(mine, lax.rem(width - quarter * g, width), 1)
            small_out[8:16, :] = pltpu.roll(total, lax.rem(width - (width // 8) * shard, width), 1)
            base = shard * (table_rows // 8) + 1
            ids = (base + lax.broadcasted_iota(jnp.int32, (nz * 8, 128), 1)).astype(F32)
            pick = jnp.where(slots[0 : nz * 8, pl.ds(width, 128)] == ids, 1.0, 0.0).astype(BF)
            rest = slots[0 : nz * 8, 0:width]
            found = jnp.zeros((128, width), F32)
            for _ in range(3):
                part = rest.astype(BF)
                found = found + dot_tn(pick, part)
                rest = rest - part.astype(F32)
            table_out[...] = found

        def zcopy(src, dst, k, u, peer):
            m = lax.rem(u, ZRING)
            return remote(src.at[urows(u)], dst.at[urows(u)], zsend.at[k, m], zrecv.at[k, m], peer)

        def end_to_inner(u):
            return zcopy(ybuf, z1, 0, u, {"dp": zpair})

        def inner_swap(u):
            return zcopy(z1, z2, 1, u, {"dp": 3 - d})

        def inner_to_end(u):
            return zcopy(z2, z1, 0, u, {"dp": zpair})

        def grad_copy(src, u):
            return pltpu.make_async_copy(src.at[urows(u)], grad_out.at[urows(u)], zout.at[lax.rem(u, ZRING)])

        def launch(copy, u):
            pl.when(u >= ZRING)(lambda: copy(u - ZRING).wait_send())
            copy(u).start()

        def put_out(src, u):
            pl.when(u >= ZRING)(lambda: grad_copy(src, u - ZRING).wait())
            grad_copy(src, u).start()

        lag3, lag4, lag5 = 3, 6, 9
        first_small, small_gap = 16, 6

        def tick(t, small=True):
            u2, u3, u4, u5 = t, t - lag3, t - lag4, t - lag5
            pl.when(u2 + ahead < units)(lambda: send_across(u2 + ahead))

            @pl.when(u2 < units)
            def _():
                sum_across(u2)

                @pl.when(end)
                def _():
                    launch(end_to_inner, u2)

            @pl.when(jnp.logical_and(inner, jnp.logical_and(u3 >= 0, u3 < units)))
            def _():
                end_to_inner(u3).wait_recv()
                add_rows(z1, urows(u3), ybuf[urows(u3), :], z1[urows(u3), :])
                launch(inner_swap, u3)

            @pl.when(jnp.logical_and(inner, jnp.logical_and(u4 >= 0, u4 < units)))
            def _():
                inner_swap(u4).wait_recv()
                add_rows(z2, urows(u4), z1[urows(u4), :], z2[urows(u4), :])
                launch(inner_to_end, u4)
                put_out(z2, u4)

            @pl.when(jnp.logical_and(end, jnp.logical_and(u5 >= 0, u5 < units)))
            def _():
                inner_to_end(u5).wait_recv()
                put_out(z1, u5)

            if not small:
                return
            pl.when(t == jnp.where(x1, units, units + 2))(small_results)

            @pl.when(x1)
            def _():
                pl.when(t == first_small)(small_start)
                for k in range(3):
                    pl.when(t == first_small + small_gap * (k + 1))(functools.partial(small_next, k))
                pl.when(t == first_small + small_gap * 4)(small_end)

    else:

        def out_sum(u):
            return pltpu.make_async_copy(ybuf.at[urows(u)], grad_out.at[urows(u)], zout.at[lax.rem(u, ZRING)])

        def tick(u, small=True):
            pl.when(u + ahead < units)(lambda: send_across(u + ahead))
            sum_across(u)
            pl.when(u >= ZRING)(lambda: out_sum(u - ZRING).wait())
            out_sum(u).start()

    def early_tick_now(t):
        tick(t, False)

    def early_tick(t, k):
        pl.when(jnp.logical_and(x0, t == 3))(lambda: early_tick_now(k))

    def step(t):
        mb = jnp.where(x0, lax.rem(t, 2), t // 2)
        is_f = jnp.where(x0, t < 2, lax.rem(t, 2) == 0)

        @pl.when(is_f)
        def _():
            @pl.when(x1)
            def _():
                relay_copy(mb, 0).wait_recv()
                relay_copy(mb, 1).wait_recv()

            first_half(mb, t)

            pl.when(jnp.logical_and(x0, t == 1))(second_half_both)

            @pl.when(x1)
            def _():
                second_half_one(mb, t)
                act_copy(mb).start()

        @pl.when(jnp.logical_not(is_f))
        def _():
            @pl.when(x0)
            def _():
                for part in range(2):
                    relay_copy(mb, part).wait_recv()

            @pl.when(jnp.logical_and(x0, t == 3))
            def _():
                gather_sent(0)

            backward_mlp(mb, t)

            @pl.when(jnp.logical_and(x0, t == 3))
            def _():
                in_terms()

            backward_attention(mb, t)

    def gather_sent(section):
        bulk(CHUNKS * quarter, gsend.at[0], nrecv.at[0, 0], {"grp": twin}).wait_send()
        n = CHUNKS * share[section] * sixth
        for k in range(1, 5):
            bulk(n, gsend.at[k], grecv.at[0, 0], {"grp": twin}).wait_send()
        if section == 0:
            for k, n in ((5, 1), (6, 2)):
                bulk(CHUNKS * n * sixth, gsend.at[k], grecv.at[0, 0], {"grp": twin}).wait_send()

    loop(4, step)

    @pl.when(x1)
    def _():
        gather_sent(1)
        loop(4, out_terms)
        in_terms()

    row_ids = lax.broadcasted_iota(jnp.int32, (8, width), 0)
    stamp_ids = lax.broadcasted_iota(jnp.int32, (8, 128), 0)
    first = 2 * g
    pay[0:8, 0:width] = jnp.where(
        row_ids == first, sums[2:3, :], jnp.where(row_ids == first + 1, sums[3:4, :], 0.0)
    )
    pay[0:8, pl.ds(width, 128)] = jnp.where(
        stamp_ids == first,
        (times_ref[0] + 1).astype(F32),
        jnp.where(stamp_ids == first + 1, (times_ref[1] + 1).astype(F32), 0.0),
    )
    pay[8:16, 0:width] = jnp.where(
        row_ids < 2, sums[...], jnp.where(row_ids == 2, sums[4:5, :], 0.0)
    )
    pay[8:16, pl.ds(width, 128)] = jnp.zeros((8, 128), F32)

    if nz == 4:
        pl.when(x0)(lambda: pay_copy.start())

    attention_terms()

    if nz == 4:
        loop(units + lag5, tick, first_tick)

        loop(units, lambda u: y_send(u).wait_send(), units - YRING)

        def drain(u):
            @pl.when(end)
            def _():
                end_to_inner(u).wait_send()
                grad_copy(z1, u).wait()

            @pl.when(inner)
            def _():
                inner_swap(u).wait_send()
                inner_to_end(u).wait_send()
                grad_copy(z2, u).wait()

        loop(units, drain, units - ZRING)

        pl.when(x0)(lambda: pay_copy.wait_send())

        @pl.when(x1)
        def _():
            pair_copy.wait_send()
            give_back.wait_send()

    else:
        small_out[...] = pay[...]
        table_out[...] = jnp.zeros_like(table_out)
        loop(units, tick, first_tick)

        loop(units, lambda u: y_send(u).wait_send(), units - YRING)
        loop(units, lambda u: out_sum(u).wait(), units - ZRING)

    for yy in range(2):
        bulk(CHUNKS * quarter, csend.at[yy], crecv.at[yy, 0], {"grp": twin}).wait_send()

    for mb in range(2):
        dx_copy(mb).wait()

        @pl.when(x1)
        def _():
            for part in range(2):
                relay_copy(mb, part).wait_send()


def run_mega(timesteps, mask_flags, vector, gains, emb, cot, table, wq, wp, wi, wo, nz):
    count, seq, width = emb.shape
    quarter = wp.shape[0]
    unit = quarter // 4
    units = CHUNKS * quarter // unit
    tokens = count * seq
    assert count == 2 and quarter * 4 == width and wi.shape[1] == 4 * width and wo.shape[0] == width
    vmem = pl.BlockSpec(memory_space=pltpu.VMEM)
    smem = pl.BlockSpec(memory_space=pltpu.SMEM)
    hbm = pl.BlockSpec(memory_space=pl.ANY)
    dma = pltpu.SemaphoreType.DMA
    small = (16, width) if nz == 4 else (16, width + 128)
    extra = [pltpu.VMEM((nz * 8 + 8, width + 128), F32), pltpu.VMEM((5, 16, width + 128), F32)]
    return pl.pallas_call(
        functools.partial(mega, (count, seq, width, nz, unit)),
        out_shape=(
            jax.ShapeDtypeStruct((count, seq, width), BF),
            jax.ShapeDtypeStruct((count, seq, width), F32),
            jax.ShapeDtypeStruct((CHUNKS * quarter, width), BF),
            jax.ShapeDtypeStruct(small, F32),
            jax.ShapeDtypeStruct((128, width), F32),
        ),
        in_specs=[smem, vmem, vmem, vmem] + [hbm] * 7,
        out_specs=(hbm, hbm, hbm, vmem, vmem),
        scratch_shapes=[
            pltpu.VMEM((CHUNKS * width, width), BF),
            pltpu.VMEM((count, seq, width), F32),
            pltpu.VMEM((count, seq, width), F32),
            pltpu.VMEM((count, seq, width), F32),
            pltpu.VMEM((seq, width), F32),
            pltpu.VMEM((count, seq, width), F32),
            pltpu.VMEM((tokens, width), BF),
            pltpu.VMEM((tokens, width), BF),
            pltpu.VMEM((tokens, width), BF),
            pltpu.VMEM((4, tokens, width), BF),
            pltpu.VMEM((4, tokens, width), BF),
            pltpu.VMEM((3, tokens, width), BF),
            pltpu.VMEM((count, HEADS, seq, seq), BF),
            pltpu.VMEM((tokens, width), BF),
            pltpu.VMEM((tokens, width), BF),
            pltpu.VMEM((3 * tokens, width), BF),
            pltpu.VMEM((seq, width), BF),
            pltpu.VMEM((count, seq, width), BF),
            pltpu.VMEM((count, seq, width), BF),
            pltpu.VMEM((count, seq, 128), F32),
            pltpu.VMEM((8, width), F32),
            pltpu.VMEM((16, width + 128), F32),
            pltpu.VMEM((8, width), F32),
            pltpu.VMEM((2, CHUNKS * quarter, width), BF),
            pltpu.VMEM((CHUNKS * quarter, width), BF),
            pltpu.VMEM((CHUNKS * quarter, width), BF),
            pltpu.VMEM((CHUNKS * quarter, width), BF),
            dma((4,)),
            dma((4,)),
            dma((8,)),
            dma((5, CHUNKS)),
            dma((4, 4)),
            dma((2, 2)),
            dma((2, 2)),
            dma((2,)),
            dma((2, 3)),
            dma((YRING,)),
            dma((YRING,)),
            dma((2, ZRING)),
            dma((2, ZRING)),
            dma((ZRING,)),
            dma((7,)),
            dma((7,)),
            dma((2, 2)),
        ]
        + (extra if nz == 4 else []),
        compiler_params=pltpu.CompilerParams(
            collective_id=0, has_side_effects=True, vmem_limit_bytes=67043328
        ),
        name="relay_layers",
    )(timesteps, mask_flags, vector, gains, emb, cot, table, wq, wp, wi, wo)


def place_results(
    act_in,
    dx_in,
    grads_in,
    small_ref,
    table_ref,
    act_out,
    dx_out,
    qkv_out,
    proj_out,
    in_out,
    out_out,
    gains_out,
    table_out,
    mask_out,
    act_buf,
    dx_buf,
    low_buf,
    wide_buf,
    ins,
    outs,
):
    quarter, width = proj_out.shape
    blocks = []
    for i in range(CHUNKS):
        part = pl.ds(i * quarter, quarter)
        if i < IN0:
            target = out_out.at[part]
        elif i < PROJ:
            target = in_out.at[:, pl.ds((i - IN0) * width, width)]
        elif i == PROJ:
            target = proj_out
        else:
            target = qkv_out.at[:, pl.ds((i - QKV0) * width, width)]
        blocks.append(
            (
                part,
                pltpu.make_async_copy(grads_in.at[part], low_buf.at[part], ins.at[i]),
                pltpu.make_async_copy(wide_buf.at[part], target, outs.at[i]),
            )
        )
    plain = [
        (
            pltpu.make_async_copy(dx_in, dx_buf, ins.at[CHUNKS]),
            pltpu.make_async_copy(dx_buf, dx_out, outs.at[CHUNKS]),
        ),
        (
            pltpu.make_async_copy(act_in, act_buf, ins.at[CHUNKS + 1]),
            pltpu.make_async_copy(act_buf, act_out, outs.at[CHUNKS + 1]),
        ),
    ]
    for _, come, _ in blocks:
        come.start()
    for come, _ in plain:
        come.start()
    for part, come, go in blocks:
        come.wait()
        wide_buf[part, :] = low_buf[part, :].astype(F32)
        go.start()
    for come, go in plain:
        come.wait()
        go.start()
    gains_out[...] = small_ref[0:2, 0:quarter]
    table_out[...] = table_ref[0 : table_out.shape[0], :]
    mask_out[...] = small_ref[10, 0 : mask_out.shape[0]]
    for _, _, go in blocks:
        go.wait()
    for _, go in plain:
        go.wait()


def run_place(activations, dx, grads, small, table, quarter, table_here, mask_here):
    count, seq, width = dx.shape
    vmem = pl.BlockSpec(memory_space=pltpu.VMEM)
    hbm = pl.BlockSpec(memory_space=pl.ANY)
    dma = pltpu.SemaphoreType.DMA
    shapes = (
        ((count, seq, width), BF),
        ((count, seq, width), F32),
        ((quarter, 3 * width), F32),
        ((quarter, width), F32),
        ((quarter, 4 * width), F32),
        ((width, width), F32),
        ((2, quarter), F32),
        ((table_here, width), F32),
        ((mask_here,), F32),
    )
    return pl.pallas_call(
        place_results,
        out_shape=tuple(jax.ShapeDtypeStruct(a, b) for a, b in shapes),
        in_specs=[hbm] * 3 + [vmem] * 2,
        out_specs=(hbm,) * 6 + (vmem,) * 3,
        scratch_shapes=[
            pltpu.VMEM((count, seq, width), BF),
            pltpu.VMEM((count, seq, width), F32),
            pltpu.VMEM((CHUNKS * quarter, width), BF),
            pltpu.VMEM((CHUNKS * quarter, width), F32),
            dma((CHUNKS + 2,)),
            dma((CHUNKS + 2,)),
        ],
        compiler_params=pltpu.CompilerParams(vmem_limit_bytes=64000000),
        name="place_results",
    )(activations, dx, grads, small, table)


def small_sums(sizes, small, timesteps, rows_count, quarter):
    ns, ng, nz = sizes
    width = quarter * 4
    section, member = lax.axis_index("section"), lax.axis_index("grp")
    every = lax.all_gather(small, ("section", "grp", "dp"), axis=0, tiled=False)
    per_plane = every.reshape(ns, ng * nz, 16, width + 128)
    mine = lax.dynamic_index_in_dim(per_plane, section, 0, keepdims=False)[:, 8:10, :width].sum(axis=0)
    grad_gains = lax.dynamic_slice(mine, (0, member * quarter), (2, quarter))
    shard = section * ng + member
    here = rows_count // (ns * ng)
    ids = (shard * here + 1 + jnp.arange(here)).astype(F32)
    stamp = per_plane[0, :, :8, width].reshape(-1)
    pick = (ids[:, None] == stamp[None, :]).astype(F32)
    tokens = per_plane[0, :, :8, :width].reshape(-1, width)
    grad_table = jnp.dot(pick, tokens, precision=lax.Precision.HIGHEST)
    mask_here = width // (ns * ng)
    grad_mask = lax.dynamic_slice(per_plane[0, :, 10, :width].sum(axis=0), (shard * mask_here,), (mask_here,))
    return grad_gains, grad_table, grad_mask


def on_device(
    sizes,
    embeddings,
    mask_flags,
    timesteps,
    time_table,
    mask_vector,
    attn_qkv,
    attn_out,
    mlp_in,
    mlp_out,
    norm_gains,
    cotangent,
):
    ns, ng, nz = sizes
    rows_count, width = time_table.shape
    activations, dx, grads, small, table = run_mega(
        timesteps,
        mask_flags,
        mask_vector,
        norm_gains[0],
        embeddings,
        cotangent,
        time_table,
        attn_qkv[0],
        attn_out[0],
        mlp_in[0],
        mlp_out[0],
        nz,
    )
    quarter = attn_out.shape[1]
    table_here, mask_here = rows_count // (ns * ng), width // (ns * ng)
    if nz != 4:
        grads = lax.psum(grads, "dp")
        gain_sums, table_sums, mask_sums = small_sums(sizes, small, timesteps, rows_count, quarter)
    placed = run_place(
        activations, dx, grads, small, table, quarter, table_here, mask_here
    )
    if nz != 4:
        placed = placed[:6] + (gain_sums, table_sums, mask_sums)
    return tuple(v[None] for v in placed[:7]) + placed[7:]


def solution(mesh):
    sizes = (mesh.shape["section"], mesh.shape["grp"], mesh.shape["dp"])
    placed = (
        P(("grp", "dp"), None, None),
        P(("grp", "dp"), None),
        P(("grp", "dp")),
        P(),
        P(),
        P("section", "grp", None),
        P("section", "grp", None),
        P("section", "grp", None),
        P("section", "grp", None),
        P("section", None, None),
        P(("grp", "dp"), None, None),
    )
    return jax.shard_map(
        functools.partial(on_device, sizes),
        mesh=mesh,
        in_specs=placed,
        out_specs=(
            P("section", ("grp", "dp"), None, None),
            P("section", ("grp", "dp"), None, None),
            P("section", "grp", None),
            P("section", "grp", None),
            P("section", "grp", None),
            P("section", "grp", None),
            P("section", None, "grp"),
            P(("section", "grp"), None),
            P(("section", "grp")),
        ),
        check_vma=False,
    )
```

```python
import functools
import math

import jax
import jax.numpy as jnp
from jax import lax
from jax.experimental import pallas as pl
from jax.experimental.pallas import tpu as pltpu
from jax.sharding import PartitionSpec as P

HEADS = 12
HEAD = 64
BF = jnp.bfloat16
F32 = jnp.float32
MESH = pl.DeviceIdType.MESH
EPS = 1e-05
GELU_C = math.sqrt(2.0 / math.pi)

OUT0, IN0, PROJ, QKV0, CHUNKS = 0, 4, 8, 9, 12
YRING, ZRING = 16, 12
GATHER_ORDER = (9, 10, 11, 8, 4, 5, 6, 7, 0, 1, 2, 3)


def dot_nn(a, b):
    return lax.dot_general(a, b, (((1,), (0,)), ((), ())), preferred_element_type=F32)


def dot_nt(a, b):
    return lax.dot_general(a, b, (((1,), (1,)), ((), ())), preferred_element_type=F32)


def dot_tn(a, b):
    return lax.dot_general(a, b, (((0,), (0,)), ((), ())), preferred_element_type=F32)


def loop(n, body, first=0):
    lax.fori_loop(first, n, lambda i, c: (body(i), c)[1], 0)


def unrolled(n, body):
    for i in range(n):
        body(i)


def mega(
    cfg,
    times_ref,
    mask_ref,
    vector_ref,
    gains_ref,
    emb_hbm,
    cot_hbm,
    table_hbm,
    wq_hbm,
    wp_hbm,
    wi_hbm,
    wo_hbm,
    act_out,
    dx_out,
    grad_out,
    small_hbm,
    table_hbm_out,
    w,
    h,
    mid,
    acc,
    tmp,
    inv_sum,
    normed,
    mixed,
    n2,
    actv,
    gp,
    packed,
    probs,
    glow,
    dmlow,
    dpk,
    do_ref,
    outb,
    relay,
    maskc,
    trow,
    pay,
    sums,
    cbuf,
    ybuf,
    z1,
    z2,
    in_sem,
    own_sem,
    gsend,
    grecv,
    nrecv,
    rsend,
    rrecv,
    csend,
    crecv,
    ysend,
    yrecv,
    zsend,
    zrecv,
    zout,
    psend,
    precv,
    osem,
    small_out,
    table_out,
    *extra,
):
    count, seq, width, nz, unit = cfg
    quarter = width // 4
    units = CHUNKS * quarter // unit
    per_block = quarter // unit
    table_rows = table_hbm.shape[0]
    s = lax.axis_index("section")
    g = lax.axis_index("grp")
    d = lax.axis_index("dp")
    x0 = s == 0
    x1 = jnp.logical_not(x0)
    c = lax.rem(g, 2)
    y = g // 2
    twin = g + 1 - 2 * c
    across = lax.rem(g + 2, 4)
    zpair = d + 1 - 2 * lax.rem(d, 2)
    zfar = lax.rem(d + 2, 4)
    half = lax.rem(d, 2)

    peers = [{"section": 1 - s}, {"grp": twin}, {"grp": across}, {"dp": zpair}]
    if nz == 4:
        peers += [{"dp": 3 - d}, {"dp": zfar}]
    barrier = pltpu.get_barrier_semaphore()
    for peer in peers:
        pl.semaphore_signal(barrier, inc=1, device_id=peer, device_id_type=MESH)

    def remote(src, dst, send, recv, peer):
        return pltpu.make_async_remote_copy(
            src_ref=src, dst_ref=dst, send_sem=send, recv_sem=recv, device_id=peer, device_id_type=MESH
        )

    def rows(start, size, by):
        return pl.ds(pl.multiple_of(start, by), size)

    def place(i, q):
        return jnp.where(i < IN0, q * width + quarter * i, i * width + quarter * q)

    def source(i):
        if i < IN0:
            return wo_hbm.at[pl.ds(i * quarter, quarter)]
        if i < PROJ:
            return wi_hbm.at[:, pl.ds((i - IN0) * width, width)]
        if i == PROJ:
            return wp_hbm
        return wq_hbm.at[:, pl.ds((i - QKV0) * width, width)]

    sixth = quarter // 6
    share = {0: 2, 1: 3}
    far = across

    group_size = (4, 4, 1, 3)

    def group_of(i):
        if isinstance(i, int):
            return i // 4 if i < PROJ else 2 + (i > PROJ)
        return jnp.where(i < PROJ, i // 4, jnp.where(i == PROJ, 2, 3))

    def piece(i, q, first, n):
        return w.at[rows(place(i, q) + first * sixth, n * sixth, sixth)]

    def stage(k, i):
        return dpk.at[rows((k * CHUNKS + i) * sixth, sixth, sixth)]

    def own_copy(i):
        return pltpu.make_async_copy(source(i), w.at[rows(place(i, g), quarter, sixth)], own_sem.at[group_of(i)])

    def own_to_twin(i):
        return remote(source(i), w.at[rows(place(i, g), quarter, sixth)], gsend.at[0], nrecv.at[0, group_of(i)], {"grp": twin})

    def own_across(i, n):
        return remote(
            source(i).at[rows(half * n * sixth, n * sixth, sixth)],
            piece(i, g, half * n, n),
            gsend.at[1],
            grecv.at[0, i],
            {"grp": across},
        )

    def own_across_sixth(i, p):
        r = half * share[1] + p
        return remote(
            source(i).at[rows(r * sixth, sixth, sixth)], piece(i, g, r, 1), gsend.at[1], grecv.at[0, i], {"grp": across}
        )

    def own_over(i):
        return remote(
            source(i).at[rows((4 + half) * sixth, sixth, sixth)],
            stage(0, i),
            gsend.at[5],
            grecv.at[2, i],
            {"section": 1 - s},
        )

    def y_part(i, n):
        return piece(i, far, half * n, n)

    def z_part(i, n):
        return piece(i, far, (1 - half) * n, n)

    def y_to_z(i, n):
        return remote(y_part(i, n), y_part(i, n), gsend.at[2], grecv.at[1, i], {"dp": zpair})

    def y_to_twin(i, n):
        return remote(y_part(i, n), y_part(i, n), gsend.at[3], nrecv.at[1, group_of(i)], {"grp": twin})

    def z_to_twin(i, n):
        return remote(z_part(i, n), z_part(i, n), gsend.at[4], nrecv.at[2, group_of(i)], {"grp": twin})

    def over_to_twin(i):
        both = piece(i, far, 4, 2)
        return remote(both, both, gsend.at[6], nrecv.at[3, group_of(i)], {"grp": twin})

    def wait_for(ref, sem):
        remote(ref, ref, gsend.at[0], sem, {"grp": twin}).wait_recv()

    def stage_across(i):
        return remote(stage(0, i), stage(1, i), gsend.at[5], grecv.at[3, i], {"grp": across})

    def stage_to_z(i):
        return remote(stage(1, i), stage(2, i), gsend.at[7], grecv.at[4, i], {"dp": zpair})

    def stage_back(k, i):
        which = half if k == 1 else 1 - half
        return remote(stage(k, i), piece(i, far, 4 + which, 1), gsend.at[6], grecv.at[2, i], {"section": 1 - s})

    def bulk(n, send, recv, peer):
        return remote(w.at[pl.ds(0, n)], w.at[pl.ds(0, n)], send, recv, peer)

    def near_ready(k):
        n = group_size[k] * quarter
        bulk(n, gsend.at[0], nrecv.at[0, k], {"grp": twin}).wait_recv()
        pltpu.make_async_copy(w.at[pl.ds(0, n)], w.at[pl.ds(0, n)], own_sem.at[k]).wait()

    def far_ready(k, section):
        n = group_size[k] * share[section] * sixth
        bulk(n, gsend.at[3], nrecv.at[1, k], {"grp": twin}).wait_recv()
        bulk(n, gsend.at[4], nrecv.at[2, k], {"grp": twin}).wait_recv()
        if section == 0:
            bulk(group_size[k] * 2 * sixth, gsend.at[6], nrecv.at[3, k], {"grp": twin}).wait_recv()

    def all_ready(k, section):
        near_ready(k)
        far_ready(k, section)

    def gather_order(k):
        return jnp.where(k < 3, QKV0 + k, jnp.where(k == 3, PROJ, jnp.where(k < 8, k, k - 8)))

    def when_block(k, body):
        pl.when(jnp.logical_and(k >= 0, k < CHUNKS))(lambda: body(gather_order(k)))

    zlag, overlag = 2, 5
    ylag, backlag = 2, 4

    def pass_on(k, section):
        n = share[section]

        def from_y(i):
            wait_for(y_part(i, n), grecv.at[0, i])
            y_to_z(i, n).start()
            y_to_twin(i, n).start()

        def from_z(i):
            wait_for(z_part(i, n), grecv.at[1, i])
            z_to_twin(i, n).start()

        when_block(k, from_y)
        when_block(k - zlag, from_z)

    def gather_step(k):
        def from_over(i):
            wait_for(piece(i, far, 4, 2), grecv.at[2, i])
            over_to_twin(i).start()

        pass_on(k, 0)
        when_block(k - overlag, from_over)

    def second_step(k):
        pass_on(k, 1)

    early_blocks = 1 + CHUNKS // share[1]

    def start_sixth(k):
        for m, i in enumerate(GATHER_ORDER[:early_blocks]):
            pl.when(k // share[1] == m)(lambda: own_across_sixth(i, lax.rem(k, share[1])).start())

    def help_step(k):
        def from_x(i):
            wait_for(stage(0, i), grecv.at[2, i])
            stage_across(i).start()

        def from_y(i):
            wait_for(stage(1, i), grecv.at[3, i])
            stage_back(1, i).start()
            stage_to_z(i).start()

        def from_z(i):
            wait_for(stage(2, i), grecv.at[4, i])
            stage_back(2, i).start()

        when_block(k, from_x)
        when_block(k - ylag, from_y)
        when_block(k - backlag, from_z)

    def load(src, dst, k):
        return pltpu.make_async_copy(src, dst, in_sem.at[k])

    table_copy = load(table_hbm, dpk.at[pl.ds(0, table_rows)], 0)
    emb_copy = load(emb_hbm, outb, 1)

    def cot_copy(mb):
        return load(cot_hbm.at[mb], glow.at[rows(mb * seq, seq, seq)], 2 + mb)

    @pl.when(x0)
    def _():
        table_copy.start()
        emb_copy.start()

    @pl.when(x1)
    def _():
        for mb in range(2):
            cot_copy(mb).start()

    for i in GATHER_ORDER:
        own_copy(i).start()
    sums[...] = jnp.zeros_like(sums)
    for mb in range(2):
        maskc[mb] = jnp.transpose(jnp.broadcast_to(mask_ref[mb : mb + 1, :].astype(F32), (128, seq)))

    def enter():
        pl.semaphore_wait(barrier, len(peers))

    enter()

    def issue():
        @pl.when(x0)
        def _():
            for i in GATHER_ORDER:
                own_across(i, share[0]).start()
                own_over(i).start()

        @pl.when(x1)
        def _():
            own_across(GATHER_ORDER[0], share[1]).start()

        for i in GATHER_ORDER:
            own_to_twin(i).start()

    issue()

    def chunk(k):
        return w[rows(k * width, width, width), :]

    step_rows = 32
    parts_of = seq // step_rows
    lane = lax.broadcasted_iota(jnp.int32, (1, 128), 1)
    low_lane = lax.broadcasted_iota(jnp.int32, (seq, 128), 1) < HEAD
    low_half = (lane < HEAD).astype(F32)
    masks = (low_half.astype(BF), (1.0 - low_half).astype(BF))
    scaled = ((low_half * 0.125).astype(BF), ((1.0 - low_half) * 0.125).astype(BF))

    def seq_rows(mb):
        return rows(mb * seq, seq, seq)

    def sub_rows(mb, r):
        return rows(mb * seq + r * step_rows, step_rows, step_rows)

    def r_rows(r):
        return rows(r * step_rows, step_rows, step_rows)

    def norm_parts(v):
        center = v - jnp.mean(v, axis=-1, keepdims=True)
        spread = jnp.mean(center * center, axis=-1, keepdims=True)
        inv = lax.rsqrt(spread + EPS)
        return center * inv, inv

    @pl.when(x1)
    def _():
        def help_and_gather(k):
            help_step(k)
            pl.when(k < CHUNKS)(lambda: start_sixth(k + share[1]))
            pl.when(lax.rem(k, 3) == 1)(lambda: second_step(k // 3))

        loop(CHUNKS, help_and_gather)
        for i in GATHER_ORDER[early_blocks:]:
            own_across(i, share[1]).start()
        loop(CHUNKS + backlag, help_and_gather, CHUNKS)
        loop(11, second_step, early_blocks)
        all_ready(3, 1)
        all_ready(2, 1)

    @pl.when(x0)
    def _():
        table_copy.wait()
        emb_copy.wait()
        ids = lax.broadcasted_iota(jnp.int32, (8, table_rows), 1)
        pick = lax.broadcasted_iota(jnp.int32, (8, table_rows), 0)
        want = jnp.where(pick == 0, times_ref[0], times_ref[1])
        hot = jnp.where(jnp.logical_and(pick < 2, ids == want), 1.0, 0.0).astype(BF)
        trow[...] = dot_nn(hot, dpk[pl.ds(0, table_rows), :])
        vector = vector_ref[...].astype(F32).reshape(1, width)
        for mb in range(2):

            def make(r):
                m = maskc[mb, r_rows(r), 0:1]
                base = jnp.where(m > 0.5, vector, outb[mb, r_rows(r), :].astype(F32))
                h[mb, r_rows(r), :] = base + trow[mb : mb + 1, :]

            loop(parts_of, make)

    def more(mb, t, k):
        @pl.when(x0)
        def _():
            if k < 2:
                gather_step(8 + 2 * t + k)
            else:
                pl.when(t == 1)(lambda: gather_step(12))

        if k < 2:
            pl.when(jnp.logical_and(x1, t == 0))(lambda: second_step(11 + k))

    def first_half(mb, t):
        @pl.when(x1)
        def _():
            h[mb] = relay[mb].astype(F32)

        def ln(r):
            xhat, _ = norm_parts(h[mb, r_rows(r), :])
            normed[sub_rows(mb, r), :] = (xhat * gains_ref[0:1, :]).astype(BF)

        unrolled(parts_of, ln)

        @pl.when(jnp.logical_and(x0, t == 0))
        def _():
            loop(8, gather_step)
            all_ready(3, 0)

        def qkv(k):
            packed[k, seq_rows(mb), :] = dot_nn(normed[seq_rows(mb), :], chunk(QKV0 + k)).astype(BF)

        unrolled(3, qkv)

        more(mb, t, 0)

        def attend(j):
            cols = pl.ds(j * 128, 128)
            q2 = packed[0, seq_rows(mb), cols]
            k2 = packed[1, seq_rows(mb), cols]
            v2 = packed[2, seq_rows(mb), cols]
            got = []
            for e in range(2):
                sc = dot_nt(q2 * scaled[e], k2)
                ex = jnp.exp(sc - jnp.max(sc, axis=-1, keepdims=True)).astype(BF)
                probs[mb, 2 * j + e] = ex
                got.append(dot_nn(ex, v2 * masks[e] + masks[1 - e]))
            inv = 1.0 / pltpu.roll(jnp.where(low_lane, got[1], got[0]), HEAD, 1)
            inv_sum[mb, :, cols] = inv
            mixed[seq_rows(mb), cols] = (jnp.where(low_lane, got[0], got[1]) * inv).astype(BF)

        unrolled(HEADS // 2, attend)

        more(mb, t, 1)

        pl.when(jnp.logical_and(x0, t == 0))(lambda: all_ready(2, 0))
        mid[mb] = h[mb] + dot_nn(mixed[seq_rows(mb), :], chunk(PROJ))

        def ln_two(r):
            xhat, _ = norm_parts(mid[mb, r_rows(r), :])
            n2[sub_rows(mb, r), :] = (xhat * gains_ref[1:2, :]).astype(BF)

        unrolled(parts_of, ln_two)
        more(mb, t, 2)

    def mlp_up(q, mb):
        lhs = n2[seq_rows(mb), :]
        piece = 256
        chunk_rows = rows((IN0 + q) * width, width, width)

        def product(j):
            return dot_nn(lhs, w[chunk_rows, pl.ds(j * piece, piece)])

        up = product(0)
        for j in range(width // piece):
            after = product(j + 1) if (j + 1) * piece < width else None
            cols = pl.ds(j * piece, piece)
            sq = up * up
            hp = 0.5 + 0.5 * jnp.tanh(up * (GELU_C + (GELU_C * 0.044715) * sq))
            act = up * hp
            actv[q, seq_rows(mb), cols] = act.astype(BF)
            gp[q, seq_rows(mb), cols] = (
                hp + act * ((1.0 - hp) * (2.0 * GELU_C + (2.0 * GELU_C * 0.134145) * sq))
            ).astype(BF)
            up = after

    def mlp_down(q, mb):
        acc[mb] += dot_nn(actv[q, seq_rows(mb), :], chunk(OUT0 + q))

    def second_half_one(mb, t):
        def at_first(body):
            pl.when(t == 0)(body)

        at_first(lambda: all_ready(1, 1))
        for q in range(4):
            mlp_up(q, mb)
        acc[mb] = mid[mb]
        at_first(lambda: near_ready(0))
        for r in range(2):
            mlp_down(2 * y + r, mb)

        @at_first
        def _():
            second_step(13)
            far_ready(0, 1)
            for k, n in ((5, 1), (6, 2), (7, 1)):
                bulk(CHUNKS * n * sixth, gsend.at[k], grecv.at[0, 0], {"grp": twin}).wait_send()

        for r in range(2):
            mlp_down(2 * (1 - y) + r, mb)
        outb[mb] = acc[mb].astype(BF)

    def second_half_both():
        all_ready(1, 0)

        def up(q):
            mlp_up(q, 0)
            gather_step(13 + q)

        def finish(mb):
            outb[mb] = acc[mb].astype(BF)
            relay_copy(mb, 0).start()
            relay_copy(mb, 1).start()
            act_copy(mb).start()

        loop(4, up)
        acc[...] = mid[...]
        near_ready(0)
        loop(2, lambda r: mlp_down(2 * y + r, 0))
        far_ready(0, 0)
        loop(2, lambda r: mlp_down(2 * (1 - y) + r, 0))
        finish(0)
        for q in range(4):
            mlp_up(q, 1)
            mlp_down(q, 1)
        finish(1)

    def relay_copy(mb, part):
        r = pl.ds(part * (seq // 2), seq // 2)
        return remote(
            outb.at[mb, r], relay.at[mb, r], rsend.at[mb, part], rrecv.at[mb, part], {"section": 1 - s}
        )

    def act_copy(mb):
        return pltpu.make_async_copy(outb.at[mb], act_out.at[mb], osem.at[0, mb])

    def dx_copy(mb):
        return pltpu.make_async_copy(h.at[mb], dx_out.at[mb], osem.at[1, mb])

    def norm_back(v, gain, dy):
        xhat, inv = norm_parts(v)
        dxh = dy * gain
        m1 = jnp.mean(dxh, axis=-1, keepdims=True)
        m2 = jnp.mean(dxh * xhat, axis=-1, keepdims=True)
        return inv * (dxh - m1 - xhat * m2), jnp.sum(dy * xhat, axis=0, keepdims=True)

    def backward_mlp(mb, t):
        @pl.when(x0)
        def _():
            glow[seq_rows(mb), :] = relay[mb]

        @pl.when(x1)
        def _():
            cot_copy(mb).wait()

        tmp[...] = jnp.zeros_like(tmp)

        def slope(q):
            da = dot_nt(glow[seq_rows(mb), :], chunk(OUT0 + q))
            du = (gp[q, seq_rows(mb), :].astype(F32) * da).astype(BF)
            gp[q, seq_rows(mb), :] = du
            return du

        def back_up(q):
            tmp[...] += dot_nt(gp[q, seq_rows(mb), :], chunk(IN0 + q))

        def mlp(q):
            tmp[...] += dot_nt(slope(q), chunk(IN0 + q))

        def slope_and_out(k):
            slope(out_order(k))
            out_terms(k)

        last = jnp.logical_and(x0, t == 3)

        @pl.when(last)
        def _():
            loop(4, slope_and_out)
            loop(4, back_up)

        pl.when(jnp.logical_not(last))(lambda: unrolled(4, mlp))

        def ln_two(r):
            dx, dg = norm_back(mid[mb, r_rows(r), :], gains_ref[1:2, :], tmp[r_rows(r), :])
            dm = glow[sub_rows(mb, r), :].astype(F32) + dx
            mid[mb, r_rows(r), :] = dm
            dmlow[sub_rows(mb, r), :] = dm.astype(BF)
            sums[1:2, :] += dg

        unrolled(parts_of, ln_two)

    def backward_attention(mb, t):
        do_ref[...] = (dot_nt(dmlow[seq_rows(mb), :], chunk(PROJ)) * inv_sum[mb]).astype(BF)

        def attend(j):
            cols = pl.ds(j * 128, 128)
            q2 = packed[0, seq_rows(mb), cols]
            k2 = packed[1, seq_rows(mb), cols]
            v2 = packed[2, seq_rows(mb), cols]
            do2 = do_ref[:, cols]
            weighed = do2.astype(F32) * mixed[seq_rows(mb), cols].astype(F32)
            dq = jnp.zeros((seq, 128), F32)
            dk = jnp.zeros((seq, 128), F32)
            dv = jnp.zeros((seq, 128), F32)
            for e in range(2):
                ex = probs[mb, 2 * j + e]
                dom = do2 * masks[e]
                inner = jnp.sum(jnp.where(low_lane if e == 0 else jnp.logical_not(low_lane), weighed, 0.0), axis=-1, keepdims=True)
                ds = (ex.astype(F32) * (dot_nt(dom, v2) - inner)).astype(BF)
                dv = dv + dot_tn(ex, dom)
                dq = dq + dot_nn(ds, k2 * scaled[e])
                dk = dk + dot_tn(ds, q2 * scaled[e])
            for k, v in enumerate((dq, dk, dv)):
                dpk[rows(k * 2 * seq + mb * seq, seq, seq), cols] = v.astype(BF)

        for j in range(HEADS // 2):
            attend(j)

        early_tick(t, 5)
        early_tick(t, 6)
        tmp[...] = jnp.zeros_like(tmp)

        def qkv(k):
            tmp[...] += dot_nt(dpk[rows(k * 2 * seq + mb * seq, seq, seq), :], chunk(QKV0 + k))

        unrolled(3, qkv)
        early_tick(t, 7)
        act_copy(mb).wait()

        @pl.when(x0)
        def _():
            for part in range(2):
                relay_copy(mb, part).wait_send()

        for part in range(2):

            def ln_one(rr):
                r = rr + part * (parts_of // 2)
                dx, dg = norm_back(h[mb, r_rows(r), :], gains_ref[0:1, :], tmp[r_rows(r), :])
                dm = mid[mb, r_rows(r), :] + dx
                outb[mb, r_rows(r), :] = dm.astype(BF)
                sums[0:1, :] += dg
                m = maskc[mb, r_rows(r), 0:1]
                kept = jnp.where(jnp.logical_and(x0, m > 0.5), 0.0, dm)
                h[mb, r_rows(r), :] = kept
                sums[pl.ds(2 + mb, 1), :] += jnp.sum(dm, axis=0, keepdims=True)
                sums[4:5, :] += jnp.sum(dm - kept, axis=0, keepdims=True)

            unrolled(parts_of // 2, ln_one)

            @pl.when(x1)
            def _():
                relay_copy(mb, part).start()

        dx_copy(mb).start()
        early_tick(t, 8)

    def grad_chunk(a, b, k):
        w[rows(k * width, width, width), :] = dot_tn(a, b).astype(BF)

    def cslot(i, yy):
        return cbuf.at[yy, rows(i * quarter, quarter, quarter)]

    def to_twin(i, yy):
        q = 2 * yy + (1 - c)
        return remote(
            w.at[rows(place(i, q), quarter, quarter)], cslot(i, yy), csend.at[yy], crecv.at[arrival(i, yy)], {"grp": twin}
        )

    def arrival(i, yy):
        return jnp.where(jnp.logical_and(yy == 1 - y, i < IN0), 6 + i, 3 * yy + i // 4)

    def from_twin(k, yy):
        ref = cbuf.at[yy, rows(4 * k * quarter, 4 * quarter, quarter)]
        remote(ref, ref, csend.at[yy], crecv.at[3 * yy + k], {"grp": twin}).wait_recv()

    def urows(u):
        return rows(u * unit, unit, unit)

    def y_send(u):
        k = lax.rem(u, YRING)
        return remote(
            cbuf.at[1 - y, urows(u)], ybuf.at[urows(u)], ysend.at[k], yrecv.at[k], {"grp": across}
        )

    def merge_far(i):
        pl.when(i < IN0)(lambda: wait_for(cslot(i, 1 - y), crecv.at[arrival(i, 1 - y)]))
        pl.when(jnp.logical_and(i >= IN0, lax.rem(i, 4) == 0))(lambda: from_twin(i // 4, 1 - y))
        part = rows(i * quarter, quarter, quarter)
        mine = w[rows(place(i, 2 * (1 - y) + c), quarter, quarter), :].astype(F32)
        cbuf[1 - y, part, :] = (cbuf[1 - y, part, :].astype(F32) + mine).astype(BF)

    ahead = 6

    def send_across(u):
        pl.when(lax.rem(u, per_block) == 0)(lambda: merge_far(u // per_block))
        pl.when(u >= YRING)(lambda: y_send(u - YRING).wait_send())
        y_send(u).start()

    def out_order(k):
        side = jnp.where(k < 2, 1 - y, y)
        return 2 * side + jnp.where(lax.rem(k, 2) == 0, 1 - c, c)

    def out_terms(k):
        q = out_order(k)
        grad_chunk(actv[q], glow[...], OUT0 + q)

        @pl.when(lax.rem(k, 2) == 0)
        def _():
            loop(4, lambda i: to_twin(i, jnp.where(k == 0, 1 - y, y)).start())

        @pl.when(k == 1)
        def _():
            loop(ahead, send_across)

    def other_terms(i, a, b):
        grad_chunk(a, b, i)
        to_twin(i, 1 - y).start()
        to_twin(i, y).start()

    def in_terms():
        early_tick_now(0)

        def one(q):
            other_terms(IN0 + q, n2[...], gp[q])
            early_tick_now(1 + q)

        loop(4, one)

    def attention_terms():
        first = jnp.where(x0, 9, 5)
        other_terms(PROJ, mixed[...], dmlow[...])
        early_tick_now(first)

        def one(k):
            other_terms(QKV0 + k, normed[...], dpk[rows(k * 2 * seq, 2 * seq, 2 * seq), :])
            early_tick_now(first + 1 + k)

        loop(3, one)

    def add_rows(dst, dst_rows, *terms):
        dst[dst_rows, :] = functools.reduce(jnp.add, [a.astype(F32) for a in terms]).astype(BF)

    def sum_across(u):
        i = u // per_block
        pl.when(lax.rem(u, 4 * per_block) == 0)(lambda: from_twin(i // 4, y))
        y_send(u).wait_recv()
        mine = w[rows(place(i, g) + lax.rem(u, per_block) * unit, unit, unit), :]
        add_rows(ybuf, urows(u), cbuf[y, urows(u), :], mine, ybuf[urows(u), :])

    first_tick = jnp.where(x0, 13, 9)
    if nz == 4:
        end = jnp.logical_or(d == 0, d == 3)
        inner = jnp.logical_not(end)
        slots, landed = extra
        pay_copy = remote(pay, landed.at[0], psend.at[0], precv.at[0], {"section": 1 - s})
        last_part = pl.ds(8, 8)

        sums_rows = pl.ds(nz * 8, 8)

        def small_copy(k):
            peer = ({"grp": twin}, {"grp": across}, {"dp": zpair}, {"dp": zfar})[k]
            part = pl.ds(0, 16) if k < 3 else last_part
            return remote(pay.at[part], landed.at[1 + k, part], psend.at[1 + k], precv.at[1 + k], peer)

        pair_rows = rows((d // 2) * 16, 16, 16)
        far_rows = rows((1 - d // 2) * 16, 16, 16)
        pair_copy = remote(slots.at[pair_rows], slots.at[pair_rows], psend.at[5], precv.at[5], {"dp": zfar})
        pair_wait = remote(slots.at[far_rows], slots.at[far_rows], psend.at[5], precv.at[5], {"dp": zfar})
        give_back = remote(slots, slots, psend.at[6], precv.at[6], {"section": 1 - s})

        def small_start():
            pay_copy.wait_recv()
            pay[0:8, :] = landed[0, 0:8, :]
            row = lax.broadcasted_iota(jnp.int32, (8, width + 128), 0)
            other = landed[0, last_part, :]
            pay[last_part, :] = jnp.where(
                row < 2, pay[last_part, :], jnp.where(row == 2, other, pltpu.roll(other, 3, 0))
            )
            small_copy(0).start()

        def small_next(k):
            small_copy(k).wait_recv()
            small_copy(k).wait_send()
            if k < 2:
                pay[...] = pay[...] + landed[1 + k]
                if k == 1:
                    slots[rows(d * 8, 8, 8), :] = pay[0:8, :]
                small_copy(k + 1).start()
            else:
                slots[rows(zpair * 8, 8, 8), :] = landed[3, 0:8, :]
                pay[last_part, :] = pay[last_part, :] + landed[3, last_part, :]
                small_copy(3).start()
                pair_copy.start()

        def small_end():
            small_copy(3).wait_recv()
            small_copy(3).wait_send()
            pair_wait.wait_recv()
            slots[sums_rows, :] = pay[last_part, :] + landed[4, last_part, :]
            give_back.start()

        def small_results():
            pl.when(x0)(lambda: give_back.wait_recv())
            total = slots[sums_rows, 0:width]
            shard = s * 4 + g
            mine = jnp.where(x0, pltpu.roll(total, 5, 0), total)
            small_out[0:8, :] = pltpu.roll(mine, lax.rem(width - quarter * g, width), 1)
            small_out[8:16, :] = pltpu.roll(total, lax.rem(width - (width // 8) * shard, width), 1)
            base = shard * (table_rows // 8) + 1
            ids = (base + lax.broadcasted_iota(jnp.int32, (nz * 8, 128), 1)).astype(F32)
            pick = jnp.where(slots[0 : nz * 8, pl.ds(width, 128)] == ids, 1.0, 0.0).astype(BF)
            rest = slots[0 : nz * 8, 0:width]
            found = jnp.zeros((128, width), F32)
            for _ in range(3):
                part = rest.astype(BF)
                found = found + dot_tn(pick, part)
                rest = rest - part.astype(F32)
            table_out[...] = found
            small_leaves()

        def zcopy(src, dst, k, u, peer):
            m = lax.rem(u, ZRING)
            return remote(src.at[urows(u)], dst.at[urows(u)], zsend.at[k, m], zrecv.at[k, m], peer)

        def end_to_inner(u):
            return zcopy(ybuf, z1, 0, u, {"dp": zpair})

        def inner_swap(u):
            return zcopy(z1, z2, 1, u, {"dp": 3 - d})

        def inner_to_end(u):
            return zcopy(z2, z1, 0, u, {"dp": zpair})

        def grad_copy(src, u):
            return pltpu.make_async_copy(src.at[urows(u)], grad_out.at[urows(u)], zout.at[lax.rem(u, ZRING)])

        def launch(copy, u):
            pl.when(u >= ZRING)(lambda: copy(u - ZRING).wait_send())
            copy(u).start()

        def put_out(src, u):
            pl.when(u >= ZRING)(lambda: grad_copy(src, u - ZRING).wait())
            grad_copy(src, u).start()

        lag3, lag4, lag5 = 3, 6, 9
        first_small, small_gap = 16, 6

        def tick(t, small=True):
            u2, u3, u4, u5 = t, t - lag3, t - lag4, t - lag5
            pl.when(u2 + ahead < units)(lambda: send_across(u2 + ahead))

            @pl.when(u2 < units)
            def _():
                sum_across(u2)

                @pl.when(end)
                def _():
                    launch(end_to_inner, u2)

            @pl.when(jnp.logical_and(inner, jnp.logical_and(u3 >= 0, u3 < units)))
            def _():
                end_to_inner(u3).wait_recv()
                add_rows(z1, urows(u3), ybuf[urows(u3), :], z1[urows(u3), :])
                launch(inner_swap, u3)

            @pl.when(jnp.logical_and(inner, jnp.logical_and(u4 >= 0, u4 < units)))
            def _():
                inner_swap(u4).wait_recv()
                add_rows(z2, urows(u4), z1[urows(u4), :], z2[urows(u4), :])
                launch(inner_to_end, u4)
                put_out(z2, u4)

            @pl.when(jnp.logical_and(end, jnp.logical_and(u5 >= 0, u5 < units)))
            def _():
                inner_to_end(u5).wait_recv()
                put_out(z1, u5)

            if not small:
                return
            pl.when(t == jnp.where(x1, units, units + 2))(small_results)

            @pl.when(x1)
            def _():
                pl.when(t == first_small)(small_start)
                for k in range(3):
                    pl.when(t == first_small + small_gap * (k + 1))(functools.partial(small_next, k))
                pl.when(t == first_small + small_gap * 4)(small_end)

    else:

        def out_sum(u):
            return pltpu.make_async_copy(ybuf.at[urows(u)], grad_out.at[urows(u)], zout.at[lax.rem(u, ZRING)])

        def tick(u, small=True):
            pl.when(u + ahead < units)(lambda: send_across(u + ahead))
            sum_across(u)
            pl.when(u >= ZRING)(lambda: out_sum(u - ZRING).wait())
            out_sum(u).start()

    def early_tick_now(t):
        tick(t, False)

    def early_tick(t, k):
        pl.when(jnp.logical_and(x0, t == 3))(lambda: early_tick_now(k))

    leaving = (
        pltpu.make_async_copy(small_out, small_hbm, osem.at[0, 2]),
        pltpu.make_async_copy(table_out, table_hbm_out, osem.at[1, 2]),
    )

    def small_leaves():
        for copy in leaving:
            copy.start()

    def step(t):
        mb = jnp.where(x0, lax.rem(t, 2), t // 2)
        is_f = jnp.where(x0, t < 2, lax.rem(t, 2) == 0)

        @pl.when(is_f)
        def _():
            @pl.when(x1)
            def _():
                relay_copy(mb, 0).wait_recv()
                relay_copy(mb, 1).wait_recv()

            first_half(mb, t)

            pl.when(jnp.logical_and(x0, t == 1))(second_half_both)

            @pl.when(x1)
            def _():
                second_half_one(mb, t)
                act_copy(mb).start()

        @pl.when(jnp.logical_not(is_f))
        def _():
            @pl.when(x0)
            def _():
                for part in range(2):
                    relay_copy(mb, part).wait_recv()

            @pl.when(jnp.logical_and(x0, t == 3))
            def _():
                gather_sent(0)

            backward_mlp(mb, t)

            @pl.when(jnp.logical_and(x0, t == 3))
            def _():
                in_terms()

            backward_attention(mb, t)

    def gather_sent(section):
        bulk(CHUNKS * quarter, gsend.at[0], nrecv.at[0, 0], {"grp": twin}).wait_send()
        n = CHUNKS * share[section] * sixth
        for k in range(1, 5):
            bulk(n, gsend.at[k], grecv.at[0, 0], {"grp": twin}).wait_send()
        if section == 0:
            for k, n in ((5, 1), (6, 2)):
                bulk(CHUNKS * n * sixth, gsend.at[k], grecv.at[0, 0], {"grp": twin}).wait_send()

    loop(4, step)

    @pl.when(x1)
    def _():
        gather_sent(1)
        loop(4, out_terms)
        in_terms()

    row_ids = lax.broadcasted_iota(jnp.int32, (8, width), 0)
    stamp_ids = lax.broadcasted_iota(jnp.int32, (8, 128), 0)
    first = 2 * g
    pay[0:8, 0:width] = jnp.where(
        row_ids == first, sums[2:3, :], jnp.where(row_ids == first + 1, sums[3:4, :], 0.0)
    )
    pay[0:8, pl.ds(width, 128)] = jnp.where(
        stamp_ids == first,
        (times_ref[0] + 1).astype(F32),
        jnp.where(stamp_ids == first + 1, (times_ref[1] + 1).astype(F32), 0.0),
    )
    pay[8:16, 0:width] = jnp.where(
        row_ids < 2, sums[...], jnp.where(row_ids == 2, sums[4:5, :], 0.0)
    )
    pay[8:16, pl.ds(width, 128)] = jnp.zeros((8, 128), F32)

    if nz == 4:
        pl.when(x0)(lambda: pay_copy.start())

    attention_terms()

    if nz == 4:
        loop(units + lag5, tick, first_tick)

        loop(units, lambda u: y_send(u).wait_send(), units - YRING)

        def drain(u):
            @pl.when(end)
            def _():
                end_to_inner(u).wait_send()
                grad_copy(z1, u).wait()

            @pl.when(inner)
            def _():
                inner_swap(u).wait_send()
                inner_to_end(u).wait_send()
                grad_copy(z2, u).wait()

        loop(units, drain, units - ZRING)

        pl.when(x0)(lambda: pay_copy.wait_send())

        @pl.when(x1)
        def _():
            pair_copy.wait_send()
            give_back.wait_send()

    else:
        small_out[...] = pay[...]
        table_out[...] = jnp.zeros_like(table_out)
        small_leaves()
        loop(units, tick, first_tick)

        loop(units, lambda u: y_send(u).wait_send(), units - YRING)
        loop(units, lambda u: out_sum(u).wait(), units - ZRING)

    for yy in range(2):
        bulk(CHUNKS * quarter, csend.at[yy], crecv.at[0], {"grp": twin}).wait_send()

    for copy in leaving:
        copy.wait()
    for mb in range(2):
        dx_copy(mb).wait()

        @pl.when(x1)
        def _():
            for part in range(2):
                relay_copy(mb, part).wait_send()


def run_mega(timesteps, mask_flags, vector, gains, emb, cot, table, wq, wp, wi, wo, nz):
    count, seq, width = emb.shape
    quarter = wp.shape[0]
    unit = quarter // 4
    units = CHUNKS * quarter // unit
    tokens = count * seq
    assert count == 2 and quarter * 4 == width and wi.shape[1] == 4 * width and wo.shape[0] == width
    vmem = pl.BlockSpec(memory_space=pltpu.VMEM)
    smem = pl.BlockSpec(memory_space=pltpu.SMEM)
    hbm = pl.BlockSpec(memory_space=pl.ANY)
    dma = pltpu.SemaphoreType.DMA
    small = (16, width) if nz == 4 else (16, width + 128)
    extra = [pltpu.VMEM((nz * 8 + 8, width + 128), F32), pltpu.VMEM((5, 16, width + 128), F32)]
    return pl.pallas_call(
        functools.partial(mega, (count, seq, width, nz, unit)),
        out_shape=(
            jax.ShapeDtypeStruct((count, seq, width), BF),
            jax.ShapeDtypeStruct((count, seq, width), F32),
            jax.ShapeDtypeStruct((CHUNKS * quarter, width), BF),
            jax.ShapeDtypeStruct(small, F32),
            jax.ShapeDtypeStruct((128, width), F32),
        ),
        in_specs=[smem, vmem, vmem, vmem] + [hbm] * 7,
        out_specs=(hbm,) * 5,
        scratch_shapes=[
            pltpu.VMEM((CHUNKS * width, width), BF),
            pltpu.VMEM((count, seq, width), F32),
            pltpu.VMEM((count, seq, width), F32),
            pltpu.VMEM((count, seq, width), F32),
            pltpu.VMEM((seq, width), F32),
            pltpu.VMEM((count, seq, width), F32),
            pltpu.VMEM((tokens, width), BF),
            pltpu.VMEM((tokens, width), BF),
            pltpu.VMEM((tokens, width), BF),
            pltpu.VMEM((4, tokens, width), BF),
            pltpu.VMEM((4, tokens, width), BF),
            pltpu.VMEM((3, tokens, width), BF),
            pltpu.VMEM((count, HEADS, seq, seq), BF),
            pltpu.VMEM((tokens, width), BF),
            pltpu.VMEM((tokens, width), BF),
            pltpu.VMEM((3 * tokens, width), BF),
            pltpu.VMEM((seq, width), BF),
            pltpu.VMEM((count, seq, width), BF),
            pltpu.VMEM((count, seq, width), BF),
            pltpu.VMEM((count, seq, 128), F32),
            pltpu.VMEM((8, width), F32),
            pltpu.VMEM((16, width + 128), F32),
            pltpu.VMEM((8, width), F32),
            pltpu.VMEM((2, CHUNKS * quarter, width), BF),
            pltpu.VMEM((CHUNKS * quarter, width), BF),
            pltpu.VMEM((CHUNKS * quarter, width), BF),
            pltpu.VMEM((CHUNKS * quarter, width), BF),
            dma((4,)),
            dma((4,)),
            dma((8,)),
            dma((5, CHUNKS)),
            dma((4, 4)),
            dma((2, 2)),
            dma((2, 2)),
            dma((2,)),
            dma((10,)),
            dma((YRING,)),
            dma((YRING,)),
            dma((2, ZRING)),
            dma((2, ZRING)),
            dma((ZRING,)),
            dma((7,)),
            dma((7,)),
            dma((2, 3)),
            pltpu.VMEM(small, F32),
            pltpu.VMEM((128, width), F32),
        ]
        + (extra if nz == 4 else []),
        compiler_params=pltpu.CompilerParams(
            collective_id=0, has_side_effects=True, vmem_limit_bytes=67043328
        ),
        name="relay_layers",
    )(timesteps, mask_flags, vector, gains, emb, cot, table, wq, wp, wi, wo)


def place_results(
    act_in,
    dx_in,
    grads_in,
    small_ref,
    table_ref,
    act_out,
    dx_out,
    qkv_out,
    proj_out,
    in_out,
    out_out,
    gains_out,
    table_out,
    mask_out,
    act_buf,
    dx_buf,
    low_buf,
    wide_buf,
    ins,
    outs,
):
    quarter, width = proj_out.shape
    blocks = []
    for i in range(CHUNKS):
        part = pl.ds(i * quarter, quarter)
        if i < IN0:
            target = out_out.at[part]
        elif i < PROJ:
            target = in_out.at[:, pl.ds((i - IN0) * width, width)]
        elif i == PROJ:
            target = proj_out
        else:
            target = qkv_out.at[:, pl.ds((i - QKV0) * width, width)]
        blocks.append(
            (
                part,
                pltpu.make_async_copy(grads_in.at[part], low_buf.at[part], ins.at[i]),
                pltpu.make_async_copy(wide_buf.at[part], target, outs.at[i]),
            )
        )
    plain = [
        (
            pltpu.make_async_copy(dx_in, dx_buf, ins.at[CHUNKS]),
            pltpu.make_async_copy(dx_buf, dx_out, outs.at[CHUNKS]),
        ),
        (
            pltpu.make_async_copy(act_in, act_buf, ins.at[CHUNKS + 1]),
            pltpu.make_async_copy(act_buf, act_out, outs.at[CHUNKS + 1]),
        ),
    ]
    for _, come, _ in blocks:
        come.start()
    for come, _ in plain:
        come.start()
    for part, come, go in blocks:
        come.wait()
        wide_buf[part, :] = low_buf[part, :].astype(F32)
        go.start()
    for come, go in plain:
        come.wait()
        go.start()
    gains_out[...] = small_ref[0:2, 0:quarter]
    table_out[...] = table_ref[0 : table_out.shape[0], :]
    mask_out[...] = small_ref[10, 0 : mask_out.shape[0]]
    for _, _, go in blocks:
        go.wait()
    for _, go in plain:
        go.wait()


def run_place(activations, dx, grads, small, table, quarter, table_here, mask_here):
    count, seq, width = dx.shape
    vmem = pl.BlockSpec(memory_space=pltpu.VMEM)
    hbm = pl.BlockSpec(memory_space=pl.ANY)
    dma = pltpu.SemaphoreType.DMA
    shapes = (
        ((count, seq, width), BF),
        ((count, seq, width), F32),
        ((quarter, 3 * width), F32),
        ((quarter, width), F32),
        ((quarter, 4 * width), F32),
        ((width, width), F32),
        ((2, quarter), F32),
        ((table_here, width), F32),
        ((mask_here,), F32),
    )
    return pl.pallas_call(
        place_results,
        out_shape=tuple(jax.ShapeDtypeStruct(a, b) for a, b in shapes),
        in_specs=[hbm] * 3 + [vmem] * 2,
        out_specs=(hbm,) * 6 + (vmem,) * 3,
        scratch_shapes=[
            pltpu.VMEM((count, seq, width), BF),
            pltpu.VMEM((count, seq, width), F32),
            pltpu.VMEM((CHUNKS * quarter, width), BF),
            pltpu.VMEM((CHUNKS * quarter, width), F32),
            dma((CHUNKS + 2,)),
            dma((CHUNKS + 2,)),
        ],
        compiler_params=pltpu.CompilerParams(vmem_limit_bytes=64000000),
        name="place_results",
    )(activations, dx, grads, small, table)


def small_sums(sizes, small, timesteps, rows_count, quarter):
    ns, ng, nz = sizes
    width = quarter * 4
    section, member = lax.axis_index("section"), lax.axis_index("grp")
    every = lax.all_gather(small, ("section", "grp", "dp"), axis=0, tiled=False)
    per_plane = every.reshape(ns, ng * nz, 16, width + 128)
    mine = lax.dynamic_index_in_dim(per_plane, section, 0, keepdims=False)[:, 8:10, :width].sum(axis=0)
    grad_gains = lax.dynamic_slice(mine, (0, member * quarter), (2, quarter))
    shard = section * ng + member
    here = rows_count // (ns * ng)
    ids = (shard * here + 1 + jnp.arange(here)).astype(F32)
    stamp = per_plane[0, :, :8, width].reshape(-1)
    pick = (ids[:, None] == stamp[None, :]).astype(F32)
    tokens = per_plane[0, :, :8, :width].reshape(-1, width)
    grad_table = jnp.dot(pick, tokens, precision=lax.Precision.HIGHEST)
    mask_here = width // (ns * ng)
    grad_mask = lax.dynamic_slice(per_plane[0, :, 10, :width].sum(axis=0), (shard * mask_here,), (mask_here,))
    return grad_gains, grad_table, grad_mask


def on_device(
    sizes,
    embeddings,
    mask_flags,
    timesteps,
    time_table,
    mask_vector,
    attn_qkv,
    attn_out,
    mlp_in,
    mlp_out,
    norm_gains,
    cotangent,
):
    ns, ng, nz = sizes
    rows_count, width = time_table.shape
    activations, dx, grads, small, table = run_mega(
        timesteps,
        mask_flags,
        mask_vector,
        norm_gains[0],
        embeddings,
        cotangent,
        time_table,
        attn_qkv[0],
        attn_out[0],
        mlp_in[0],
        mlp_out[0],
        nz,
    )
    quarter = attn_out.shape[1]
    table_here, mask_here = rows_count // (ns * ng), width // (ns * ng)
    if nz != 4:
        grads = lax.psum(grads, "dp")
        gain_sums, table_sums, mask_sums = small_sums(sizes, small, timesteps, rows_count, quarter)
    placed = run_place(
        activations, dx, grads, small, table, quarter, table_here, mask_here
    )
    if nz != 4:
        placed = placed[:6] + (gain_sums, table_sums, mask_sums)
    return tuple(v[None] for v in placed[:7]) + placed[7:]


def solution(mesh):
    sizes = (mesh.shape["section"], mesh.shape["grp"], mesh.shape["dp"])
    placed = (
        P(("grp", "dp"), None, None),
        P(("grp", "dp"), None),
        P(("grp", "dp")),
        P(),
        P(),
        P("section", "grp", None),
        P("section", "grp", None),
        P("section", "grp", None),
        P("section", "grp", None),
        P("section", None, None),
        P(("grp", "dp"), None, None),
    )
    return jax.shard_map(
        functools.partial(on_device, sizes),
        mesh=mesh,
        in_specs=placed,
        out_specs=(
            P("section", ("grp", "dp"), None, None),
            P("section", ("grp", "dp"), None, None),
            P("section", "grp", None),
            P("section", "grp", None),
            P("section", "grp", None),
            P("section", "grp", None),
            P("section", None, "grp"),
            P(("section", "grp"), None),
            P(("section", "grp")),
        ),
        check_vma=False,
    )
```

```python
import functools
import math

import jax
import jax.numpy as jnp
from jax import lax
from jax.experimental import pallas as pl
from jax.experimental.pallas import tpu as pltpu
from jax.sharding import PartitionSpec as P

HEADS = 12
HEAD = 64
BF = jnp.bfloat16
F32 = jnp.float32
MESH = pl.DeviceIdType.MESH
EPS = 1e-05
GELU_C = math.sqrt(2.0 / math.pi)

OUT0, IN0, PROJ, QKV0, CHUNKS = 0, 4, 8, 9, 12
YRING, ZRING = 16, 12
GATHER_ORDER = (9, 10, 11, 8, 4, 5, 6, 7, 0, 1, 2, 3)


def dot_nn(a, b):
    return lax.dot_general(a, b, (((1,), (0,)), ((), ())), preferred_element_type=F32)


def dot_nt(a, b):
    return lax.dot_general(a, b, (((1,), (1,)), ((), ())), preferred_element_type=F32)


def dot_tn(a, b):
    return lax.dot_general(a, b, (((0,), (0,)), ((), ())), preferred_element_type=F32)


def loop(n, body, first=0):
    lax.fori_loop(first, n, lambda i, c: (body(i), c)[1], 0)


def unrolled(n, body):
    for i in range(n):
        body(i)


def mega(
    cfg,
    times_ref,
    mask_ref,
    vector_ref,
    gains_ref,
    emb_hbm,
    cot_hbm,
    table_hbm,
    wq_hbm,
    wp_hbm,
    wi_hbm,
    wo_hbm,
    act_out,
    dx_out,
    grad_out,
    small_hbm,
    table_hbm_out,
    w,
    h,
    mid,
    acc,
    tmp,
    inv_sum,
    normed,
    mixed,
    n2,
    actv,
    gp,
    packed,
    probs,
    glow,
    dmlow,
    dpk,
    do_ref,
    outb,
    relay,
    maskc,
    trow,
    pay,
    sums,
    cbuf,
    ybuf,
    z1,
    z2,
    in_sem,
    own_sem,
    gsend,
    grecv,
    nrecv,
    rsend,
    rrecv,
    csend,
    crecv,
    ysend,
    yrecv,
    zsend,
    zrecv,
    zout,
    psend,
    precv,
    osem,
    small_out,
    table_out,
    *extra,
):
    count, seq, width, nz, unit = cfg
    quarter = width // 4
    units = CHUNKS * quarter // unit
    per_block = quarter // unit
    table_rows = table_hbm.shape[0]
    s = lax.axis_index("section")
    g = lax.axis_index("grp")
    d = lax.axis_index("dp")
    x0 = s == 0
    x1 = jnp.logical_not(x0)
    c = lax.rem(g, 2)
    y = g // 2
    twin = g + 1 - 2 * c
    across = lax.rem(g + 2, 4)
    zpair = d + 1 - 2 * lax.rem(d, 2)
    zfar = lax.rem(d + 2, 4)
    half = lax.rem(d, 2)

    peers = [{"section": 1 - s}, {"grp": twin}, {"grp": across}, {"dp": zpair}]
    if nz == 4:
        peers += [{"dp": 3 - d}, {"dp": zfar}]
    barrier = pltpu.get_barrier_semaphore()
    for peer in peers:
        pl.semaphore_signal(barrier, inc=1, device_id=peer, device_id_type=MESH)

    def remote(src, dst, send, recv, peer):
        return pltpu.make_async_remote_copy(
            src_ref=src, dst_ref=dst, send_sem=send, recv_sem=recv, device_id=peer, device_id_type=MESH
        )

    def rows(start, size, by):
        return pl.ds(pl.multiple_of(start, by), size)

    def place(i, q):
        return jnp.where(i < IN0, q * width + quarter * i, i * width + quarter * q)

    def source(i):
        if i < IN0:
            return wo_hbm.at[pl.ds(i * quarter, quarter)]
        if i < PROJ:
            return wi_hbm.at[:, pl.ds((i - IN0) * width, width)]
        if i == PROJ:
            return wp_hbm
        return wq_hbm.at[:, pl.ds((i - QKV0) * width, width)]

    sixth = quarter // 6
    share = {0: 2, 1: 3}
    far = across

    group_size = (4, 4, 1, 3)

    def group_of(i):
        if isinstance(i, int):
            return i // 4 if i < PROJ else 2 + (i > PROJ)
        return jnp.where(i < PROJ, i // 4, jnp.where(i == PROJ, 2, 3))

    def piece(i, q, first, n):
        return w.at[rows(place(i, q) + first * sixth, n * sixth, sixth)]

    def stage(k, i):
        return dpk.at[rows((k * CHUNKS + i) * sixth, sixth, sixth)]

    def own_copy(i):
        return pltpu.make_async_copy(source(i), w.at[rows(place(i, g), quarter, sixth)], own_sem.at[group_of(i)])

    def own_to_twin(i):
        return remote(source(i), w.at[rows(place(i, g), quarter, sixth)], gsend.at[0], nrecv.at[0, group_of(i)], {"grp": twin})

    def own_across(i, n):
        return remote(
            source(i).at[rows(half * n * sixth, n * sixth, sixth)],
            piece(i, g, half * n, n),
            gsend.at[1],
            grecv.at[0, i],
            {"grp": across},
        )

    def own_across_sixth(i, p):
        r = half * share[1] + p
        return remote(
            source(i).at[rows(r * sixth, sixth, sixth)], piece(i, g, r, 1), gsend.at[1], grecv.at[0, i], {"grp": across}
        )

    def own_over(i):
        return remote(
            source(i).at[rows((4 + half) * sixth, sixth, sixth)],
            stage(0, i),
            gsend.at[5],
            grecv.at[2, i],
            {"section": 1 - s},
        )

    def y_part(i, n):
        return piece(i, far, half * n, n)

    def z_part(i, n):
        return piece(i, far, (1 - half) * n, n)

    def y_to_z(i, n):
        return remote(y_part(i, n), y_part(i, n), gsend.at[2], grecv.at[1, i], {"dp": zpair})

    def y_to_twin(i, n):
        return remote(y_part(i, n), y_part(i, n), gsend.at[3], nrecv.at[1, group_of(i)], {"grp": twin})

    def z_to_twin(i, n):
        return remote(z_part(i, n), z_part(i, n), gsend.at[4], nrecv.at[2, group_of(i)], {"grp": twin})

    def over_to_twin(i):
        both = piece(i, far, 4, 2)
        return remote(both, both, gsend.at[6], nrecv.at[3, group_of(i)], {"grp": twin})

    def wait_for(ref, sem):
        remote(ref, ref, gsend.at[0], sem, {"grp": twin}).wait_recv()

    def stage_across(i):
        return remote(stage(0, i), stage(1, i), gsend.at[5], grecv.at[3, i], {"grp": across})

    def stage_to_z(i):
        return remote(stage(1, i), stage(2, i), gsend.at[7], grecv.at[4, i], {"dp": zpair})

    def stage_back(k, i):
        which = half if k == 1 else 1 - half
        return remote(stage(k, i), piece(i, far, 4 + which, 1), gsend.at[6], grecv.at[2, i], {"section": 1 - s})

    def bulk(n, send, recv, peer):
        return remote(w.at[pl.ds(0, n)], w.at[pl.ds(0, n)], send, recv, peer)

    def near_ready(k):
        n = group_size[k] * quarter
        bulk(n, gsend.at[0], nrecv.at[0, k], {"grp": twin}).wait_recv()
        pltpu.make_async_copy(w.at[pl.ds(0, n)], w.at[pl.ds(0, n)], own_sem.at[k]).wait()

    def far_ready(k, section):
        n = group_size[k] * share[section] * sixth
        bulk(n, gsend.at[3], nrecv.at[1, k], {"grp": twin}).wait_recv()
        bulk(n, gsend.at[4], nrecv.at[2, k], {"grp": twin}).wait_recv()
        if section == 0:
            bulk(group_size[k] * 2 * sixth, gsend.at[6], nrecv.at[3, k], {"grp": twin}).wait_recv()

    def all_ready(k, section):
        near_ready(k)
        far_ready(k, section)

    def gather_order(k):
        return jnp.where(k < 3, QKV0 + k, jnp.where(k == 3, PROJ, jnp.where(k < 8, k, k - 8)))

    def when_block(k, body):
        pl.when(jnp.logical_and(k >= 0, k < CHUNKS))(lambda: body(gather_order(k)))

    zlag, overlag = 2, 5
    ylag, backlag = 2, 4

    def pass_on(k, section):
        n = share[section]

        def from_y(i):
            wait_for(y_part(i, n), grecv.at[0, i])
            y_to_z(i, n).start()
            y_to_twin(i, n).start()

        def from_z(i):
            wait_for(z_part(i, n), grecv.at[1, i])
            z_to_twin(i, n).start()

        when_block(k, from_y)
        when_block(k - zlag, from_z)

    def gather_step(k):
        def from_over(i):
            wait_for(piece(i, far, 4, 2), grecv.at[2, i])
            over_to_twin(i).start()

        pass_on(k, 0)
        when_block(k - overlag, from_over)

    def second_step(k):
        pass_on(k, 1)

    early_blocks = 1 + CHUNKS // share[1]

    def start_sixth(k):
        for m, i in enumerate(GATHER_ORDER[:early_blocks]):
            pl.when(k // share[1] == m)(lambda: own_across_sixth(i, lax.rem(k, share[1])).start())

    def help_step(k):
        def from_x(i):
            wait_for(stage(0, i), grecv.at[2, i])
            stage_across(i).start()

        def from_y(i):
            wait_for(stage(1, i), grecv.at[3, i])
            stage_back(1, i).start()
            stage_to_z(i).start()

        def from_z(i):
            wait_for(stage(2, i), grecv.at[4, i])
            stage_back(2, i).start()

        when_block(k, from_x)
        when_block(k - ylag, from_y)
        when_block(k - backlag, from_z)

    def load(src, dst, k):
        return pltpu.make_async_copy(src, dst, in_sem.at[k])

    table_copy = load(table_hbm, dpk.at[pl.ds(0, table_rows)], 0)
    emb_copy = load(emb_hbm, outb, 1)

    def cot_copy(mb):
        return load(cot_hbm.at[mb], glow.at[rows(mb * seq, seq, seq)], 2 + mb)

    @pl.when(x0)
    def _():
        table_copy.start()
        emb_copy.start()

    @pl.when(x1)
    def _():
        for mb in range(2):
            cot_copy(mb).start()

    for i in GATHER_ORDER:
        own_copy(i).start()
    sums[...] = jnp.zeros_like(sums)
    for mb in range(2):
        maskc[mb] = jnp.transpose(jnp.broadcast_to(mask_ref[mb : mb + 1, :].astype(F32), (128, seq)))

    def enter():
        pl.semaphore_wait(barrier, len(peers))

    enter()

    def issue():
        @pl.when(x0)
        def _():
            for i in GATHER_ORDER:
                own_across(i, share[0]).start()
                own_over(i).start()

        @pl.when(x1)
        def _():
            own_across(GATHER_ORDER[0], share[1]).start()

        for i in GATHER_ORDER:
            own_to_twin(i).start()

    issue()

    def chunk(k):
        return w[rows(k * width, width, width), :]

    step_rows = 32
    parts_of = seq // step_rows
    lane = lax.broadcasted_iota(jnp.int32, (1, 128), 1)
    low_lane = lax.broadcasted_iota(jnp.int32, (seq, 128), 1) < HEAD
    low_half = (lane < HEAD).astype(F32)
    masks = (low_half.astype(BF), (1.0 - low_half).astype(BF))
    scaled = ((low_half * 0.125).astype(BF), ((1.0 - low_half) * 0.125).astype(BF))

    def seq_rows(mb):
        return rows(mb * seq, seq, seq)

    def sub_rows(mb, r):
        return rows(mb * seq + r * step_rows, step_rows, step_rows)

    def r_rows(r):
        return rows(r * step_rows, step_rows, step_rows)

    def norm_parts(v):
        center = v - jnp.mean(v, axis=-1, keepdims=True)
        spread = jnp.mean(center * center, axis=-1, keepdims=True)
        inv = lax.rsqrt(spread + EPS)
        return center * inv, inv

    @pl.when(x1)
    def _():
        def help_and_gather(k):
            help_step(k)
            pl.when(k < CHUNKS)(lambda: start_sixth(k + share[1]))
            pl.when(lax.rem(k, 3) == 1)(lambda: second_step(k // 3))

        loop(CHUNKS, help_and_gather)
        for i in GATHER_ORDER[early_blocks:]:
            own_across(i, share[1]).start()
        loop(CHUNKS + backlag, help_and_gather, CHUNKS)
        loop(11, second_step, early_blocks)
        all_ready(3, 1)
        all_ready(2, 1)

    @pl.when(x0)
    def _():
        table_copy.wait()
        emb_copy.wait()
        ids = lax.broadcasted_iota(jnp.int32, (8, table_rows), 1)
        pick = lax.broadcasted_iota(jnp.int32, (8, table_rows), 0)
        want = jnp.where(pick == 0, times_ref[0], times_ref[1])
        hot = jnp.where(jnp.logical_and(pick < 2, ids == want), 1.0, 0.0).astype(BF)
        trow[...] = dot_nn(hot, dpk[pl.ds(0, table_rows), :])
        vector = vector_ref[...].astype(F32).reshape(1, width)
        for mb in range(2):

            def make(r):
                m = maskc[mb, r_rows(r), 0:1]
                base = jnp.where(m > 0.5, vector, outb[mb, r_rows(r), :].astype(F32))
                h[mb, r_rows(r), :] = base + trow[mb : mb + 1, :]

            loop(parts_of, make)

    def more(mb, t, k):
        @pl.when(x0)
        def _():
            if k < 2:
                gather_step(8 + 2 * t + k)
            else:
                pl.when(t == 1)(lambda: gather_step(12))

        if k < 2:
            pl.when(jnp.logical_and(x1, t == 0))(lambda: second_step(11 + k))

    def first_half(mb, t):
        @pl.when(x1)
        def _():
            h[mb] = relay[mb].astype(F32)

        def ln(r):
            xhat, _ = norm_parts(h[mb, r_rows(r), :])
            normed[sub_rows(mb, r), :] = (xhat * gains_ref[0:1, :]).astype(BF)

        unrolled(parts_of, ln)

        @pl.when(jnp.logical_and(x0, t == 0))
        def _():
            loop(8, gather_step)
            all_ready(3, 0)

        def qkv(k):
            packed[k, seq_rows(mb), :] = dot_nn(normed[seq_rows(mb), :], chunk(QKV0 + k)).astype(BF)

        unrolled(3, qkv)

        more(mb, t, 0)

        def attend(j):
            cols = pl.ds(j * 128, 128)
            q2 = packed[0, seq_rows(mb), cols]
            k2 = packed[1, seq_rows(mb), cols]
            v2 = packed[2, seq_rows(mb), cols]
            got = []
            for e in range(2):
                sc = dot_nt(q2 * scaled[e], k2)
                ex = jnp.exp(sc - jnp.max(sc, axis=-1, keepdims=True)).astype(BF)
                probs[mb, 2 * j + e] = ex
                got.append(dot_nn(ex, v2 * masks[e] + masks[1 - e]))
            inv = 1.0 / pltpu.roll(jnp.where(low_lane, got[1], got[0]), HEAD, 1)
            inv_sum[mb, :, cols] = inv
            mixed[seq_rows(mb), cols] = (jnp.where(low_lane, got[0], got[1]) * inv).astype(BF)

        unrolled(HEADS // 2, attend)

        more(mb, t, 1)

        pl.when(jnp.logical_and(x0, t == 0))(lambda: all_ready(2, 0))
        mid[mb] = h[mb] + dot_nn(mixed[seq_rows(mb), :], chunk(PROJ))

        def ln_two(r):
            xhat, _ = norm_parts(mid[mb, r_rows(r), :])
            n2[sub_rows(mb, r), :] = (xhat * gains_ref[1:2, :]).astype(BF)

        unrolled(parts_of, ln_two)
        more(mb, t, 2)

    def mlp_up(q, mb):
        lhs = n2[seq_rows(mb), :]
        piece = 256
        chunk_rows = rows((IN0 + q) * width, width, width)

        def product(j):
            return dot_nn(lhs, w[chunk_rows, pl.ds(j * piece, piece)])

        up = product(0)
        for j in range(width // piece):
            after = product(j + 1) if (j + 1) * piece < width else None
            cols = pl.ds(j * piece, piece)
            sq = up * up
            hp = 0.5 + 0.5 * jnp.tanh(up * (GELU_C + (GELU_C * 0.044715) * sq))
            act = up * hp
            actv[q, seq_rows(mb), cols] = act.astype(BF)
            gp[q, seq_rows(mb), cols] = (
                hp + act * ((1.0 - hp) * (2.0 * GELU_C + (2.0 * GELU_C * 0.134145) * sq))
            ).astype(BF)
            up = after

    def mlp_down(q, mb):
        acc[mb] += dot_nn(actv[q, seq_rows(mb), :], chunk(OUT0 + q))

    def second_half_one(mb, t):
        def at_first(body):
            pl.when(t == 0)(body)

        at_first(lambda: all_ready(1, 1))
        for q in range(4):
            mlp_up(q, mb)
        acc[mb] = mid[mb]
        at_first(lambda: near_ready(0))
        for r in range(2):
            mlp_down(2 * y + r, mb)

        @at_first
        def _():
            second_step(13)
            far_ready(0, 1)
            for k, n in ((5, 1), (6, 2), (7, 1)):
                bulk(CHUNKS * n * sixth, gsend.at[k], grecv.at[0, 0], {"grp": twin}).wait_send()

        for r in range(2):
            mlp_down(2 * (1 - y) + r, mb)
        outb[mb] = acc[mb].astype(BF)

    def second_half_both():
        all_ready(1, 0)

        def up(q):
            mlp_up(q, 0)
            gather_step(13 + q)

        def finish(mb):
            outb[mb] = acc[mb].astype(BF)
            relay_copy(mb, 0).start()
            relay_copy(mb, 1).start()
            act_copy(mb).start()

        loop(4, up)
        acc[...] = mid[...]
        near_ready(0)
        loop(2, lambda r: mlp_down(2 * y + r, 0))
        far_ready(0, 0)
        loop(2, lambda r: mlp_down(2 * (1 - y) + r, 0))
        finish(0)
        for q in range(4):
            mlp_up(q, 1)
            mlp_down(q, 1)
        finish(1)

    def relay_copy(mb, part):
        r = pl.ds(part * (seq // 2), seq // 2)
        return remote(
            outb.at[mb, r], relay.at[mb, r], rsend.at[mb, part], rrecv.at[mb, part], {"section": 1 - s}
        )

    def act_copy(mb):
        return pltpu.make_async_copy(outb.at[mb], act_out.at[mb], osem.at[0, mb])

    def dx_copy(mb):
        return pltpu.make_async_copy(h.at[mb], dx_out.at[mb], osem.at[1, mb])

    def norm_back(v, gain, dy):
        xhat, inv = norm_parts(v)
        dxh = dy * gain
        m1 = jnp.mean(dxh, axis=-1, keepdims=True)
        m2 = jnp.mean(dxh * xhat, axis=-1, keepdims=True)
        return inv * (dxh - m1 - xhat * m2), jnp.sum(dy * xhat, axis=0, keepdims=True)

    def backward_mlp(mb, t):
        @pl.when(x0)
        def _():
            glow[seq_rows(mb), :] = relay[mb]

        @pl.when(x1)
        def _():
            cot_copy(mb).wait()

        def slope(q):
            da = dot_nt(glow[seq_rows(mb), :], chunk(OUT0 + q))
            du = (gp[q, seq_rows(mb), :].astype(F32) * da).astype(BF)
            gp[q, seq_rows(mb), :] = du
            return du

        def back_up(q):
            tmp[...] += dot_nt(gp[q, seq_rows(mb), :], chunk(IN0 + q))

        def mlp(q):
            got = dot_nt(slope(q), chunk(IN0 + q))
            tmp[...] = got if q == 0 else tmp[...] + got

        def slope_and_out(k):
            slope(out_order(k))
            out_terms(k)

        last = jnp.logical_and(x0, t == 3)

        @pl.when(last)
        def _():
            tmp[...] = jnp.zeros_like(tmp)
            loop(4, slope_and_out)
            loop(4, back_up)

        pl.when(jnp.logical_not(last))(lambda: unrolled(4, mlp))

        def ln_two(r):
            dx, dg = norm_back(mid[mb, r_rows(r), :], gains_ref[1:2, :], tmp[r_rows(r), :])
            dm = glow[sub_rows(mb, r), :].astype(F32) + dx
            mid[mb, r_rows(r), :] = dm
            dmlow[sub_rows(mb, r), :] = dm.astype(BF)
            sums[1:2, :] += dg

        unrolled(parts_of, ln_two)

    def backward_attention(mb, t):
        do_ref[...] = (dot_nt(dmlow[seq_rows(mb), :], chunk(PROJ)) * inv_sum[mb]).astype(BF)

        def attend(j):
            cols = pl.ds(j * 128, 128)
            q2 = packed[0, seq_rows(mb), cols]
            k2 = packed[1, seq_rows(mb), cols]
            v2 = packed[2, seq_rows(mb), cols]
            do2 = do_ref[:, cols]
            weighed = do2.astype(F32) * mixed[seq_rows(mb), cols].astype(F32)
            dq = jnp.zeros((seq, 128), F32)
            dk = jnp.zeros((seq, 128), F32)
            dv = jnp.zeros((seq, 128), F32)
            for e in range(2):
                ex = probs[mb, 2 * j + e]
                dom = do2 * masks[e]
                inner = jnp.sum(jnp.where(low_lane if e == 0 else jnp.logical_not(low_lane), weighed, 0.0), axis=-1, keepdims=True)
                ds = (ex.astype(F32) * (dot_nt(dom, v2) - inner)).astype(BF)
                dv = dv + dot_tn(ex, dom)
                dq = dq + dot_nn(ds, k2 * scaled[e])
                dk = dk + dot_tn(ds, q2 * scaled[e])
            for k, v in enumerate((dq, dk, dv)):
                dpk[rows(k * 2 * seq + mb * seq, seq, seq), cols] = v.astype(BF)

        for j in range(HEADS // 2):
            attend(j)

        early_tick(t, 5)
        early_tick(t, 6)
        tmp[...] = functools.reduce(
            jnp.add,
            [dot_nt(dpk[rows(k * 2 * seq + mb * seq, seq, seq), :], chunk(QKV0 + k)) for k in range(3)],
        )
        early_tick(t, 7)
        act_copy(mb).wait()

        @pl.when(x0)
        def _():
            for part in range(2):
                relay_copy(mb, part).wait_send()

        for part in range(2):

            def ln_one(rr):
                r = rr + part * (parts_of // 2)
                dx, dg = norm_back(h[mb, r_rows(r), :], gains_ref[0:1, :], tmp[r_rows(r), :])
                dm = mid[mb, r_rows(r), :] + dx
                outb[mb, r_rows(r), :] = dm.astype(BF)
                sums[0:1, :] += dg
                m = maskc[mb, r_rows(r), 0:1]
                kept = jnp.where(jnp.logical_and(x0, m > 0.5), 0.0, dm)
                h[mb, r_rows(r), :] = kept
                sums[pl.ds(2 + mb, 1), :] += jnp.sum(dm, axis=0, keepdims=True)
                sums[4:5, :] += jnp.sum(dm - kept, axis=0, keepdims=True)

            unrolled(parts_of // 2, ln_one)

            @pl.when(x1)
            def _():
                relay_copy(mb, part).start()

        dx_copy(mb).start()
        early_tick(t, 8)

    def grad_chunk(a, b, k):
        w[rows(k * width, width, width), :] = dot_tn(a, b).astype(BF)

    def cslot(i, yy):
        return cbuf.at[yy, rows(i * quarter, quarter, quarter)]

    def to_twin(i, yy):
        q = 2 * yy + (1 - c)
        return remote(
            w.at[rows(place(i, q), quarter, quarter)], cslot(i, yy), csend.at[yy], crecv.at[arrival(i, yy)], {"grp": twin}
        )

    def arrival(i, yy):
        return jnp.where(jnp.logical_and(yy == 1 - y, i < IN0), 6 + i, 3 * yy + i // 4)

    def from_twin(k, yy):
        ref = cbuf.at[yy, rows(4 * k * quarter, 4 * quarter, quarter)]
        remote(ref, ref, csend.at[yy], crecv.at[3 * yy + k], {"grp": twin}).wait_recv()

    def urows(u):
        return rows(u * unit, unit, unit)

    def y_send(u):
        k = lax.rem(u, YRING)
        return remote(
            cbuf.at[1 - y, urows(u)], ybuf.at[urows(u)], ysend.at[k], yrecv.at[k], {"grp": across}
        )

    def merge_far(i):
        pl.when(i < IN0)(lambda: wait_for(cslot(i, 1 - y), crecv.at[arrival(i, 1 - y)]))
        pl.when(jnp.logical_and(i >= IN0, lax.rem(i, 4) == 0))(lambda: from_twin(i // 4, 1 - y))
        part = rows(i * quarter, quarter, quarter)
        mine = w[rows(place(i, 2 * (1 - y) + c), quarter, quarter), :].astype(F32)
        cbuf[1 - y, part, :] = (cbuf[1 - y, part, :].astype(F32) + mine).astype(BF)

    ahead = 6

    def send_across(u):
        pl.when(lax.rem(u, per_block) == 0)(lambda: merge_far(u // per_block))
        pl.when(u >= YRING)(lambda: y_send(u - YRING).wait_send())
        y_send(u).start()

    def out_order(k):
        side = jnp.where(k < 2, 1 - y, y)
        return 2 * side + jnp.where(lax.rem(k, 2) == 0, 1 - c, c)

    def out_terms(k):
        q = out_order(k)
        grad_chunk(actv[q], glow[...], OUT0 + q)

        @pl.when(lax.rem(k, 2) == 0)
        def _():
            loop(4, lambda i: to_twin(i, jnp.where(k == 0, 1 - y, y)).start())

        @pl.when(k == 1)
        def _():
            loop(ahead, send_across)

    def other_terms(i, a, b):
        grad_chunk(a, b, i)
        to_twin(i, 1 - y).start()
        to_twin(i, y).start()

    def in_terms():
        early_tick_now(0)

        def one(q):
            other_terms(IN0 + q, n2[...], gp[q])
            early_tick_now(1 + q)

        loop(4, one)

    def attention_terms():
        first = jnp.where(x0, 9, 5)
        other_terms(PROJ, mixed[...], dmlow[...])
        early_tick_now(first)

        def one(k):
            other_terms(QKV0 + k, normed[...], dpk[rows(k * 2 * seq, 2 * seq, 2 * seq), :])
            early_tick_now(first + 1 + k)

        loop(3, one)

    def add_rows(dst, dst_rows, *terms):
        dst[dst_rows, :] = functools.reduce(jnp.add, [a.astype(F32) for a in terms]).astype(BF)

    def sum_across(u):
        i = u // per_block
        pl.when(lax.rem(u, 4 * per_block) == 0)(lambda: from_twin(i // 4, y))
        y_send(u).wait_recv()
        mine = w[rows(place(i, g) + lax.rem(u, per_block) * unit, unit, unit), :]
        add_rows(ybuf, urows(u), cbuf[y, urows(u), :], mine, ybuf[urows(u), :])

    first_tick = jnp.where(x0, 13, 9)
    if nz == 4:
        end = jnp.logical_or(d == 0, d == 3)
        inner = jnp.logical_not(end)
        slots, landed = extra
        pay_copy = remote(pay, landed.at[0], psend.at[0], precv.at[0], {"section": 1 - s})
        last_part = pl.ds(8, 8)

        sums_rows = pl.ds(nz * 8, 8)

        def small_copy(k):
            peer = ({"grp": twin}, {"grp": across}, {"dp": zpair}, {"dp": zfar})[k]
            part = pl.ds(0, 16) if k < 3 else last_part
            return remote(pay.at[part], landed.at[1 + k, part], psend.at[1 + k], precv.at[1 + k], peer)

        pair_rows = rows((d // 2) * 16, 16, 16)
        far_rows = rows((1 - d // 2) * 16, 16, 16)
        pair_copy = remote(slots.at[pair_rows], slots.at[pair_rows], psend.at[5], precv.at[5], {"dp": zfar})
        pair_wait = remote(slots.at[far_rows], slots.at[far_rows], psend.at[5], precv.at[5], {"dp": zfar})
        give_back = remote(slots, slots, psend.at[6], precv.at[6], {"section": 1 - s})

        def small_start():
            pay_copy.wait_recv()
            pay[0:8, :] = landed[0, 0:8, :]
            row = lax.broadcasted_iota(jnp.int32, (8, width + 128), 0)
            other = landed[0, last_part, :]
            pay[last_part, :] = jnp.where(
                row < 2, pay[last_part, :], jnp.where(row == 2, other, pltpu.roll(other, 3, 0))
            )
            small_copy(0).start()

        def small_next(k):
            small_copy(k).wait_recv()
            small_copy(k).wait_send()
            if k < 2:
                pay[...] = pay[...] + landed[1 + k]
                if k == 1:
                    slots[rows(d * 8, 8, 8), :] = pay[0:8, :]
                small_copy(k + 1).start()
            else:
                slots[rows(zpair * 8, 8, 8), :] = landed[3, 0:8, :]
                pay[last_part, :] = pay[last_part, :] + landed[3, last_part, :]
                small_copy(3).start()
                pair_copy.start()

        def small_end():
            small_copy(3).wait_recv()
            small_copy(3).wait_send()
            pair_wait.wait_recv()
            slots[sums_rows, :] = pay[last_part, :] + landed[4, last_part, :]
            give_back.start()

        def small_results():
            pl.when(x0)(lambda: give_back.wait_recv())
            total = slots[sums_rows, 0:width]
            shard = s * 4 + g
            mine = jnp.where(x0, pltpu.roll(total, 5, 0), total)
            small_out[0:8, :] = pltpu.roll(mine, lax.rem(width - quarter * g, width), 1)
            small_out[8:16, :] = pltpu.roll(total, lax.rem(width - (width // 8) * shard, width), 1)
            base = shard * (table_rows // 8) + 1
            ids = (base + lax.broadcasted_iota(jnp.int32, (nz * 8, 128), 1)).astype(F32)
            pick = jnp.where(slots[0 : nz * 8, pl.ds(width, 128)] == ids, 1.0, 0.0).astype(BF)
            rest = slots[0 : nz * 8, 0:width]
            found = jnp.zeros((128, width), F32)
            for _ in range(3):
                part = rest.astype(BF)
                found = found + dot_tn(pick, part)
                rest = rest - part.astype(F32)
            table_out[...] = found
            small_leaves()

        def zcopy(src, dst, k, u, peer):
            m = lax.rem(u, ZRING)
            return remote(src.at[urows(u)], dst.at[urows(u)], zsend.at[k, m], zrecv.at[k, m], peer)

        def end_to_inner(u):
            return zcopy(ybuf, z1, 0, u, {"dp": zpair})

        def inner_swap(u):
            return zcopy(z1, z2, 1, u, {"dp": 3 - d})

        def inner_to_end(u):
            return zcopy(z2, z1, 0, u, {"dp": zpair})

        def grad_copy(src, u):
            return pltpu.make_async_copy(src.at[urows(u)], grad_out.at[urows(u)], zout.at[lax.rem(u, ZRING)])

        def launch(copy, u):
            pl.when(u >= ZRING)(lambda: copy(u - ZRING).wait_send())
            copy(u).start()

        def put_out(src, u):
            pl.when(u >= ZRING)(lambda: grad_copy(src, u - ZRING).wait())
            grad_copy(src, u).start()

        lag3, lag4, lag5 = 3, 6, 9
        first_small, small_gap = 16, 6

        def tick(t, small=True):
            u2, u3, u4, u5 = t, t - lag3, t - lag4, t - lag5
            pl.when(u2 + ahead < units)(lambda: send_across(u2 + ahead))

            @pl.when(u2 < units)
            def _():
                sum_across(u2)

                @pl.when(end)
                def _():
                    launch(end_to_inner, u2)

            @pl.when(jnp.logical_and(inner, jnp.logical_and(u3 >= 0, u3 < units)))
            def _():
                end_to_inner(u3).wait_recv()
                add_rows(z1, urows(u3), ybuf[urows(u3), :], z1[urows(u3), :])
                launch(inner_swap, u3)

            @pl.when(jnp.logical_and(inner, jnp.logical_and(u4 >= 0, u4 < units)))
            def _():
                inner_swap(u4).wait_recv()
                add_rows(z2, urows(u4), z1[urows(u4), :], z2[urows(u4), :])
                launch(inner_to_end, u4)
                put_out(z2, u4)

            @pl.when(jnp.logical_and(end, jnp.logical_and(u5 >= 0, u5 < units)))
            def _():
                inner_to_end(u5).wait_recv()
                put_out(z1, u5)

            if not small:
                return
            pl.when(t == jnp.where(x1, units, units + 2))(small_results)

            @pl.when(x1)
            def _():
                pl.when(t == first_small)(small_start)
                for k in range(3):
                    pl.when(t == first_small + small_gap * (k + 1))(functools.partial(small_next, k))
                pl.when(t == first_small + small_gap * 4)(small_end)

    else:

        def out_sum(u):
            return pltpu.make_async_copy(ybuf.at[urows(u)], grad_out.at[urows(u)], zout.at[lax.rem(u, ZRING)])

        def tick(u, small=True):
            pl.when(u + ahead < units)(lambda: send_across(u + ahead))
            sum_across(u)
            pl.when(u >= ZRING)(lambda: out_sum(u - ZRING).wait())
            out_sum(u).start()

    def early_tick_now(t):
        tick(t, False)

    def early_tick(t, k):
        pl.when(jnp.logical_and(x0, t == 3))(lambda: early_tick_now(k))

    leaving = (
        pltpu.make_async_copy(small_out, small_hbm, osem.at[0, 2]),
        pltpu.make_async_copy(table_out, table_hbm_out, osem.at[1, 2]),
    )

    def small_leaves():
        for copy in leaving:
            copy.start()

    def step(t):
        mb = jnp.where(x0, lax.rem(t, 2), t // 2)
        is_f = jnp.where(x0, t < 2, lax.rem(t, 2) == 0)

        @pl.when(is_f)
        def _():
            @pl.when(x1)
            def _():
                relay_copy(mb, 0).wait_recv()
                relay_copy(mb, 1).wait_recv()

            first_half(mb, t)

            pl.when(jnp.logical_and(x0, t == 1))(second_half_both)

            @pl.when(x1)
            def _():
                second_half_one(mb, t)
                act_copy(mb).start()

        @pl.when(jnp.logical_not(is_f))
        def _():
            @pl.when(x0)
            def _():
                for part in range(2):
                    relay_copy(mb, part).wait_recv()

            @pl.when(jnp.logical_and(x0, t == 3))
            def _():
                gather_sent(0)

            backward_mlp(mb, t)

            @pl.when(jnp.logical_and(x0, t == 3))
            def _():
                in_terms()

            backward_attention(mb, t)

    def gather_sent(section):
        bulk(CHUNKS * quarter, gsend.at[0], nrecv.at[0, 0], {"grp": twin}).wait_send()
        n = CHUNKS * share[section] * sixth
        for k in range(1, 5):
            bulk(n, gsend.at[k], grecv.at[0, 0], {"grp": twin}).wait_send()
        if section == 0:
            for k, n in ((5, 1), (6, 2)):
                bulk(CHUNKS * n * sixth, gsend.at[k], grecv.at[0, 0], {"grp": twin}).wait_send()

    loop(4, step)

    @pl.when(x1)
    def _():
        gather_sent(1)
        loop(4, out_terms)
        in_terms()

    row_ids = lax.broadcasted_iota(jnp.int32, (8, width), 0)
    stamp_ids = lax.broadcasted_iota(jnp.int32, (8, 128), 0)
    first = 2 * g
    pay[0:8, 0:width] = jnp.where(
        row_ids == first, sums[2:3, :], jnp.where(row_ids == first + 1, sums[3:4, :], 0.0)
    )
    pay[0:8, pl.ds(width, 128)] = jnp.where(
        stamp_ids == first,
        (times_ref[0] + 1).astype(F32),
        jnp.where(stamp_ids == first + 1, (times_ref[1] + 1).astype(F32), 0.0),
    )
    pay[8:16, 0:width] = jnp.where(
        row_ids < 2, sums[...], jnp.where(row_ids == 2, sums[4:5, :], 0.0)
    )
    pay[8:16, pl.ds(width, 128)] = jnp.zeros((8, 128), F32)

    if nz == 4:
        pl.when(x0)(lambda: pay_copy.start())

    attention_terms()

    if nz == 4:
        loop(units + lag5, tick, first_tick)

        loop(units, lambda u: y_send(u).wait_send(), units - YRING)

        def drain(u):
            @pl.when(end)
            def _():
                end_to_inner(u).wait_send()
                grad_copy(z1, u).wait()

            @pl.when(inner)
            def _():
                inner_swap(u).wait_send()
                inner_to_end(u).wait_send()
                grad_copy(z2, u).wait()

        loop(units, drain, units - ZRING)

        pl.when(x0)(lambda: pay_copy.wait_send())

        @pl.when(x1)
        def _():
            pair_copy.wait_send()
            give_back.wait_send()

    else:
        small_out[...] = pay[...]
        table_out[...] = jnp.zeros_like(table_out)
        small_leaves()
        loop(units, tick, first_tick)

        loop(units, lambda u: y_send(u).wait_send(), units - YRING)
        loop(units, lambda u: out_sum(u).wait(), units - ZRING)

    for yy in range(2):
        bulk(CHUNKS * quarter, csend.at[yy], crecv.at[0], {"grp": twin}).wait_send()

    for copy in leaving:
        copy.wait()
    for mb in range(2):
        dx_copy(mb).wait()

        @pl.when(x1)
        def _():
            for part in range(2):
                relay_copy(mb, part).wait_send()


def run_mega(timesteps, mask_flags, vector, gains, emb, cot, table, wq, wp, wi, wo, nz):
    count, seq, width = emb.shape
    quarter = wp.shape[0]
    unit = quarter // 4
    units = CHUNKS * quarter // unit
    tokens = count * seq
    assert count == 2 and quarter * 4 == width and wi.shape[1] == 4 * width and wo.shape[0] == width
    vmem = pl.BlockSpec(memory_space=pltpu.VMEM)
    smem = pl.BlockSpec(memory_space=pltpu.SMEM)
    hbm = pl.BlockSpec(memory_space=pl.ANY)
    dma = pltpu.SemaphoreType.DMA
    small = (16, width) if nz == 4 else (16, width + 128)
    extra = [pltpu.VMEM((nz * 8 + 8, width + 128), F32), pltpu.VMEM((5, 16, width + 128), F32)]
    return pl.pallas_call(
        functools.partial(mega, (count, seq, width, nz, unit)),
        out_shape=(
            jax.ShapeDtypeStruct((count, seq, width), BF),
            jax.ShapeDtypeStruct((count, seq, width), F32),
            jax.ShapeDtypeStruct((CHUNKS * quarter, width), BF),
            jax.ShapeDtypeStruct(small, F32),
            jax.ShapeDtypeStruct((128, width), F32),
        ),
        in_specs=[smem, vmem, vmem, vmem] + [hbm] * 7,
        out_specs=(hbm,) * 5,
        scratch_shapes=[
            pltpu.VMEM((CHUNKS * width, width), BF),
            pltpu.VMEM((count, seq, width), F32),
            pltpu.VMEM((count, seq, width), F32),
            pltpu.VMEM((count, seq, width), F32),
            pltpu.VMEM((seq, width), F32),
            pltpu.VMEM((count, seq, width), F32),
            pltpu.VMEM((tokens, width), BF),
            pltpu.VMEM((tokens, width), BF),
            pltpu.VMEM((tokens, width), BF),
            pltpu.VMEM((4, tokens, width), BF),
            pltpu.VMEM((4, tokens, width), BF),
            pltpu.VMEM((3, tokens, width), BF),
            pltpu.VMEM((count, HEADS, seq, seq), BF),
            pltpu.VMEM((tokens, width), BF),
            pltpu.VMEM((tokens, width), BF),
            pltpu.VMEM((3 * tokens, width), BF),
            pltpu.VMEM((seq, width), BF),
            pltpu.VMEM((count, seq, width), BF),
            pltpu.VMEM((count, seq, width), BF),
            pltpu.VMEM((count, seq, 128), F32),
            pltpu.VMEM((8, width), F32),
            pltpu.VMEM((16, width + 128), F32),
            pltpu.VMEM((8, width), F32),
            pltpu.VMEM((2, CHUNKS * quarter, width), BF),
            pltpu.VMEM((CHUNKS * quarter, width), BF),
            pltpu.VMEM((CHUNKS * quarter, width), BF),
            pltpu.VMEM((CHUNKS * quarter, width), BF),
            dma((4,)),
            dma((4,)),
            dma((8,)),
            dma((5, CHUNKS)),
            dma((4, 4)),
            dma((2, 2)),
            dma((2, 2)),
            dma((2,)),
            dma((10,)),
            dma((YRING,)),
            dma((YRING,)),
            dma((2, ZRING)),
            dma((2, ZRING)),
            dma((ZRING,)),
            dma((7,)),
            dma((7,)),
            dma((2, 3)),
            pltpu.VMEM(small, F32),
            pltpu.VMEM((128, width), F32),
        ]
        + (extra if nz == 4 else []),
        compiler_params=pltpu.CompilerParams(
            collective_id=0, has_side_effects=True, vmem_limit_bytes=67043328
        ),
        name="relay_layers",
    )(timesteps, mask_flags, vector, gains, emb, cot, table, wq, wp, wi, wo)


def place_results(
    act_in,
    dx_in,
    grads_in,
    small_ref,
    table_ref,
    act_out,
    dx_out,
    qkv_out,
    proj_out,
    in_out,
    out_out,
    gains_out,
    table_out,
    mask_out,
    act_buf,
    dx_buf,
    low_buf,
    wide_buf,
    ins,
    outs,
):
    quarter, width = proj_out.shape
    blocks = []
    for i in range(CHUNKS):
        part = pl.ds(i * quarter, quarter)
        if i < IN0:
            target = out_out.at[part]
        elif i < PROJ:
            target = in_out.at[:, pl.ds((i - IN0) * width, width)]
        elif i == PROJ:
            target = proj_out
        else:
            target = qkv_out.at[:, pl.ds((i - QKV0) * width, width)]
        blocks.append(
            (
                part,
                pltpu.make_async_copy(grads_in.at[part], low_buf.at[part], ins.at[i]),
                pltpu.make_async_copy(wide_buf.at[part], target, outs.at[i]),
            )
        )
    plain = [
        (
            pltpu.make_async_copy(dx_in, dx_buf, ins.at[CHUNKS]),
            pltpu.make_async_copy(dx_buf, dx_out, outs.at[CHUNKS]),
        ),
        (
            pltpu.make_async_copy(act_in, act_buf, ins.at[CHUNKS + 1]),
            pltpu.make_async_copy(act_buf, act_out, outs.at[CHUNKS + 1]),
        ),
    ]
    for come, _ in plain:
        come.start()
    for _, come, _ in blocks:
        come.start()
    for come, go in plain:
        come.wait()
        go.start()
    for part, come, go in blocks:
        come.wait()
        wide_buf[part, :] = low_buf[part, :].astype(F32)
        go.start()
    gains_out[...] = small_ref[0:2, 0:quarter]
    table_out[...] = table_ref[0 : table_out.shape[0], :]
    mask_out[...] = small_ref[10, 0 : mask_out.shape[0]]
    for _, _, go in blocks:
        go.wait()
    for _, go in plain:
        go.wait()


def run_place(activations, dx, grads, small, table, quarter, table_here, mask_here):
    count, seq, width = dx.shape
    vmem = pl.BlockSpec(memory_space=pltpu.VMEM)
    hbm = pl.BlockSpec(memory_space=pl.ANY)
    dma = pltpu.SemaphoreType.DMA
    shapes = (
        ((count, seq, width), BF),
        ((count, seq, width), F32),
        ((quarter, 3 * width), F32),
        ((quarter, width), F32),
        ((quarter, 4 * width), F32),
        ((width, width), F32),
        ((2, quarter), F32),
        ((table_here, width), F32),
        ((mask_here,), F32),
    )
    return pl.pallas_call(
        place_results,
        out_shape=tuple(jax.ShapeDtypeStruct(a, b) for a, b in shapes),
        in_specs=[hbm] * 3 + [vmem] * 2,
        out_specs=(hbm,) * 6 + (vmem,) * 3,
        scratch_shapes=[
            pltpu.VMEM((count, seq, width), BF),
            pltpu.VMEM((count, seq, width), F32),
            pltpu.VMEM((CHUNKS * quarter, width), BF),
            pltpu.VMEM((CHUNKS * quarter, width), F32),
            dma((CHUNKS + 2,)),
            dma((CHUNKS + 2,)),
        ],
        compiler_params=pltpu.CompilerParams(vmem_limit_bytes=64000000),
        name="place_results",
    )(activations, dx, grads, small, table)


def small_sums(sizes, small, timesteps, rows_count, quarter):
    ns, ng, nz = sizes
    width = quarter * 4
    section, member = lax.axis_index("section"), lax.axis_index("grp")
    every = lax.all_gather(small, ("section", "grp", "dp"), axis=0, tiled=False)
    per_plane = every.reshape(ns, ng * nz, 16, width + 128)
    mine = lax.dynamic_index_in_dim(per_plane, section, 0, keepdims=False)[:, 8:10, :width].sum(axis=0)
    grad_gains = lax.dynamic_slice(mine, (0, member * quarter), (2, quarter))
    shard = section * ng + member
    here = rows_count // (ns * ng)
    ids = (shard * here + 1 + jnp.arange(here)).astype(F32)
    stamp = per_plane[0, :, :8, width].reshape(-1)
    pick = (ids[:, None] == stamp[None, :]).astype(F32)
    tokens = per_plane[0, :, :8, :width].reshape(-1, width)
    grad_table = jnp.dot(pick, tokens, precision=lax.Precision.HIGHEST)
    mask_here = width // (ns * ng)
    grad_mask = lax.dynamic_slice(per_plane[0, :, 10, :width].sum(axis=0), (shard * mask_here,), (mask_here,))
    return grad_gains, grad_table, grad_mask


def on_device(
    sizes,
    embeddings,
    mask_flags,
    timesteps,
    time_table,
    mask_vector,
    attn_qkv,
    attn_out,
    mlp_in,
    mlp_out,
    norm_gains,
    cotangent,
):
    ns, ng, nz = sizes
    rows_count, width = time_table.shape
    activations, dx, grads, small, table = run_mega(
        timesteps,
        mask_flags,
        mask_vector,
        norm_gains[0],
        embeddings,
        cotangent,
        time_table,
        attn_qkv[0],
        attn_out[0],
        mlp_in[0],
        mlp_out[0],
        nz,
    )
    quarter = attn_out.shape[1]
    table_here, mask_here = rows_count // (ns * ng), width // (ns * ng)
    if nz != 4:
        grads = lax.psum(grads, "dp")
        gain_sums, table_sums, mask_sums = small_sums(sizes, small, timesteps, rows_count, quarter)
    placed = run_place(
        activations, dx, grads, small, table, quarter, table_here, mask_here
    )
    if nz != 4:
        placed = placed[:6] + (gain_sums, table_sums, mask_sums)
    return tuple(v[None] for v in placed[:7]) + placed[7:]


def solution(mesh):
    sizes = (mesh.shape["section"], mesh.shape["grp"], mesh.shape["dp"])
    placed = (
        P(("grp", "dp"), None, None),
        P(("grp", "dp"), None),
        P(("grp", "dp")),
        P(),
        P(),
        P("section", "grp", None),
        P("section", "grp", None),
        P("section", "grp", None),
        P("section", "grp", None),
        P("section", None, None),
        P(("grp", "dp"), None, None),
    )
    return jax.shard_map(
        functools.partial(on_device, sizes),
        mesh=mesh,
        in_specs=placed,
        out_specs=(
            P("section", ("grp", "dp"), None, None),
            P("section", ("grp", "dp"), None, None),
            P("section", "grp", None),
            P("section", "grp", None),
            P("section", "grp", None),
            P("section", "grp", None),
            P("section", None, "grp"),
            P(("section", "grp"), None),
            P(("section", "grp")),
        ),
        check_vma=False,
    )
```
